32 devices in a mesh: group: 16 (over z, y, core), shard: 2 (over x).
Axes of the slice: x: 2, y: 2, z: 4, core: 2. Of those that a mesh axis runs over, the one named last changes fastest.
Arguments:
- tokens: float32 [16384, 1024], P(('group', 'shard')), may hold values from -6 to 6
- cotangent: float32 [16384, 1024], P(('group', 'shard')), may hold values from -6 to 6
- lengths: int32 [16], replicated, may hold values from 512 to 1024, as said below
- qkv_weight: float32 [1024, 3072], P('shard'), may hold values from -0.1875 to 0.1875
- qkv_momentum: float32 [1024, 3072], P('shard')
- qkv_average: float32 [1024, 3072], P('shard'), may hold values from -0.1875 to 0.1875
- out_weight: float32 [1024, 1024], P('shard'), may hold values from -0.5 to 0.5
- out_momentum: float32 [1024, 1024], P('shard')
- out_average: float32 [1024, 1024], P('shard'), may hold values from -0.5 to 0.5
- up_weight: float32 [1024, 4096], P(None, 'shard'), may hold values from -0.1875 to 0.1875
- up_momentum: float32 [1024, 4096], P(None, 'shard')
- up_average: float32 [1024, 4096], P(None, 'shard'), may hold values from -0.1875 to 0.1875
- down_weight: float32 [4096, 1024], P('shard'), may hold values from -0.09375 to 0.09375
- down_momentum: float32 [4096, 1024], P('shard')
- down_average: float32 [4096, 1024], P('shard'), may hold values from -0.09375 to 0.09375
- small_params: float32 [12, 1024], P(None, 'shard')
- small_momentum: float32 [12, 1024], P(None, 'shard')
- small_average: float32 [12, 1024], P(None, 'shard')
Outputs:
- block_out: float32 [16384, 1024], P(('group', 'shard'))
- input_grad: float32 [16384, 1024], P(('group', 'shard'))
- qkv_weight_new: float32 [1024, 3072], P('shard')
- qkv_momentum_new: float32 [1024, 3072], P('shard')
- qkv_average_new: float32 [1024, 3072], P('shard')
- out_weight_new: float32 [1024, 1024], P('shard')
- out_momentum_new: float32 [1024, 1024], P('shard')
- out_average_new: float32 [1024, 1024], P('shard')
- up_weight_new: float32 [1024, 4096], P(None, 'shard')
- up_momentum_new: float32 [1024, 4096], P(None, 'shard')
- up_average_new: float32 [1024, 4096], P(None, 'shard')
- down_weight_new: float32 [4096, 1024], P('shard')
- down_momentum_new: float32 [4096, 1024], P('shard')
- down_average_new: float32 [4096, 1024], P('shard')
- small_params_new: float32 [12, 1024], P(None, 'shard')
- small_momentum_new: float32 [12, 1024], P(None, 'shard')
- small_average_new: float32 [12, 1024], P(None, 'shard')
The draws below stay inside these ranges and needn't reach their ends.
Inputs may be any that keep to these rules, and one draw needn't show every extreme that they name: `lengths`: the first 512 positions of every sequence are live; in every draw some sequence is live in all 1024 positions and some in exactly 512.
All inputs are finite; a program needn't handle non-finite values.
Results may differ from the reference program's by a relative error of at most 0.012.
Values may be sent and summed in bfloat16 or wider, within the bound.
A program may use at most 384 MiB of HBM per device.

```python
import math
import jax
import jax.numpy as jnp
from jax import lax

D = 1024
HEADS = 16
HD = 64
FF = 4096
NSMALL = 12
TOK_DEV = 512
TOKENS = 16384
SEQS = 16


def draw_lengths(key, part):
    first_key, second_key = jax.random.split(jax.random.fold_in(key, 3))
    counts = jax.random.randint(first_key, (SEQS,), TOK_DEV, 2 * TOK_DEV + 1)
    order = jax.random.permutation(second_key, SEQS)
    counts = counts.at[order[0]].set(2 * TOK_DEV)
    counts = counts.at[order[1]].set(TOK_DEV)
    return counts.astype(jnp.int32)


def moment_draw(key, row_count, col_count, factor):
    scale_value = factor * math.sqrt(TOKENS)
    noise = jnp.clip(jax.random.normal(key, (row_count, col_count), jnp.float32), -4.0, 4.0)
    return scale_value * noise


def draw_qkv_momentum(key, part):
    return moment_draw(jax.random.fold_in(key, 11), D, 3 * D, 0.05)


def draw_out_momentum(key, part):
    return moment_draw(jax.random.fold_in(key, 12), D, D, 0.25)


def draw_up_momentum(key, part):
    return moment_draw(jax.random.fold_in(key, 13), D, FF, 0.2)


def draw_down_momentum(key, part):
    return moment_draw(jax.random.fold_in(key, 14), FF, D, 0.5)


def draw_small_momentum(key, part):
    return moment_draw(jax.random.fold_in(key, 15), NSMALL, D, 0.5)


def table_draw(key):
    noise = jnp.clip(jax.random.normal(key, (NSMALL, D), jnp.float32), -4.0, 4.0)
    row_index = jnp.arange(NSMALL)[:, None]
    gain_rows = (row_index == 0) | (row_index == 5)
    return jnp.where(gain_rows, 1.0 + 0.15 * noise, 0.3 * noise)


def draw_small_params(key, part):
    return table_draw(jax.random.fold_in(key, 21))


def draw_small_average(key, part):
    return table_draw(jax.random.fold_in(key, 22))


def block_scale(key, shape, cuts, least, top_value):
    def one(axis_at, shards_of):
        heights = jax.random.uniform(jax.random.fold_in(jax.random.fold_in(key, 6), axis_at), (shards_of,), jnp.float32, least / len(cuts), top_value / len(cuts))
        return jnp.repeat(jnp.exp(heights), shape[axis_at] // shards_of).reshape((-1,) + (1,) * (len(shape) - axis_at - 1))

    gain = one(*cuts[0])
    for cut in cuts[1:]:
        gain = gain * one(*cut)
    return gain


def normal_values(own_key, shape, scale, limit, shards=(), held_as=jnp.bfloat16):
    array = scale * jax.random.normal(own_key, shape, jnp.float32)
    if shards:
        array = array * block_scale(own_key, shape, shards, -0.22, 0.18)
    return jnp.clip(array, -limit, limit).astype(held_as)


def setup_inputs(seed: int = 0) -> dict:
    keys = jax.random.split(jax.random.key(seed), 19)
    tokens = normal_values(keys[0], (TOKENS, D), 1.0, 6.0, ((0, 32),), jnp.float32)
    cotangent = normal_values(keys[1], (TOKENS, D), 1.0, 6.0, ((0, 32),), jnp.float32)
    lengths = draw_lengths(jax.random.fold_in(keys[18], 71), 0)
    qkv_weight = normal_values(keys[3], (D, 3 * D), D ** -0.5, 0.1875, ((0, 2),), jnp.float32)
    qkv_momentum = draw_qkv_momentum(jax.random.fold_in(keys[18], 71), 0)
    qkv_average = normal_values(keys[5], (D, 3 * D), D ** -0.5, 0.1875, ((0, 2),), jnp.float32)
    out_weight = normal_values(keys[6], (D, D), (D // 8) ** -0.5, 0.5, ((0, 2),), jnp.float32)
    out_momentum = draw_out_momentum(jax.random.fold_in(keys[18], 71), 0)
    out_average = normal_values(keys[8], (D, D), (D // 8) ** -0.5, 0.5, ((0, 2),), jnp.float32)
    up_weight = normal_values(keys[9], (D, FF), D ** -0.5, 0.1875, ((1, 2),), jnp.float32)
    up_momentum = draw_up_momentum(jax.random.fold_in(keys[18], 71), 0)
    up_average = normal_values(keys[11], (D, FF), D ** -0.5, 0.1875, ((1, 2),), jnp.float32)
    down_weight = normal_values(keys[12], (FF, D), FF ** -0.5, 0.09375, ((0, 2),), jnp.float32)
    down_momentum = draw_down_momentum(jax.random.fold_in(keys[18], 71), 0)
    down_average = normal_values(keys[14], (FF, D), FF ** -0.5, 0.09375, ((0, 2),), jnp.float32)
    small_params = draw_small_params(jax.random.fold_in(keys[18], 71), 0)
    small_momentum = draw_small_momentum(jax.random.fold_in(keys[18], 71), 0)
    small_average = draw_small_average(jax.random.fold_in(keys[18], 71), 0)
    return dict(tokens=tokens, cotangent=cotangent, lengths=lengths, qkv_weight=qkv_weight, qkv_momentum=qkv_momentum, qkv_average=qkv_average, out_weight=out_weight, out_momentum=out_momentum, out_average=out_average, up_weight=up_weight, up_momentum=up_momentum, up_average=up_average, down_weight=down_weight, down_momentum=down_momentum, down_average=down_average, small_params=small_params, small_momentum=small_momentum, small_average=small_average)


@jax.custom_vjp
def low(v):
    return lax.optimization_barrier(v.astype(jnp.bfloat16)).astype(jnp.float32)

@jax.custom_vjp
def low_back(v):
    return v

def low_keep(v):
    return (low(v), None)

def low_pass(kept, grad):
    return (grad,)

def back_keep(v):
    return (v, None)

def back_low(kept, grad):
    return (low(grad),)
low.defvjp(low_keep, low_pass)
low_back.defvjp(back_keep, back_low)
EPS = 1e-05
MOMENTUM = 0.9
AVERAGING = 0.9
NEG_FILL = -1e+30
HIGHEST = lax.Precision.HIGHEST

def layer_norm(field_in, gain_row, shift_row):
    centred = field_in - lax.optimization_barrier(jnp.mean(field_in, axis=-1, keepdims=True))
    inverse = lax.rsqrt(lax.optimization_barrier(jnp.mean(centred * centred, axis=-1, keepdims=True)) + EPS)
    return centred * inverse * gain_row + shift_row

def project(field_in, matrix):
    return jnp.einsum('bsd,dn->bsn', field_in, matrix, precision=HIGHEST)

def block_forward(params, field_in, seq_lengths):
    qkv_matrix, out_matrix, up_matrix, down_matrix, table = [low(member) for member in params]
    batch_size = field_in.shape[0]
    slot_len = field_in.shape[1]
    entry = low(layer_norm(field_in, table[0], table[1]))
    mapped = low_back(project(entry, qkv_matrix))
    queries = low(mapped[..., :D] + table[2])
    key_all = low(mapped[..., D:2 * D])
    value_all = low(mapped[..., 2 * D:] + table[3])
    query_heads = queries.reshape(batch_size, slot_len, HEADS, HD)
    key_heads = key_all.reshape(batch_size, slot_len, HEADS, HD)
    value_heads = value_all.reshape(batch_size, slot_len, HEADS, HD)
    scores = jnp.einsum('bqhd,bkhd->bhqk', query_heads, key_heads, precision=HIGHEST) * HD ** (-0.5)
    positions = jnp.arange(slot_len, dtype=jnp.int32)
    distance = (positions[:, None] - positions[None, :]).astype(jnp.float32)
    slopes = 2.0 ** (-8.0 * (jnp.arange(HEADS, dtype=jnp.float32) + 1.0) / HEADS)
    scores = scores - slopes[None, :, None, None] * distance[None, None]
    scores = low_back(scores)
    causal = (positions[None, :] <= positions[:, None])[None, None]
    within = positions[None, None, None, :] < seq_lengths[:, None, None, None]
    scores = jnp.where(causal & within, scores, NEG_FILL)
    probs = jax.nn.softmax(scores, axis=-1)
    mixture = jnp.einsum('bhqk,bkhd->bqhd', low(probs), value_heads, precision=HIGHEST)
    mixture = low(low_back(mixture.reshape(batch_size, slot_len, D)))
    resid = field_in + low_back(project(mixture, out_matrix)) + table[4]
    inner = low(layer_norm(resid, table[5], table[6]))
    pre_act = low_back(project(inner, up_matrix)) + table[8:12].reshape(FF)
    act = low(jax.nn.gelu(pre_act, approximate=True))
    return resid + low_back(project(act, down_matrix)) + table[7]

def add_pair(left_side, right_side):
    return left_side + right_side

def zeros_like_f32(member):
    return jnp.zeros(member.shape, jnp.float32)

def nesterov(grad_total, weight_old, moment_old, average_old, rate):
    moment_new = MOMENTUM * moment_old + grad_total
    weight_new = weight_old - rate * (grad_total + MOMENTUM * moment_new)
    average_new = AVERAGING * average_old + (1.0 - AVERAGING) * weight_new
    return (weight_new, moment_new, average_new)

def reference(tokens, cotangent, lengths, qkv_weight, qkv_momentum, qkv_average, out_weight, out_momentum, out_average, up_weight, up_momentum, up_average, down_weight, down_momentum, down_average, small_params, small_momentum, small_average):
    slot_len = 2 * TOK_DEV
    batches = SEQS // 4
    params = (qkv_weight, out_weight, up_weight, down_weight, small_params)
    token_blocks = tokens.reshape(batches, 4, slot_len, D)
    back_blocks = cotangent.reshape(batches, 4, slot_len, D)
    length_blocks = lengths.reshape(batches, 4)

    def scan_step(carry, member):
        field_in, back_in, seq_lengths = member

        def forward_fn(param_set, field_set):
            return block_forward(param_set, field_set, seq_lengths)
        outputs, pull_back = jax.vjp(forward_fn, params, field_in)
        live_rows = (jnp.arange(slot_len, dtype=jnp.int32)[None, :] < seq_lengths[:, None]).astype(jnp.float32)
        param_grads, field_grad = pull_back(back_in * live_rows[:, :, None])
        return (jax.tree.map(add_pair, carry, param_grads), (outputs, field_grad))
    start = jax.tree.map(zeros_like_f32, params)
    grads, stacked = lax.scan(scan_step, start, (token_blocks, back_blocks, length_blocks))
    block_out = stacked[0].reshape(TOKENS, D)
    input_grad = stacked[1].reshape(TOKENS, D)
    rate = 2.0 / math.sqrt(D * TOKENS)
    qkv_new = nesterov(grads[0], qkv_weight, qkv_momentum, qkv_average, rate)
    out_new = nesterov(grads[1], out_weight, out_momentum, out_average, rate)
    up_new = nesterov(grads[2], up_weight, up_momentum, up_average, rate)
    down_new = nesterov(grads[3], down_weight, down_momentum, down_average, rate)
    small_new = nesterov(grads[4], small_params, small_momentum, small_average, rate)
    return (block_out, input_grad, qkv_new[0], qkv_new[1], qkv_new[2], out_new[0], out_new[1], out_new[2], up_new[0], up_new[1], up_new[2], down_new[0], down_new[1], down_new[2], small_new[0], small_new[1], small_new[2])
```

```python
import math

import jax
import jax.numpy as jnp
from jax import lax
from jax.sharding import PartitionSpec as P

HEADS = 16
FF = 4096


EPS = 1e-05
MOMENTUM = 0.9
AVERAGING = 0.9
NEG_FILL = -1e30


def passed_along(value, axis, steps):
    count = lax.axis_size(axis)
    leading, last = (max(0, -steps), min(count, count - steps))
    return lax.ppermute(value, axis, [(source, source + steps) for source in range(leading, last)])


def gather_weight(weight_own, dim):
    low_own = weight_own.astype(jnp.bfloat16)
    cores = lax.axis_size("core")
    quarter = low_own.shape[dim] // cores
    mine = lax.dynamic_slice_in_dim(low_own, lax.axis_index("core") * quarter, quarter, axis=dim)
    across = lax.all_gather(mine, "shard", axis=0, tiled=False)
    both = lax.all_gather(across, "core", axis=0, tiled=False)
    if dim == 0:
        ordered = both.transpose(1, 0, 2, 3)
        return ordered.reshape(-1, ordered.shape[-1])
    ordered = both.transpose(2, 1, 0, 3)
    return ordered.reshape(ordered.shape[0], -1)


def reduce_grad(grad_full, dim):
    low_full = grad_full.astype(jnp.bfloat16)
    shard_count = lax.axis_size("shard")
    cores = lax.axis_size("core")
    outer = lax.axis_size("outer")
    rows, cols = low_full.shape
    if dim == 0:
        split = low_full.reshape(shard_count, cores, rows // (shard_count * cores), cols)
        split = split.transpose(1, 0, 2, 3)
    else:
        split = low_full.reshape(rows, shard_count, cores, cols // (shard_count * cores))
        split = split.transpose(2, 1, 0, 3)
    split = lax.psum_scatter(split, "core", scatter_dimension=0, tiled=True)
    split = lax.psum_scatter(split, "shard", scatter_dimension=1, tiled=True)
    piece = split.reshape(split.shape[2:])
    spread_dim = 0 if piece.shape[0] % outer == 0 else 1
    piece = lax.psum_scatter(piece, "outer", scatter_dimension=spread_dim, tiled=True)
    piece = lax.all_gather(piece, "outer", axis=spread_dim, tiled=True)
    piece = lax.all_gather(piece, "core", axis=0, tiled=False)
    if dim == 0:
        piece = piece.reshape(-1, piece.shape[-1])
    else:
        piece = piece.transpose(1, 0, 2).reshape(piece.shape[1], -1)
    return piece.astype(jnp.float32)


def norm_stats(field_in):
    centred = field_in - jnp.mean(field_in, axis=-1, keepdims=True)
    inverse = lax.rsqrt(jnp.mean(centred * centred, axis=-1, keepdims=True) + EPS)
    return (centred * inverse, inverse)


def norm_back(grad_hat, normed, inverse):
    first_mean = jnp.mean(grad_hat, axis=-1, keepdims=True)
    second_mean = jnp.mean(grad_hat * normed, axis=-1, keepdims=True)
    return inverse * (grad_hat - first_mean - normed * second_mean)


def contract_rows(left_side, right_side):
    return lax.dot_general(
        left_side, right_side, (((0,), (0,)), ((), ())), preferred_element_type=jnp.float32
    )


def contract_cols(left_side, right_side):
    return lax.dot_general(
        left_side, right_side, (((1,), (1,)), ((), ())), preferred_element_type=jnp.float32
    )


def split_heads(field_in):
    return field_in.reshape(field_in.shape[0], HEADS, -1).transpose(1, 0, 2)


def merge_heads(field_in):
    return field_in.transpose(1, 0, 2).reshape(field_in.shape[1], -1)


def gelu_tanh(field_in):
    return jax.nn.gelu(field_in, approximate=True)


def gelu_back(pre_act, grad_act):
    unused, pull_back = jax.vjp(gelu_tanh, pre_act)
    return pull_back(grad_act)[0]


def head_scores(queries, key_block, slope, allowed, distance, score_scale):
    raw = contract_cols(queries, key_block) * score_scale - slope * distance
    return jnp.where(allowed, raw, NEG_FILL)


def nesterov(grad_total, weight_old, moment_old, average_old, rate):
    moment_new = MOMENTUM * moment_old + grad_total
    weight_new = weight_old - rate * (grad_total + MOMENTUM * moment_new)
    average_new = AVERAGING * average_old + (1.0 - AVERAGING) * weight_new
    return (weight_new, moment_new, average_new)


def body(
    tokens,
    cotangent,
    lengths,
    qkv_weight,
    qkv_momentum,
    qkv_average,
    out_weight,
    out_momentum,
    out_average,
    up_weight,
    up_momentum,
    up_average,
    down_weight,
    down_momentum,
    down_average,
    small_params,
    small_momentum,
    small_average,
):
    tok_rows = tokens.shape[0]
    model_width = tokens.shape[1]
    shard_count = lax.axis_size("shard")
    group_count = lax.axis_size("outer") * lax.axis_size("core")
    shard_place = lax.axis_index("shard")
    group_place = lax.axis_index("outer") * lax.axis_size("core") + lax.axis_index("core")
    upper_half = shard_place % 2
    seq_place = group_place * (shard_count // 2) + shard_place // 2
    seq_length = lax.dynamic_index_in_dim(lengths, seq_place, 0, keepdims=False)
    local_pos = jnp.arange(tok_rows, dtype=jnp.int32)
    query_pos = upper_half * tok_rows + local_pos
    key_pos = jnp.concatenate([local_pos, query_pos])
    prev_live = jnp.full((tok_rows,), upper_half == 1)
    key_live = jnp.concatenate([prev_live, jnp.ones((tok_rows,), bool)]) & (key_pos < seq_length)
    allowed = key_live[None, :] & (key_pos[None, :] <= query_pos[:, None])
    distance = (query_pos[:, None] - key_pos[None, :]).astype(jnp.float32)
    row_live = (query_pos < seq_length).astype(jnp.float32)[:, None]
    head_size = model_width // HEADS
    score_scale = head_size ** (-0.5)
    slopes = 2.0 ** (-8.0 * (jnp.arange(HEADS, dtype=jnp.float32) + 1.0) / HEADS)
    qkv_full = gather_weight(qkv_weight, 0)
    out_full = gather_weight(out_weight, 0)
    small_full = gather_weight(small_params, 1)
    up_full = gather_weight(up_weight, 1)
    down_full = gather_weight(down_weight, 0)
    table = small_full.astype(jnp.float32)
    up_bias = table[8:12].reshape(FF)
    normed_one, inverse_one = norm_stats(tokens)
    entry_low = (normed_one * table[0] + table[1]).astype(jnp.bfloat16)
    mapped = jnp.dot(entry_low, qkv_full, preferred_element_type=jnp.float32)
    queries = (mapped[:, :model_width] + table[2]).astype(jnp.bfloat16)
    key_own = mapped[:, model_width : 2 * model_width].astype(jnp.bfloat16)
    value_own = (mapped[:, 2 * model_width :] + table[3]).astype(jnp.bfloat16)
    received = passed_along(jnp.concatenate([key_own, value_own], 1), "shard", 1)
    key_all = jnp.concatenate([received[:, :model_width], key_own], 0)
    value_all = jnp.concatenate([received[:, model_width:], value_own], 0)
    query_heads = split_heads(queries)
    key_heads = split_heads(key_all)
    value_heads = split_heads(value_all)

    def head_forward(head_item):
        head_query, head_keys, head_values, slope = head_item
        scores = head_scores(head_query, head_keys, slope, allowed, distance, score_scale)
        row_top = jnp.max(scores, axis=-1, keepdims=True)
        weights = jnp.exp(scores - row_top)
        row_total = jnp.sum(weights, axis=-1, keepdims=True)
        probs_low = (weights / row_total).astype(jnp.bfloat16)
        mixture = jnp.dot(probs_low, head_values, preferred_element_type=jnp.float32)
        return (mixture, (row_top + jnp.log(row_total))[:, 0])

    mixture_heads, log_total = lax.map(head_forward, (query_heads, key_heads, value_heads, slopes))
    attended_low = merge_heads(mixture_heads).astype(jnp.bfloat16)
    resid_one = (
        tokens + jnp.dot(attended_low, out_full, preferred_element_type=jnp.float32) + table[4]
    )
    normed_two, inverse_two = norm_stats(resid_one)
    inner_low = (normed_two * table[5] + table[6]).astype(jnp.bfloat16)
    grad_out = cotangent * row_live
    down_bias_grad = jnp.sum(grad_out, axis=0)
    grad_low = grad_out.astype(jnp.bfloat16)
    pre_act = jnp.dot(inner_low, up_full, preferred_element_type=jnp.float32) + up_bias
    act_low = gelu_tanh(pre_act).astype(jnp.bfloat16)
    branch_out = jnp.dot(act_low, down_full, preferred_element_type=jnp.float32)
    block_out = resid_one + branch_out + table[7]
    grad_act = contract_cols(grad_low, down_full)
    down_grad = contract_rows(act_low, grad_low)
    grad_pre = gelu_back(pre_act, grad_act)
    up_bias_grad = jnp.sum(grad_pre, axis=0)
    pre_low = grad_pre.astype(jnp.bfloat16)
    up_grad = contract_rows(inner_low, pre_low)
    grad_inner = contract_cols(pre_low, up_full)
    gain_two_grad = jnp.sum(grad_inner * normed_two, axis=0)
    shift_two_grad = jnp.sum(grad_inner, axis=0)
    grad_resid = grad_out + norm_back(grad_inner * table[5], normed_two, inverse_two)
    out_bias_grad = jnp.sum(grad_resid, axis=0)
    resid_low = grad_resid.astype(jnp.bfloat16)
    out_grad = contract_rows(attended_low, resid_low)
    grad_mixture = contract_cols(resid_low, out_full).astype(jnp.bfloat16)
    grad_heads = split_heads(grad_mixture)

    def head_backward(head_item):
        head_query, head_keys, head_values, head_grad, head_lse, slope = head_item
        scores = head_scores(head_query, head_keys, slope, allowed, distance, score_scale)
        probs = jnp.exp(scores - head_lse[:, None])
        probs_low = probs.astype(jnp.bfloat16)
        grad_values = contract_rows(probs_low, head_grad)
        grad_probs = contract_cols(head_grad, head_values)
        row_delta = jnp.sum(probs * grad_probs, axis=-1, keepdims=True)
        grad_scores = (probs * (grad_probs - row_delta)).astype(jnp.bfloat16)
        grad_query = (
            jnp.dot(grad_scores, head_keys, preferred_element_type=jnp.float32) * score_scale
        )
        grad_keys = contract_rows(grad_scores, head_query) * score_scale
        return (grad_query, grad_keys, grad_values)

    query_grads, key_grads, value_grads = lax.map(
        head_backward, (query_heads, key_heads, value_heads, grad_heads, log_total, slopes)
    )
    grad_query = merge_heads(query_grads)
    grad_keys = merge_heads(key_grads)
    grad_values = merge_heads(value_grads)
    returned = passed_along(
        jnp.concatenate([grad_keys[:tok_rows], grad_values[:tok_rows]], 1).astype(jnp.bfloat16),
        "shard",
        -1,
    ).astype(jnp.float32)
    grad_key_own = grad_keys[tok_rows:] + returned[:, :model_width]
    grad_value_own = grad_values[tok_rows:] + returned[:, model_width:]
    query_bias_grad = jnp.sum(grad_query, axis=0)
    value_bias_grad = jnp.sum(grad_value_own, axis=0)
    mapped_low = jnp.concatenate([grad_query, grad_key_own, grad_value_own], 1).astype(jnp.bfloat16)
    qkv_grad = contract_rows(entry_low, mapped_low)
    grad_entry = contract_cols(mapped_low, qkv_full)
    gain_one_grad = jnp.sum(grad_entry * normed_one, axis=0)
    shift_one_grad = jnp.sum(grad_entry, axis=0)
    input_grad = grad_resid + norm_back(grad_entry * table[0], normed_one, inverse_one)
    head_rows = jnp.stack(
        [
            gain_one_grad,
            shift_one_grad,
            query_bias_grad,
            value_bias_grad,
            out_bias_grad,
            gain_two_grad,
            shift_two_grad,
            down_bias_grad,
        ]
    )
    small_grad = jnp.concatenate([head_rows, up_bias_grad.reshape(4, model_width)], 0)
    qkv_total = reduce_grad(qkv_grad, 0)
    out_total = reduce_grad(out_grad, 0)
    up_total = reduce_grad(up_grad, 1)
    down_total = reduce_grad(down_grad, 0)
    small_total = reduce_grad(small_grad, 1)
    rate = 2.0 / math.sqrt(model_width * tok_rows * shard_count * group_count)
    qkv_new = nesterov(qkv_total, qkv_weight, qkv_momentum, qkv_average, rate)
    out_new = nesterov(out_total, out_weight, out_momentum, out_average, rate)
    up_new = nesterov(up_total, up_weight, up_momentum, up_average, rate)
    down_new = nesterov(down_total, down_weight, down_momentum, down_average, rate)
    small_new = nesterov(small_total, small_params, small_momentum, small_average, rate)
    return (
        block_out,
        input_grad,
        qkv_new[0],
        qkv_new[1],
        qkv_new[2],
        out_new[0],
        out_new[1],
        out_new[2],
        up_new[0],
        up_new[1],
        up_new[2],
        down_new[0],
        down_new[1],
        down_new[2],
        small_new[0],
        small_new[1],
        small_new[2],
    )


def solution(mesh):
    cores = 2
    devices = mesh.devices.reshape(mesh.shape["group"] // cores, cores, mesh.shape["shard"])
    inner_mesh = jax.sharding.Mesh(devices, ("outer", "core", "shard"))
    rows = P(("outer", "core", "shard"), None)
    in_specs = (
        rows,
        rows,
        P(),
        P("shard", None),
        P("shard", None),
        P("shard", None),
        P("shard", None),
        P("shard", None),
        P("shard", None),
        P(None, "shard"),
        P(None, "shard"),
        P(None, "shard"),
        P("shard", None),
        P("shard", None),
        P("shard", None),
        P(None, "shard"),
        P(None, "shard"),
        P(None, "shard"),
    )
    out_specs = (
        rows,
        rows,
        P("shard", None),
        P("shard", None),
        P("shard", None),
        P("shard", None),
        P("shard", None),
        P("shard", None),
        P(None, "shard"),
        P(None, "shard"),
        P(None, "shard"),
        P("shard", None),
        P("shard", None),
        P("shard", None),
        P(None, "shard"),
        P(None, "shard"),
        P(None, "shard"),
    )
    return jax.shard_map(body, mesh=inner_mesh, in_specs=in_specs, out_specs=out_specs, check_vma=False)
```

```python
import math

import jax
import jax.numpy as jnp
from jax import lax
from jax.sharding import PartitionSpec as P


HEADS = 16
FF = 4096


EPS = 1e-05
MOMENTUM = 0.9
AVERAGING = 0.9
NEG_FILL = -1e30


def passed_along(value, axis, steps):
    count = lax.axis_size(axis)
    leading, last = (max(0, -steps), min(count, count - steps))
    return lax.ppermute(value, axis, [(source, source + steps) for source in range(leading, last)])


def gather_weight(weight_own, dim):
    low_own = weight_own.astype(jnp.bfloat16)
    cores = lax.axis_size("core")
    quarter = low_own.shape[dim] // cores
    mine = lax.dynamic_slice_in_dim(low_own, lax.axis_index("core") * quarter, quarter, axis=dim)
    across = lax.all_gather(mine, "shard", axis=0, tiled=False)
    both = lax.all_gather(across, "core", axis=0, tiled=False)
    if dim == 0:
        ordered = both.transpose(1, 0, 2, 3)
        return ordered.reshape(-1, ordered.shape[-1])
    ordered = both.transpose(2, 1, 0, 3)
    return ordered.reshape(ordered.shape[0], -1)


LANE = 1024


def pack_halves(grad_full, dim, blocks):
    shard_count = lax.axis_size("shard")
    rows, cols = grad_full.shape
    if dim == 0:
        halves = grad_full.reshape(shard_count, -1)
    else:
        halves = grad_full.reshape(rows, shard_count, cols // shard_count).transpose(1, 0, 2)
        halves = halves.reshape(shard_count, -1)
    half_size = halves.shape[1]
    padded = -(-half_size // (blocks * LANE)) * blocks * LANE
    if padded != half_size:
        halves = jnp.pad(halves, ((0, 0), (0, padded - half_size)))
    return halves.reshape(shard_count, blocks, -1, LANE), half_size


def unpack_half(packed, half_size, half_shape):
    return packed.reshape(-1)[:half_size].reshape(half_shape)


def reduce_grads(grads):
    shard_count = lax.axis_size("shard")
    cores = lax.axis_size("core")
    outer = lax.axis_size("outer")
    blocks = cores * outer
    packed, sizes, shapes = [], [], []
    for grad_full, dim in grads:
        piece, half_size = pack_halves(grad_full, dim, blocks)
        packed.append(piece)
        sizes.append(half_size)
        rows, cols = grad_full.shape
        shapes.append((rows // shard_count, cols) if dim == 0 else (rows, cols // shard_count))
    widths = [piece.shape[2] for piece in packed]
    return reduce_packed(packed, widths, sizes, shapes)


def reduce_packed(packed, widths, sizes, shapes):
    shard_count = lax.axis_size("shard")
    cores = lax.axis_size("core")
    outer = lax.axis_size("outer")
    blocks = cores * outer
    stacked = jnp.concatenate(packed, axis=2).astype(jnp.bfloat16)
    stacked = stacked.reshape(shard_count, cores, outer, -1, LANE).transpose(1, 2, 0, 3, 4)
    stacked = stacked.reshape(cores, -1, LANE)
    stacked = lax.psum_scatter(stacked, "core", scatter_dimension=0, tiled=True)
    stacked = stacked.reshape(outer, -1, LANE)
    stacked = lax.psum_scatter(stacked, "outer", scatter_dimension=0, tiled=True)
    stacked = stacked.reshape(shard_count, -1, LANE)
    stacked = lax.psum_scatter(stacked, "shard", scatter_dimension=0, tiled=True)
    stacked = stacked.reshape(stacked.shape[1:])
    stacked = lax.all_gather(stacked, "outer", axis=0, tiled=True)
    stacked = lax.all_gather(stacked, "core", axis=0, tiled=True)
    stacked = stacked.reshape(blocks, -1, LANE).astype(jnp.float32)
    totals = []
    offset = 0
    for width, half_size, half_shape in zip(widths, sizes, shapes):
        totals.append(unpack_half(stacked[:, offset : offset + width], half_size, half_shape))
        offset += width
    return totals


def norm_stats(field_in):
    centred = field_in - jnp.mean(field_in, axis=-1, keepdims=True)
    inverse = lax.rsqrt(jnp.mean(centred * centred, axis=-1, keepdims=True) + EPS)
    return (centred * inverse, inverse)


def norm_back(grad_hat, normed, inverse):
    first_mean = jnp.mean(grad_hat, axis=-1, keepdims=True)
    second_mean = jnp.mean(grad_hat * normed, axis=-1, keepdims=True)
    return inverse * (grad_hat - first_mean - normed * second_mean)


def contract_rows(left_side, right_side):
    return lax.dot_general(
        left_side, right_side, (((0,), (0,)), ((), ())), preferred_element_type=jnp.float32
    )


def contract_cols(left_side, right_side):
    return lax.dot_general(
        left_side, right_side, (((1,), (1,)), ((), ())), preferred_element_type=jnp.float32
    )


def split_heads(field_in):
    return field_in.reshape(field_in.shape[0], HEADS, -1).transpose(1, 0, 2)


def merge_heads(field_in):
    return field_in.transpose(1, 0, 2).reshape(field_in.shape[1], -1)


def gelu_tanh(field_in):
    return jax.nn.gelu(field_in, approximate=True)


def gelu_back(pre_act, grad_act):
    _, pull_back = jax.vjp(gelu_tanh, pre_act)
    return pull_back(grad_act)[0]


def head_scores(queries, key_block, slope, allowed, distance, score_scale):
    raw = contract_cols(queries, key_block) * score_scale - slope * distance
    return jnp.where(allowed, raw, NEG_FILL)


def nesterov(grad_total, weight_old, moment_old, average_old, rate):
    moment_new = MOMENTUM * moment_old + grad_total
    weight_new = weight_old - rate * (grad_total + MOMENTUM * moment_new)
    average_new = AVERAGING * average_old + (1.0 - AVERAGING) * weight_new
    return (weight_new, moment_new, average_new)


def body(
    tokens,
    cotangent,
    lengths,
    qkv_weight,
    qkv_momentum,
    qkv_average,
    out_weight,
    out_momentum,
    out_average,
    up_weight,
    up_momentum,
    up_average,
    down_weight,
    down_momentum,
    down_average,
    small_params,
    small_momentum,
    small_average,
):
    tok_rows = tokens.shape[0]
    model_width = tokens.shape[1]
    shard_count = lax.axis_size("shard")
    group_count = lax.axis_size("outer") * lax.axis_size("core")
    shard_place = lax.axis_index("shard")
    group_place = lax.axis_index("outer") * lax.axis_size("core") + lax.axis_index("core")
    upper_half = shard_place % 2
    seq_place = group_place * (shard_count // 2) + shard_place // 2
    seq_length = lax.dynamic_index_in_dim(lengths, seq_place, 0, keepdims=False)
    local_pos = jnp.arange(tok_rows, dtype=jnp.int32)
    query_pos = upper_half * tok_rows + local_pos
    key_pos = jnp.concatenate([local_pos, query_pos])
    prev_live = jnp.full((tok_rows,), upper_half == 1)
    key_live = jnp.concatenate([prev_live, jnp.ones((tok_rows,), bool)]) & (key_pos < seq_length)
    allowed = key_live[None, :] & (key_pos[None, :] <= query_pos[:, None])
    distance = (query_pos[:, None] - key_pos[None, :]).astype(jnp.float32)
    row_live = (query_pos < seq_length).astype(jnp.float32)[:, None]
    head_size = model_width // HEADS
    score_scale = head_size ** (-0.5)
    slopes = 2.0 ** (-8.0 * (jnp.arange(HEADS, dtype=jnp.float32) + 1.0) / HEADS)
    qkv_full = gather_weight(qkv_weight, 0)
    out_full = gather_weight(out_weight, 0)
    small_full = gather_weight(small_params, 1)
    up_full = gather_weight(up_weight, 1)
    down_full = gather_weight(down_weight, 0)
    table = small_full.astype(jnp.float32)
    up_bias = table[8:12].reshape(FF)
    normed_one, inverse_one = norm_stats(tokens)
    entry_low = (normed_one * table[0] + table[1]).astype(jnp.bfloat16)
    mapped = jnp.dot(entry_low, qkv_full, preferred_element_type=jnp.float32)
    queries = (mapped[:, :model_width] + table[2]).astype(jnp.bfloat16)
    key_own = mapped[:, model_width : 2 * model_width].astype(jnp.bfloat16)
    value_own = (mapped[:, 2 * model_width :] + table[3]).astype(jnp.bfloat16)
    received = passed_along(jnp.concatenate([key_own, value_own], 1), "shard", 1)
    key_all = jnp.concatenate([received[:, :model_width], key_own], 0)
    value_all = jnp.concatenate([received[:, model_width:], value_own], 0)
    query_heads = split_heads(queries)
    key_heads = split_heads(key_all)
    value_heads = split_heads(value_all)

    def head_forward(head_item):
        head_query, head_keys, head_values, slope = head_item
        scores = head_scores(head_query, head_keys, slope, allowed, distance, score_scale)
        row_top = jnp.max(scores, axis=-1, keepdims=True)
        weights = jnp.exp(scores - row_top)
        row_total = jnp.sum(weights, axis=-1, keepdims=True)
        probs_low = (weights / row_total).astype(jnp.bfloat16)
        mixture = jnp.dot(probs_low, head_values, preferred_element_type=jnp.float32)
        return (mixture, (row_top + jnp.log(row_total))[:, 0])

    mixture_heads, log_total = lax.map(head_forward, (query_heads, key_heads, value_heads, slopes))
    attended_low = merge_heads(mixture_heads).astype(jnp.bfloat16)
    resid_one = (
        tokens + jnp.dot(attended_low, out_full, preferred_element_type=jnp.float32) + table[4]
    )
    normed_two, inverse_two = norm_stats(resid_one)
    inner_low = (normed_two * table[5] + table[6]).astype(jnp.bfloat16)
    grad_out = cotangent * row_live
    down_bias_grad = jnp.sum(grad_out, axis=0)
    grad_low = grad_out.astype(jnp.bfloat16)
    pre_act = jnp.dot(inner_low, up_full, preferred_element_type=jnp.float32) + up_bias
    act_low = gelu_tanh(pre_act).astype(jnp.bfloat16)
    branch_out = jnp.dot(act_low, down_full, preferred_element_type=jnp.float32)
    block_out = resid_one + branch_out + table[7]
    grad_act = contract_cols(grad_low, down_full)
    down_grad = contract_rows(act_low, grad_low)
    grad_pre = gelu_back(pre_act, grad_act)
    up_bias_grad = jnp.sum(grad_pre, axis=0)
    pre_low = grad_pre.astype(jnp.bfloat16)
    up_grad = contract_rows(inner_low, pre_low)
    grad_inner = contract_cols(pre_low, up_full)
    gain_two_grad = jnp.sum(grad_inner * normed_two, axis=0)
    shift_two_grad = jnp.sum(grad_inner, axis=0)
    grad_resid = grad_out + norm_back(grad_inner * table[5], normed_two, inverse_two)
    grad_resid, up_grad, down_grad = lax.optimization_barrier((grad_resid, up_grad, down_grad))
    up_total, down_total = reduce_grads([(up_grad, 1), (down_grad, 0)])
    out_bias_grad = jnp.sum(grad_resid, axis=0)
    resid_low = grad_resid.astype(jnp.bfloat16)
    out_grad = contract_rows(attended_low, resid_low)
    grad_mixture = contract_cols(resid_low, out_full).astype(jnp.bfloat16)
    grad_heads = split_heads(grad_mixture)

    def head_backward(head_item):
        head_query, head_keys, head_values, head_grad, head_lse, slope = head_item
        scores = head_scores(head_query, head_keys, slope, allowed, distance, score_scale)
        probs = jnp.exp(scores - head_lse[:, None])
        probs_low = probs.astype(jnp.bfloat16)
        grad_values = contract_rows(probs_low, head_grad)
        grad_probs = contract_cols(head_grad, head_values)
        row_delta = jnp.sum(probs * grad_probs, axis=-1, keepdims=True)
        grad_scores = (probs * (grad_probs - row_delta)).astype(jnp.bfloat16)
        grad_query = (
            jnp.dot(grad_scores, head_keys, preferred_element_type=jnp.float32) * score_scale
        )
        grad_keys = contract_rows(grad_scores, head_query) * score_scale
        return (grad_query, grad_keys, grad_values)

    query_grads, key_grads, value_grads = lax.map(
        head_backward, (query_heads, key_heads, value_heads, grad_heads, log_total, slopes)
    )
    grad_query = merge_heads(query_grads)
    grad_keys = merge_heads(key_grads)
    grad_values = merge_heads(value_grads)
    returned = passed_along(
        jnp.concatenate([grad_keys[:tok_rows], grad_values[:tok_rows]], 1).astype(jnp.bfloat16),
        "shard",
        -1,
    ).astype(jnp.float32)
    grad_key_own = grad_keys[tok_rows:] + returned[:, :model_width]
    grad_value_own = grad_values[tok_rows:] + returned[:, model_width:]
    query_bias_grad = jnp.sum(grad_query, axis=0)
    value_bias_grad = jnp.sum(grad_value_own, axis=0)
    mapped_low = jnp.concatenate([grad_query, grad_key_own, grad_value_own], 1).astype(jnp.bfloat16)
    qkv_grad = contract_rows(entry_low, mapped_low)
    grad_entry = contract_cols(mapped_low, qkv_full)
    gain_one_grad = jnp.sum(grad_entry * normed_one, axis=0)
    shift_one_grad = jnp.sum(grad_entry, axis=0)
    input_grad = grad_resid + norm_back(grad_entry * table[0], normed_one, inverse_one)
    head_rows = jnp.stack(
        [
            gain_one_grad,
            shift_one_grad,
            query_bias_grad,
            value_bias_grad,
            out_bias_grad,
            gain_two_grad,
            shift_two_grad,
            down_bias_grad,
        ]
    )
    small_grad = jnp.concatenate([head_rows, up_bias_grad.reshape(4, model_width)], 0)
    qkv_total, out_total, small_total = reduce_grads([(qkv_grad, 0), (out_grad, 0), (small_grad, 1)])
    rate = 2.0 / math.sqrt(model_width * tok_rows * shard_count * group_count)
    qkv_new = nesterov(qkv_total, qkv_weight, qkv_momentum, qkv_average, rate)
    out_new = nesterov(out_total, out_weight, out_momentum, out_average, rate)
    up_new = nesterov(up_total, up_weight, up_momentum, up_average, rate)
    down_new = nesterov(down_total, down_weight, down_momentum, down_average, rate)
    small_new = nesterov(small_total, small_params, small_momentum, small_average, rate)
    return (
        block_out,
        input_grad,
        qkv_new[0],
        qkv_new[1],
        qkv_new[2],
        out_new[0],
        out_new[1],
        out_new[2],
        up_new[0],
        up_new[1],
        up_new[2],
        down_new[0],
        down_new[1],
        down_new[2],
        small_new[0],
        small_new[1],
        small_new[2],
    )


def solution(mesh):
    cores = 2
    devices = mesh.devices.reshape(mesh.shape["group"] // cores, cores, mesh.shape["shard"])
    inner_mesh = jax.sharding.Mesh(devices, ("outer", "core", "shard"))
    rows = P(("outer", "core", "shard"), None)
    in_specs = (
        rows,
        rows,
        P(),
        P("shard", None),
        P("shard", None),
        P("shard", None),
        P("shard", None),
        P("shard", None),
        P("shard", None),
        P(None, "shard"),
        P(None, "shard"),
        P(None, "shard"),
        P("shard", None),
        P("shard", None),
        P("shard", None),
        P(None, "shard"),
        P(None, "shard"),
        P(None, "shard"),
    )
    out_specs = (
        rows,
        rows,
        P("shard", None),
        P("shard", None),
        P("shard", None),
        P("shard", None),
        P("shard", None),
        P("shard", None),
        P(None, "shard"),
        P(None, "shard"),
        P(None, "shard"),
        P("shard", None),
        P("shard", None),
        P("shard", None),
        P(None, "shard"),
        P(None, "shard"),
        P(None, "shard"),
    )

    return jax.shard_map(body, mesh=inner_mesh, in_specs=in_specs, out_specs=out_specs, check_vma=False)
```

```python
import math

import jax
import jax.numpy as jnp
from jax import lax
from jax.sharding import PartitionSpec as P


HEADS = 16
FF = 4096


EPS = 1e-05
MOMENTUM = 0.9
AVERAGING = 0.9
NEG_FILL = -1e30


def passed_along(value, axis, steps):
    count = lax.axis_size(axis)
    leading, last = (max(0, -steps), min(count, count - steps))
    return lax.ppermute(value, axis, [(source, source + steps) for source in range(leading, last)])


LANE = 1024


def to_blocks(half, blocks):
    flat = half.reshape(-1)
    size = flat.shape[0]
    padded = -(-size // (blocks * LANE)) * blocks * LANE
    if padded != size:
        flat = jnp.pad(flat, (0, padded - size))
    return flat.reshape(blocks, -1, LANE)


def gather_weights(halves):
    cores = lax.axis_size("core")
    outer = lax.axis_size("outer")
    blocks = cores * outer
    lows = [half.astype(jnp.bfloat16) for half, unused in halves]
    packed = [to_blocks(low, blocks) for low in lows]
    widths = [piece.shape[1] for piece in packed]
    own = jnp.concatenate(packed, axis=1)
    place = lax.axis_index("core") * outer + lax.axis_index("outer")
    mine = lax.dynamic_index_in_dim(own, place, 0, keepdims=False)
    other = lax.ppermute(mine, "shard", [(0, 1), (1, 0)])
    got = lax.all_gather(other, "outer", axis=0, tiled=False)
    got = lax.all_gather(got, "core", axis=0, tiled=False)
    got = got.reshape(blocks, -1, LANE)
    upper = lax.axis_index("shard") == 1
    fulls = []
    offset = 0
    for (half, dim), low, width in zip(halves, lows, widths):
        other_half = got[:, offset : offset + width].reshape(-1)[: low.size].reshape(low.shape)
        offset += width
        in_order = jnp.concatenate([low, other_half], axis=dim)
        swapped = jnp.concatenate([other_half, low], axis=dim)
        fulls.append(jnp.where(upper, swapped, in_order))
    return fulls


def pack_halves(grad_full, dim, blocks):
    shard_count = lax.axis_size("shard")
    rows, cols = grad_full.shape
    if dim == 0:
        halves = grad_full.reshape(shard_count, -1)
    else:
        halves = grad_full.reshape(rows, shard_count, cols // shard_count).transpose(1, 0, 2)
        halves = halves.reshape(shard_count, -1)
    half_size = halves.shape[1]
    padded = -(-half_size // (blocks * LANE)) * blocks * LANE
    if padded != half_size:
        halves = jnp.pad(halves, ((0, 0), (0, padded - half_size)))
    return halves.reshape(shard_count, blocks, -1, LANE), half_size


def unpack_half(packed, half_size, half_shape):
    return packed.reshape(-1)[:half_size].reshape(half_shape)


def reduce_grads(grads):
    shard_count = lax.axis_size("shard")
    cores = lax.axis_size("core")
    outer = lax.axis_size("outer")
    blocks = cores * outer
    packed, sizes, shapes = [], [], []
    for grad_full, dim in grads:
        piece, half_size = pack_halves(grad_full, dim, blocks)
        packed.append(piece)
        sizes.append(half_size)
        rows, cols = grad_full.shape
        shapes.append((rows // shard_count, cols) if dim == 0 else (rows, cols // shard_count))
    widths = [piece.shape[2] for piece in packed]
    return reduce_packed(packed, widths, sizes, shapes)


def reduce_packed(packed, widths, sizes, shapes):
    shard_count = lax.axis_size("shard")
    cores = lax.axis_size("core")
    outer = lax.axis_size("outer")
    blocks = cores * outer
    stacked = jnp.concatenate(packed, axis=2).astype(jnp.bfloat16)
    stacked = stacked.reshape(shard_count, cores, outer, -1, LANE).transpose(1, 2, 0, 3, 4)
    stacked = stacked.reshape(cores, -1, LANE)
    stacked = lax.psum_scatter(stacked, "core", scatter_dimension=0, tiled=True)
    stacked = stacked.reshape(outer, -1, LANE)
    stacked = lax.psum_scatter(stacked, "outer", scatter_dimension=0, tiled=True)
    stacked = stacked.reshape(shard_count, -1, LANE)
    stacked = lax.psum_scatter(stacked, "shard", scatter_dimension=0, tiled=True)
    stacked = stacked.reshape(stacked.shape[1:])
    stacked = lax.all_gather(stacked, "outer", axis=0, tiled=True)
    stacked = lax.all_gather(stacked, "core", axis=0, tiled=True)
    stacked = stacked.reshape(blocks, -1, LANE).astype(jnp.float32)
    totals = []
    offset = 0
    for width, half_size, half_shape in zip(widths, sizes, shapes):
        totals.append(unpack_half(stacked[:, offset : offset + width], half_size, half_shape))
        offset += width
    return totals


def norm_stats(field_in):
    centred = field_in - jnp.mean(field_in, axis=-1, keepdims=True)
    inverse = lax.rsqrt(jnp.mean(centred * centred, axis=-1, keepdims=True) + EPS)
    return (centred * inverse, inverse)


def norm_back(grad_hat, normed, inverse):
    first_mean = jnp.mean(grad_hat, axis=-1, keepdims=True)
    second_mean = jnp.mean(grad_hat * normed, axis=-1, keepdims=True)
    return inverse * (grad_hat - first_mean - normed * second_mean)


def contract_rows(left_side, right_side):
    return lax.dot_general(
        left_side, right_side, (((0,), (0,)), ((), ())), preferred_element_type=jnp.float32
    )


def contract_cols(left_side, right_side):
    return lax.dot_general(
        left_side, right_side, (((1,), (1,)), ((), ())), preferred_element_type=jnp.float32
    )


def split_heads(field_in):
    return field_in.reshape(field_in.shape[0], HEADS, -1).transpose(1, 0, 2)


def merge_heads(field_in):
    return field_in.transpose(1, 0, 2).reshape(field_in.shape[1], -1)


def gelu_tanh(field_in):
    return jax.nn.gelu(field_in, approximate=True)


def gelu_back(pre_act, grad_act):
    _, pull_back = jax.vjp(gelu_tanh, pre_act)
    return pull_back(grad_act)[0]


def head_scores(queries, key_block, slope, allowed, distance, score_scale):
    raw = contract_cols(queries, key_block) * score_scale - slope * distance
    return jnp.where(allowed, raw, NEG_FILL)


def nesterov(grad_total, weight_old, moment_old, average_old, rate):
    moment_new = MOMENTUM * moment_old + grad_total
    weight_new = weight_old - rate * (grad_total + MOMENTUM * moment_new)
    average_new = AVERAGING * average_old + (1.0 - AVERAGING) * weight_new
    return (weight_new, moment_new, average_new)


def body(
    tokens,
    cotangent,
    lengths,
    qkv_weight,
    qkv_momentum,
    qkv_average,
    out_weight,
    out_momentum,
    out_average,
    up_weight,
    up_momentum,
    up_average,
    down_weight,
    down_momentum,
    down_average,
    small_params,
    small_momentum,
    small_average,
):
    tok_rows = tokens.shape[0]
    model_width = tokens.shape[1]
    shard_count = lax.axis_size("shard")
    group_count = lax.axis_size("outer") * lax.axis_size("core")
    shard_place = lax.axis_index("shard")
    group_place = lax.axis_index("outer") * lax.axis_size("core") + lax.axis_index("core")
    upper_half = shard_place % 2
    seq_place = group_place * (shard_count // 2) + shard_place // 2
    seq_length = lax.dynamic_index_in_dim(lengths, seq_place, 0, keepdims=False)
    local_pos = jnp.arange(tok_rows, dtype=jnp.int32)
    query_pos = upper_half * tok_rows + local_pos
    key_pos = jnp.concatenate([local_pos, query_pos])
    prev_live = jnp.full((tok_rows,), upper_half == 1)
    key_live = jnp.concatenate([prev_live, jnp.ones((tok_rows,), bool)]) & (key_pos < seq_length)
    allowed = key_live[None, :] & (key_pos[None, :] <= query_pos[:, None])
    distance = (query_pos[:, None] - key_pos[None, :]).astype(jnp.float32)
    row_live = (query_pos < seq_length).astype(jnp.float32)[:, None]
    head_size = model_width // HEADS
    score_scale = head_size ** (-0.5)
    slopes = 2.0 ** (-8.0 * (jnp.arange(HEADS, dtype=jnp.float32) + 1.0) / HEADS)
    qkv_full, small_full = gather_weights([(qkv_weight, 0), (small_params, 1)])
    out_full, up_full, down_full = gather_weights(
        [(out_weight, 0), (up_weight, 1), (down_weight, 0)]
    )
    table = small_full.astype(jnp.float32)
    up_bias = table[8:12].reshape(FF)
    normed_one, inverse_one = norm_stats(tokens)
    entry_low = (normed_one * table[0] + table[1]).astype(jnp.bfloat16)
    mapped = jnp.dot(entry_low, qkv_full, preferred_element_type=jnp.float32)
    queries = (mapped[:, :model_width] + table[2]).astype(jnp.bfloat16)
    key_own = mapped[:, model_width : 2 * model_width].astype(jnp.bfloat16)
    value_own = (mapped[:, 2 * model_width :] + table[3]).astype(jnp.bfloat16)
    received = passed_along(jnp.concatenate([key_own, value_own], 1), "shard", 1)
    key_all = jnp.concatenate([received[:, :model_width], key_own], 0)
    value_all = jnp.concatenate([received[:, model_width:], value_own], 0)
    query_heads = split_heads(queries)
    key_heads = split_heads(key_all)
    value_heads = split_heads(value_all)

    def head_forward(head_item):
        head_query, head_keys, head_values, slope = head_item
        scores = head_scores(head_query, head_keys, slope, allowed, distance, score_scale)
        row_top = jnp.max(scores, axis=-1, keepdims=True)
        weights = jnp.exp(scores - row_top)
        row_total = jnp.sum(weights, axis=-1, keepdims=True)
        probs_low = (weights / row_total).astype(jnp.bfloat16)
        mixture = jnp.dot(probs_low, head_values, preferred_element_type=jnp.float32)
        return (mixture, (row_top + jnp.log(row_total))[:, 0])

    mixture_heads, log_total = lax.map(head_forward, (query_heads, key_heads, value_heads, slopes))
    attended_low = merge_heads(mixture_heads).astype(jnp.bfloat16)
    resid_one = (
        tokens + jnp.dot(attended_low, out_full, preferred_element_type=jnp.float32) + table[4]
    )
    normed_two, inverse_two = norm_stats(resid_one)
    inner_low = (normed_two * table[5] + table[6]).astype(jnp.bfloat16)
    grad_out = cotangent * row_live
    down_bias_grad = jnp.sum(grad_out, axis=0)
    grad_low = grad_out.astype(jnp.bfloat16)
    pre_act = jnp.dot(inner_low, up_full, preferred_element_type=jnp.float32) + up_bias
    act_low = gelu_tanh(pre_act).astype(jnp.bfloat16)
    branch_out = jnp.dot(act_low, down_full, preferred_element_type=jnp.float32)
    block_out = resid_one + branch_out + table[7]
    grad_act = contract_cols(grad_low, down_full)
    down_grad = contract_rows(act_low, grad_low)
    grad_pre = gelu_back(pre_act, grad_act)
    up_bias_grad = jnp.sum(grad_pre, axis=0)
    pre_low = grad_pre.astype(jnp.bfloat16)
    up_grad = contract_rows(inner_low, pre_low)
    grad_inner = contract_cols(pre_low, up_full)
    gain_two_grad = jnp.sum(grad_inner * normed_two, axis=0)
    shift_two_grad = jnp.sum(grad_inner, axis=0)
    grad_resid = grad_out + norm_back(grad_inner * table[5], normed_two, inverse_two)
    resid_low = grad_resid.astype(jnp.bfloat16)
    out_grad = contract_rows(attended_low, resid_low)
    grad_resid, resid_low, up_grad, down_grad, out_grad = lax.optimization_barrier(
        (grad_resid, resid_low, up_grad, down_grad, out_grad)
    )
    up_total, down_total, out_total = reduce_grads([(up_grad, 1), (down_grad, 0), (out_grad, 0)])
    out_bias_grad = jnp.sum(grad_resid, axis=0)
    grad_mixture = contract_cols(resid_low, out_full).astype(jnp.bfloat16)
    grad_heads = split_heads(grad_mixture)

    def head_backward(head_item):
        head_query, head_keys, head_values, head_grad, head_lse, slope = head_item
        scores = head_scores(head_query, head_keys, slope, allowed, distance, score_scale)
        probs = jnp.exp(scores - head_lse[:, None])
        probs_low = probs.astype(jnp.bfloat16)
        grad_values = contract_rows(probs_low, head_grad)
        grad_probs = contract_cols(head_grad, head_values)
        row_delta = jnp.sum(probs * grad_probs, axis=-1, keepdims=True)
        grad_scores = (probs * (grad_probs - row_delta)).astype(jnp.bfloat16)
        grad_query = (
            jnp.dot(grad_scores, head_keys, preferred_element_type=jnp.float32) * score_scale
        )
        grad_keys = contract_rows(grad_scores, head_query) * score_scale
        return (grad_query, grad_keys, grad_values)

    groups = 4
    per_group = HEADS // groups
    parts = []
    for group in range(groups):
        chosen = slice(group * per_group, (group + 1) * per_group)
        parts.append(
            lax.map(
                head_backward,
                (
                    query_heads[chosen],
                    key_heads[chosen],
                    value_heads[chosen],
                    grad_heads[chosen],
                    log_total[chosen],
                    slopes[chosen],
                ),
            )
        )
    query_grads, key_grads, value_grads = (
        jnp.concatenate([part[index] for part in parts], 0) for index in range(3)
    )
    grad_query = merge_heads(query_grads)
    grad_keys = merge_heads(key_grads)
    grad_values = merge_heads(value_grads)
    returned = passed_along(
        jnp.concatenate([grad_keys[:tok_rows], grad_values[:tok_rows]], 1).astype(jnp.bfloat16),
        "shard",
        -1,
    ).astype(jnp.float32)
    grad_key_own = grad_keys[tok_rows:] + returned[:, :model_width]
    grad_value_own = grad_values[tok_rows:] + returned[:, model_width:]
    query_bias_grad = jnp.sum(grad_query, axis=0)
    value_bias_grad = jnp.sum(grad_value_own, axis=0)
    mapped_low = jnp.concatenate([grad_query, grad_key_own, grad_value_own], 1).astype(jnp.bfloat16)
    qkv_grad = contract_rows(entry_low, mapped_low)
    grad_entry = contract_cols(mapped_low, qkv_full)
    gain_one_grad = jnp.sum(grad_entry * normed_one, axis=0)
    shift_one_grad = jnp.sum(grad_entry, axis=0)
    input_grad = grad_resid + norm_back(grad_entry * table[0], normed_one, inverse_one)
    head_rows = jnp.stack(
        [
            gain_one_grad,
            shift_one_grad,
            query_bias_grad,
            value_bias_grad,
            out_bias_grad,
            gain_two_grad,
            shift_two_grad,
            down_bias_grad,
        ]
    )
    small_grad = jnp.concatenate([head_rows, up_bias_grad.reshape(4, model_width)], 0)
    qkv_total, small_total = reduce_grads([(qkv_grad, 0), (small_grad, 1)])
    rate = 2.0 / math.sqrt(model_width * tok_rows * shard_count * group_count)
    qkv_new = nesterov(qkv_total, qkv_weight, qkv_momentum, qkv_average, rate)
    out_new = nesterov(out_total, out_weight, out_momentum, out_average, rate)
    up_new = nesterov(up_total, up_weight, up_momentum, up_average, rate)
    down_new = nesterov(down_total, down_weight, down_momentum, down_average, rate)
    small_new = nesterov(small_total, small_params, small_momentum, small_average, rate)
    return (
        block_out,
        input_grad,
        qkv_new[0],
        qkv_new[1],
        qkv_new[2],
        out_new[0],
        out_new[1],
        out_new[2],
        up_new[0],
        up_new[1],
        up_new[2],
        down_new[0],
        down_new[1],
        down_new[2],
        small_new[0],
        small_new[1],
        small_new[2],
    )


def solution(mesh):
    cores = 2
    devices = mesh.devices.reshape(mesh.shape["group"] // cores, cores, mesh.shape["shard"])
    inner_mesh = jax.sharding.Mesh(devices, ("outer", "core", "shard"))
    rows = P(("outer", "core", "shard"), None)
    in_specs = (
        rows,
        rows,
        P(),
        P("shard", None),
        P("shard", None),
        P("shard", None),
        P("shard", None),
        P("shard", None),
        P("shard", None),
        P(None, "shard"),
        P(None, "shard"),
        P(None, "shard"),
        P("shard", None),
        P("shard", None),
        P("shard", None),
        P(None, "shard"),
        P(None, "shard"),
        P(None, "shard"),
    )
    out_specs = (
        rows,
        rows,
        P("shard", None),
        P("shard", None),
        P("shard", None),
        P("shard", None),
        P("shard", None),
        P("shard", None),
        P(None, "shard"),
        P(None, "shard"),
        P(None, "shard"),
        P("shard", None),
        P("shard", None),
        P("shard", None),
        P(None, "shard"),
        P(None, "shard"),
        P(None, "shard"),
    )

    return jax.shard_map(body, mesh=inner_mesh, in_specs=in_specs, out_specs=out_specs, check_vma=False)
```

```python
import math

import jax
import jax.numpy as jnp
from jax import lax
from jax.sharding import PartitionSpec as P


HEADS = 16
FF = 4096


EPS = 1e-05
MOMENTUM = 0.9
AVERAGING = 0.9
NEG_FILL = -1e30


def passed_along(value, axis, steps):
    count = lax.axis_size(axis)
    leading, last = (max(0, -steps), min(count, count - steps))
    return lax.ppermute(value, axis, [(source, source + steps) for source in range(leading, last)])


LANE = 1024


def to_blocks(half, blocks):
    flat = half.reshape(-1)
    size = flat.shape[0]
    padded = -(-size // (blocks * LANE)) * blocks * LANE
    if padded != size:
        flat = jnp.pad(flat, (0, padded - size))
    return flat.reshape(blocks, -1, LANE)


def gather_weights(halves):
    cores = lax.axis_size("core")
    outer = lax.axis_size("outer")
    blocks = cores * outer
    lows = [half.astype(jnp.bfloat16) for half, unused in halves]
    packed = [to_blocks(low, blocks) for low in lows]
    widths = [piece.shape[1] for piece in packed]
    own = jnp.concatenate(packed, axis=1)
    place = lax.axis_index("core") * outer + lax.axis_index("outer")
    mine = lax.dynamic_index_in_dim(own, place, 0, keepdims=False)
    other = lax.ppermute(mine, "shard", [(0, 1), (1, 0)])
    got = lax.all_gather(other, "outer", axis=0, tiled=False)
    got = lax.all_gather(got, "core", axis=0, tiled=False)
    got = got.reshape(blocks, -1, LANE)
    upper = lax.axis_index("shard") == 1
    fulls = []
    offset = 0
    for (half, dim), low, width in zip(halves, lows, widths):
        other_half = got[:, offset : offset + width].reshape(-1)[: low.size].reshape(low.shape)
        offset += width
        in_order = jnp.concatenate([low, other_half], axis=dim)
        swapped = jnp.concatenate([other_half, low], axis=dim)
        fulls.append(jnp.where(upper, swapped, in_order))
    return fulls


def pack_halves(grad_full, dim, blocks):
    shard_count = lax.axis_size("shard")
    rows, cols = grad_full.shape
    if dim == 0:
        halves = grad_full.reshape(shard_count, -1)
    else:
        halves = grad_full.reshape(rows, shard_count, cols // shard_count).transpose(1, 0, 2)
        halves = halves.reshape(shard_count, -1)
    half_size = halves.shape[1]
    padded = -(-half_size // (blocks * LANE)) * blocks * LANE
    if padded != half_size:
        halves = jnp.pad(halves, ((0, 0), (0, padded - half_size)))
    return halves.reshape(shard_count, blocks, -1, LANE), half_size


def unpack_half(packed, half_size, half_shape):
    return packed.reshape(-1)[:half_size].reshape(half_shape)


def reduce_grads(grads):
    shard_count = lax.axis_size("shard")
    cores = lax.axis_size("core")
    outer = lax.axis_size("outer")
    blocks = cores * outer
    packed, sizes, shapes = [], [], []
    for grad_full, dim in grads:
        piece, half_size = pack_halves(grad_full, dim, blocks)
        packed.append(piece)
        sizes.append(half_size)
        rows, cols = grad_full.shape
        shapes.append((rows // shard_count, cols) if dim == 0 else (rows, cols // shard_count))
    widths = [piece.shape[2] for piece in packed]
    return reduce_packed(packed, widths, sizes, shapes)


def reduce_packed(packed, widths, sizes, shapes):
    shard_count = lax.axis_size("shard")
    cores = lax.axis_size("core")
    outer = lax.axis_size("outer")
    blocks = cores * outer
    stacked = jnp.concatenate(packed, axis=2).astype(jnp.bfloat16)
    stacked = stacked.reshape(shard_count, cores, outer, -1, LANE).transpose(1, 2, 0, 3, 4)
    stacked = stacked.reshape(cores, -1, LANE)
    stacked = lax.psum_scatter(stacked, "core", scatter_dimension=0, tiled=True)
    stacked = stacked.reshape(outer, -1, LANE)
    stacked = lax.psum_scatter(stacked, "outer", scatter_dimension=0, tiled=True)
    stacked = stacked.reshape(shard_count, -1, LANE)
    stacked = lax.psum_scatter(stacked, "shard", scatter_dimension=0, tiled=True)
    stacked = stacked.reshape(stacked.shape[1:])
    stacked = lax.all_gather(stacked, "outer", axis=0, tiled=True)
    stacked = lax.all_gather(stacked, "core", axis=0, tiled=True)
    stacked = stacked.reshape(blocks, -1, LANE).astype(jnp.float32)
    totals = []
    offset = 0
    for width, half_size, half_shape in zip(widths, sizes, shapes):
        totals.append(unpack_half(stacked[:, offset : offset + width], half_size, half_shape))
        offset += width
    return totals


def norm_stats(field_in):
    centred = field_in - jnp.mean(field_in, axis=-1, keepdims=True)
    inverse = lax.rsqrt(jnp.mean(centred * centred, axis=-1, keepdims=True) + EPS)
    return (centred * inverse, inverse)


def norm_back(grad_hat, normed, inverse):
    first_mean = jnp.mean(grad_hat, axis=-1, keepdims=True)
    second_mean = jnp.mean(grad_hat * normed, axis=-1, keepdims=True)
    return inverse * (grad_hat - first_mean - normed * second_mean)


def contract_rows(left_side, right_side):
    return lax.dot_general(
        left_side, right_side, (((0,), (0,)), ((), ())), preferred_element_type=jnp.float32
    )


def contract_cols(left_side, right_side):
    return lax.dot_general(
        left_side, right_side, (((1,), (1,)), ((), ())), preferred_element_type=jnp.float32
    )


def split_heads(field_in):
    return field_in.reshape(field_in.shape[0], HEADS, -1).transpose(1, 0, 2)


def split_heads_n(field_in, heads):
    return field_in.reshape(field_in.shape[0], heads, -1).transpose(1, 0, 2)


def merge_heads(field_in):
    return field_in.transpose(1, 0, 2).reshape(field_in.shape[1], -1)


def gelu_tanh(field_in):
    return jax.nn.gelu(field_in, approximate=True)


def gelu_back(pre_act, grad_act):
    _, pull_back = jax.vjp(gelu_tanh, pre_act)
    return pull_back(grad_act)[0]


def head_scores(queries, key_block, slope, allowed, distance, score_scale):
    raw = contract_cols(queries, key_block) * score_scale - slope * distance
    return jnp.where(allowed, raw, NEG_FILL)


def nesterov(grad_total, weight_old, moment_old, average_old, rate):
    moment_new = MOMENTUM * moment_old + grad_total
    weight_new = weight_old - rate * (grad_total + MOMENTUM * moment_new)
    average_new = AVERAGING * average_old + (1.0 - AVERAGING) * weight_new
    return (weight_new, moment_new, average_new)


def body(
    tokens,
    cotangent,
    lengths,
    qkv_weight,
    qkv_momentum,
    qkv_average,
    out_weight,
    out_momentum,
    out_average,
    up_weight,
    up_momentum,
    up_average,
    down_weight,
    down_momentum,
    down_average,
    small_params,
    small_momentum,
    small_average,
):
    tok_rows = tokens.shape[0]
    model_width = tokens.shape[1]
    shard_count = lax.axis_size("shard")
    group_count = lax.axis_size("outer") * lax.axis_size("core")
    shard_place = lax.axis_index("shard")
    group_place = lax.axis_index("outer") * lax.axis_size("core") + lax.axis_index("core")
    upper_half = shard_place % 2
    seq_place = group_place * (shard_count // 2) + shard_place // 2
    seq_length = lax.dynamic_index_in_dim(lengths, seq_place, 0, keepdims=False)
    local_pos = jnp.arange(tok_rows, dtype=jnp.int32)
    query_pos = upper_half * tok_rows + local_pos
    key_pos = jnp.concatenate([local_pos, query_pos])
    prev_live = jnp.full((tok_rows,), upper_half == 1)
    key_live = jnp.concatenate([prev_live, jnp.ones((tok_rows,), bool)]) & (key_pos < seq_length)
    allowed = key_live[None, :] & (key_pos[None, :] <= query_pos[:, None])
    distance = (query_pos[:, None] - key_pos[None, :]).astype(jnp.float32)
    row_live = (query_pos < seq_length).astype(jnp.float32)[:, None]
    head_size = model_width // HEADS
    score_scale = head_size ** (-0.5)
    slopes = 2.0 ** (-8.0 * (jnp.arange(HEADS, dtype=jnp.float32) + 1.0) / HEADS)
    qkv_full, small_full = gather_weights([(qkv_weight, 0), (small_params, 1)])
    out_full, up_full, down_full = gather_weights(
        [(out_weight, 0), (up_weight, 1), (down_weight, 0)]
    )
    table = small_full.astype(jnp.float32)
    up_bias = table[8:12].reshape(FF)
    normed_one, inverse_one = norm_stats(tokens)
    entry_low = (normed_one * table[0] + table[1]).astype(jnp.bfloat16)
    mapped = jnp.dot(entry_low, qkv_full, preferred_element_type=jnp.float32)
    queries = (mapped[:, :model_width] + table[2]).astype(jnp.bfloat16)
    key_own = mapped[:, model_width : 2 * model_width].astype(jnp.bfloat16)
    value_own = (mapped[:, 2 * model_width :] + table[3]).astype(jnp.bfloat16)
    groups = 4
    per_group = HEADS // groups
    group_width = per_group * (model_width // HEADS)
    query_groups, key_groups, value_groups = [], [], []
    for group in range(groups):
        cols = slice(group * group_width, (group + 1) * group_width)
        received = passed_along(
            jnp.concatenate([key_own[:, cols], value_own[:, cols]], 1), "shard", 1
        )
        query_groups.append(split_heads_n(queries[:, cols], per_group))
        key_groups.append(
            split_heads_n(jnp.concatenate([received[:, :group_width], key_own[:, cols]], 0), per_group)
        )
        value_groups.append(
            split_heads_n(jnp.concatenate([received[:, group_width:], value_own[:, cols]], 0), per_group)
        )

    def head_forward(head_item):
        head_query, head_keys, head_values, slope = head_item
        scores = head_scores(head_query, head_keys, slope, allowed, distance, score_scale)
        row_top = jnp.max(scores, axis=-1, keepdims=True)
        weights = jnp.exp(scores - row_top)
        row_total = jnp.sum(weights, axis=-1, keepdims=True)
        probs_low = (weights / row_total).astype(jnp.bfloat16)
        mixture = jnp.dot(probs_low, head_values, preferred_element_type=jnp.float32)
        return (mixture, (row_top + jnp.log(row_total))[:, 0])

    fwd_parts = []
    for group in range(groups):
        chosen = slice(group * per_group, (group + 1) * per_group)
        fwd_parts.append(
            lax.map(
                head_forward,
                (query_groups[group], key_groups[group], value_groups[group], slopes[chosen]),
            )
        )
    mixture_heads = jnp.concatenate([part[0] for part in fwd_parts], 0)
    log_total = jnp.concatenate([part[1] for part in fwd_parts], 0)
    attended_low = merge_heads(mixture_heads).astype(jnp.bfloat16)
    resid_one = (
        tokens + jnp.dot(attended_low, out_full, preferred_element_type=jnp.float32) + table[4]
    )
    normed_two, inverse_two = norm_stats(resid_one)
    inner_low = (normed_two * table[5] + table[6]).astype(jnp.bfloat16)
    grad_out = cotangent * row_live
    down_bias_grad = jnp.sum(grad_out, axis=0)
    grad_low = grad_out.astype(jnp.bfloat16)
    pre_act = jnp.dot(inner_low, up_full, preferred_element_type=jnp.float32) + up_bias
    act_low = gelu_tanh(pre_act).astype(jnp.bfloat16)
    branch_out = jnp.dot(act_low, down_full, preferred_element_type=jnp.float32)
    block_out = resid_one + branch_out + table[7]
    grad_act = contract_cols(grad_low, down_full)
    down_grad = contract_rows(act_low, grad_low)
    grad_pre = gelu_back(pre_act, grad_act)
    up_bias_grad = jnp.sum(grad_pre, axis=0)
    pre_low = grad_pre.astype(jnp.bfloat16)
    up_grad = contract_rows(inner_low, pre_low)
    grad_inner = contract_cols(pre_low, up_full)
    gain_two_grad = jnp.sum(grad_inner * normed_two, axis=0)
    shift_two_grad = jnp.sum(grad_inner, axis=0)
    grad_resid = grad_out + norm_back(grad_inner * table[5], normed_two, inverse_two)
    resid_low = grad_resid.astype(jnp.bfloat16)
    out_grad = contract_rows(attended_low, resid_low)
    grad_resid, resid_low, up_grad, down_grad, out_grad = lax.optimization_barrier(
        (grad_resid, resid_low, up_grad, down_grad, out_grad)
    )
    up_total, down_total, out_total = reduce_grads([(up_grad, 1), (down_grad, 0), (out_grad, 0)])
    out_bias_grad = jnp.sum(grad_resid, axis=0)
    grad_mixture = contract_cols(resid_low, out_full).astype(jnp.bfloat16)
    grad_heads = split_heads(grad_mixture)

    def head_backward(head_item):
        head_query, head_keys, head_values, head_grad, head_lse, slope = head_item
        scores = head_scores(head_query, head_keys, slope, allowed, distance, score_scale)
        probs = jnp.exp(scores - head_lse[:, None])
        probs_low = probs.astype(jnp.bfloat16)
        grad_values = contract_rows(probs_low, head_grad)
        grad_probs = contract_cols(head_grad, head_values)
        row_delta = jnp.sum(probs * grad_probs, axis=-1, keepdims=True)
        grad_scores = (probs * (grad_probs - row_delta)).astype(jnp.bfloat16)
        grad_query = (
            jnp.dot(grad_scores, head_keys, preferred_element_type=jnp.float32) * score_scale
        )
        grad_keys = contract_rows(grad_scores, head_query) * score_scale
        return (grad_query, grad_keys, grad_values)

    query_parts, key_parts, value_parts = [], [], []
    for group in range(groups):
        chosen = slice(group * per_group, (group + 1) * per_group)
        group_query, group_keys, group_values = lax.map(
            head_backward,
            (
                query_groups[group],
                key_groups[group],
                value_groups[group],
                grad_heads[chosen],
                log_total[chosen],
                slopes[chosen],
            ),
        )
        returned = passed_along(
            jnp.concatenate(
                [merge_heads(group_keys[:, :tok_rows]), merge_heads(group_values[:, :tok_rows])], 1
            ).astype(jnp.bfloat16),
            "shard",
            -1,
        ).astype(jnp.float32)
        query_parts.append(merge_heads(group_query))
        key_parts.append(merge_heads(group_keys[:, tok_rows:]) + returned[:, :group_width])
        value_parts.append(merge_heads(group_values[:, tok_rows:]) + returned[:, group_width:])
    grad_query = jnp.concatenate(query_parts, 1)
    grad_key_own = jnp.concatenate(key_parts, 1)
    grad_value_own = jnp.concatenate(value_parts, 1)
    query_bias_grad = jnp.sum(grad_query, axis=0)
    value_bias_grad = jnp.sum(grad_value_own, axis=0)
    mapped_low = jnp.concatenate([grad_query, grad_key_own, grad_value_own], 1).astype(jnp.bfloat16)
    qkv_grad = contract_rows(entry_low, mapped_low)
    grad_entry = contract_cols(mapped_low, qkv_full)
    gain_one_grad = jnp.sum(grad_entry * normed_one, axis=0)
    shift_one_grad = jnp.sum(grad_entry, axis=0)
    input_grad = grad_resid + norm_back(grad_entry * table[0], normed_one, inverse_one)
    head_rows = jnp.stack(
        [
            gain_one_grad,
            shift_one_grad,
            query_bias_grad,
            value_bias_grad,
            out_bias_grad,
            gain_two_grad,
            shift_two_grad,
            down_bias_grad,
        ]
    )
    small_grad = jnp.concatenate([head_rows, up_bias_grad.reshape(4, model_width)], 0)
    qkv_total, small_total = reduce_grads([(qkv_grad, 0), (small_grad, 1)])
    rate = 2.0 / math.sqrt(model_width * tok_rows * shard_count * group_count)
    qkv_new = nesterov(qkv_total, qkv_weight, qkv_momentum, qkv_average, rate)
    out_new = nesterov(out_total, out_weight, out_momentum, out_average, rate)
    up_new = nesterov(up_total, up_weight, up_momentum, up_average, rate)
    down_new = nesterov(down_total, down_weight, down_momentum, down_average, rate)
    small_new = nesterov(small_total, small_params, small_momentum, small_average, rate)
    return (
        block_out,
        input_grad,
        qkv_new[0],
        qkv_new[1],
        qkv_new[2],
        out_new[0],
        out_new[1],
        out_new[2],
        up_new[0],
        up_new[1],
        up_new[2],
        down_new[0],
        down_new[1],
        down_new[2],
        small_new[0],
        small_new[1],
        small_new[2],
    )


def solution(mesh):
    cores = 2
    devices = mesh.devices.reshape(mesh.shape["group"] // cores, cores, mesh.shape["shard"])
    inner_mesh = jax.sharding.Mesh(devices, ("outer", "core", "shard"))
    rows = P(("outer", "core", "shard"), None)
    in_specs = (
        rows,
        rows,
        P(),
        P("shard", None),
        P("shard", None),
        P("shard", None),
        P("shard", None),
        P("shard", None),
        P("shard", None),
        P(None, "shard"),
        P(None, "shard"),
        P(None, "shard"),
        P("shard", None),
        P("shard", None),
        P("shard", None),
        P(None, "shard"),
        P(None, "shard"),
        P(None, "shard"),
    )
    out_specs = (
        rows,
        rows,
        P("shard", None),
        P("shard", None),
        P("shard", None),
        P("shard", None),
        P("shard", None),
        P("shard", None),
        P(None, "shard"),
        P(None, "shard"),
        P(None, "shard"),
        P("shard", None),
        P("shard", None),
        P("shard", None),
        P(None, "shard"),
        P(None, "shard"),
        P(None, "shard"),
    )

    return jax.shard_map(body, mesh=inner_mesh, in_specs=in_specs, out_specs=out_specs, check_vma=False)
```

```python
import math

import jax
import jax.numpy as jnp
from jax import lax
from jax.sharding import PartitionSpec as P


HEADS = 16
FF = 4096


EPS = 1e-05
MOMENTUM = 0.9
AVERAGING = 0.9
NEG_FILL = -1e30


def passed_along(value, axis, steps):
    count = lax.axis_size(axis)
    leading, last = (max(0, -steps), min(count, count - steps))
    return lax.ppermute(value, axis, [(source, source + steps) for source in range(leading, last)])


SMALL_WIDTH = 3072


def small_rows(small_half, blocks):
    flat = small_half.reshape(-1)
    padded = blocks * SMALL_WIDTH
    return jnp.pad(flat, (0, padded - flat.shape[0])).reshape(blocks, 1, SMALL_WIDTH)


def gather_rows(row_arrays):
    cores = lax.axis_size("core")
    outer = lax.axis_size("outer")
    blocks = cores * outer
    place = lax.axis_index("core") * outer + lax.axis_index("outer")
    heights = [piece.shape[1] for piece in row_arrays]
    mine = jnp.concatenate(
        [lax.dynamic_index_in_dim(piece, place, 0, keepdims=False) for piece in row_arrays], 0
    )
    other = lax.ppermute(mine, "shard", [(0, 1), (1, 0)])
    got = lax.all_gather(other, "outer", axis=0, tiled=False)
    got = lax.all_gather(got, "core", axis=0, tiled=False)
    got = got.reshape(blocks, -1, got.shape[-1])
    pieces = []
    offset = 0
    for height in heights:
        pieces.append(got[:, offset : offset + height])
        offset += height
    return pieces


def join_halves(own, other, dim):
    upper = lax.axis_index("shard") == 1
    in_order = jnp.concatenate([own, other], axis=dim)
    swapped = jnp.concatenate([other, own], axis=dim)
    return jnp.where(upper, swapped, in_order)


def reduce_rows(row_grads):
    shard_count = lax.axis_size("shard")
    cores = lax.axis_size("core")
    outer = lax.axis_size("outer")
    blocks = cores * outer
    heights = [piece.shape[3] for piece in row_grads]
    width = row_grads[0].shape[-1]
    stacked = jnp.concatenate(
        [piece.astype(jnp.bfloat16).transpose(1, 2, 0, 3, 4) for piece in row_grads], 3
    )
    stacked = stacked.reshape(cores, -1, width)
    stacked = lax.psum_scatter(stacked, "core", scatter_dimension=0, tiled=True)
    stacked = stacked.reshape(outer, -1, width)
    stacked = lax.psum_scatter(stacked, "outer", scatter_dimension=0, tiled=True)
    stacked = stacked.reshape(shard_count, -1, width)
    stacked = lax.psum_scatter(stacked, "shard", scatter_dimension=0, tiled=True)
    stacked = stacked.reshape(stacked.shape[1:])
    stacked = lax.all_gather(stacked, "outer", axis=0, tiled=True)
    stacked = lax.all_gather(stacked, "core", axis=0, tiled=True)
    stacked = stacked.reshape(blocks, -1, width)
    pieces = []
    offset = 0
    for height in heights:
        pieces.append(stacked[:, offset : offset + height].astype(jnp.float32))
        offset += height
    return pieces


def split_rows(grad_full):
    shard_count = lax.axis_size("shard")
    cores = lax.axis_size("core")
    outer = lax.axis_size("outer")
    rows, cols = grad_full.shape
    return grad_full.reshape(shard_count, cores, outer, rows // (shard_count * cores * outer), cols)


def norm_stats(field_in):
    centred = field_in - jnp.mean(field_in, axis=-1, keepdims=True)
    inverse = lax.rsqrt(jnp.mean(centred * centred, axis=-1, keepdims=True) + EPS)
    return (centred * inverse, inverse)


def norm_back(grad_hat, normed, inverse):
    first_mean = jnp.mean(grad_hat, axis=-1, keepdims=True)
    second_mean = jnp.mean(grad_hat * normed, axis=-1, keepdims=True)
    return inverse * (grad_hat - first_mean - normed * second_mean)


def contract_rows(left_side, right_side):
    return lax.dot_general(
        left_side, right_side, (((0,), (0,)), ((), ())), preferred_element_type=jnp.float32
    )


def contract_cols(left_side, right_side):
    return lax.dot_general(
        left_side, right_side, (((1,), (1,)), ((), ())), preferred_element_type=jnp.float32
    )


def split_heads(field_in):
    return field_in.reshape(field_in.shape[0], HEADS, -1).transpose(1, 0, 2)


def split_heads_n(field_in, heads):
    return field_in.reshape(field_in.shape[0], heads, -1).transpose(1, 0, 2)


def merge_heads(field_in):
    return field_in.transpose(1, 0, 2).reshape(field_in.shape[1], -1)


def gelu_tanh(field_in):
    return jax.nn.gelu(field_in, approximate=True)


def gelu_back(pre_act, grad_act):
    _, pull_back = jax.vjp(gelu_tanh, pre_act)
    return pull_back(grad_act)[0]


def head_scores(queries, key_block, slope, allowed, distance, score_scale):
    raw = contract_cols(queries, key_block) * score_scale - slope * distance
    return jnp.where(allowed, raw, NEG_FILL)


def nesterov(grad_total, weight_old, moment_old, average_old, rate):
    moment_new = MOMENTUM * moment_old + grad_total
    weight_new = weight_old - rate * (grad_total + MOMENTUM * moment_new)
    average_new = AVERAGING * average_old + (1.0 - AVERAGING) * weight_new
    return (weight_new, moment_new, average_new)


def body(
    tokens,
    cotangent,
    lengths,
    qkv_weight,
    qkv_momentum,
    qkv_average,
    out_weight,
    out_momentum,
    out_average,
    up_weight,
    up_momentum,
    up_average,
    down_weight,
    down_momentum,
    down_average,
    small_params,
    small_momentum,
    small_average,
):
    tok_rows = tokens.shape[0]
    model_width = tokens.shape[1]
    shard_count = lax.axis_size("shard")
    group_count = lax.axis_size("outer") * lax.axis_size("core")
    shard_place = lax.axis_index("shard")
    group_place = lax.axis_index("outer") * lax.axis_size("core") + lax.axis_index("core")
    upper_half = shard_place % 2
    seq_place = group_place * (shard_count // 2) + shard_place // 2
    seq_length = lax.dynamic_index_in_dim(lengths, seq_place, 0, keepdims=False)
    local_pos = jnp.arange(tok_rows, dtype=jnp.int32)
    query_pos = upper_half * tok_rows + local_pos
    key_pos = jnp.concatenate([local_pos, query_pos])
    prev_live = jnp.full((tok_rows,), upper_half == 1)
    key_live = jnp.concatenate([prev_live, jnp.ones((tok_rows,), bool)]) & (key_pos < seq_length)
    allowed = key_live[None, :] & (key_pos[None, :] <= query_pos[:, None])
    distance = (query_pos[:, None] - key_pos[None, :]).astype(jnp.float32)
    row_live = (query_pos < seq_length).astype(jnp.float32)[:, None]
    head_size = model_width // HEADS
    score_scale = head_size ** (-0.5)
    slopes = 2.0 ** (-8.0 * (jnp.arange(HEADS, dtype=jnp.float32) + 1.0) / HEADS)
    blocks = lax.axis_size("core") * lax.axis_size("outer")
    qkv_own = qkv_weight.astype(jnp.bfloat16)
    small_own = small_params.astype(jnp.bfloat16)
    qkv_other, small_other = gather_rows(
        [qkv_own.reshape(blocks, -1, qkv_own.shape[1]), small_rows(small_own, blocks)]
    )
    qkv_full = join_halves(qkv_own, qkv_other.reshape(qkv_own.shape), 0)
    small_full = join_halves(
        small_own, small_other.reshape(-1)[: small_own.size].reshape(small_own.shape), 1
    )
    out_own = out_weight.astype(jnp.bfloat16)
    up_own_t = up_weight.astype(jnp.bfloat16).T
    down_own = down_weight.astype(jnp.bfloat16)
    out_other, up_other_t, down_other = gather_rows(
        [piece.reshape(blocks, -1, piece.shape[1]) for piece in (out_own, up_own_t, down_own)],
    )
    out_full = join_halves(out_own, out_other.reshape(out_own.shape), 0)
    up_full_t = join_halves(up_own_t, up_other_t.reshape(up_own_t.shape), 0)
    down_full = join_halves(down_own, down_other.reshape(down_own.shape), 0)
    table = small_full.astype(jnp.float32)
    up_bias = table[8:12].reshape(FF)
    normed_one, inverse_one = norm_stats(tokens)
    entry_low = (normed_one * table[0] + table[1]).astype(jnp.bfloat16)
    mapped = jnp.dot(entry_low, qkv_full, preferred_element_type=jnp.float32)
    queries = (mapped[:, :model_width] + table[2]).astype(jnp.bfloat16)
    key_own = mapped[:, model_width : 2 * model_width].astype(jnp.bfloat16)
    value_own = (mapped[:, 2 * model_width :] + table[3]).astype(jnp.bfloat16)
    groups = 4
    per_group = HEADS // groups
    group_width = per_group * (model_width // HEADS)
    query_groups, key_groups, value_groups = [], [], []
    for group in range(groups):
        cols = slice(group * group_width, (group + 1) * group_width)
        received = passed_along(
            jnp.concatenate([key_own[:, cols], value_own[:, cols]], 1), "shard", 1
        )
        query_groups.append(split_heads_n(queries[:, cols], per_group))
        key_groups.append(
            split_heads_n(jnp.concatenate([received[:, :group_width], key_own[:, cols]], 0), per_group)
        )
        value_groups.append(
            split_heads_n(jnp.concatenate([received[:, group_width:], value_own[:, cols]], 0), per_group)
        )

    def head_forward(head_item):
        head_query, head_keys, head_values, slope = head_item
        scores = head_scores(head_query, head_keys, slope, allowed, distance, score_scale)
        row_top = jnp.max(scores, axis=-1, keepdims=True)
        weights = jnp.exp(scores - row_top)
        row_total = jnp.sum(weights, axis=-1, keepdims=True)
        probs_low = (weights / row_total).astype(jnp.bfloat16)
        mixture = jnp.dot(probs_low, head_values, preferred_element_type=jnp.float32)
        return (mixture, (row_top + jnp.log(row_total))[:, 0])

    fwd_parts = []
    for group in range(groups):
        chosen = slice(group * per_group, (group + 1) * per_group)
        fwd_parts.append(
            lax.map(
                head_forward,
                (query_groups[group], key_groups[group], value_groups[group], slopes[chosen]),
            )
        )
    mixture_heads = jnp.concatenate([part[0] for part in fwd_parts], 0)
    log_total = jnp.concatenate([part[1] for part in fwd_parts], 0)
    attended_low = merge_heads(mixture_heads).astype(jnp.bfloat16)
    resid_one = (
        tokens + jnp.dot(attended_low, out_full, preferred_element_type=jnp.float32) + table[4]
    )
    normed_two, inverse_two = norm_stats(resid_one)
    inner_low = (normed_two * table[5] + table[6]).astype(jnp.bfloat16)
    grad_out = cotangent * row_live
    down_bias_grad = jnp.sum(grad_out, axis=0)
    grad_low = grad_out.astype(jnp.bfloat16)
    pre_act = contract_cols(inner_low, up_full_t) + up_bias
    act_low = gelu_tanh(pre_act).astype(jnp.bfloat16)
    branch_out = jnp.dot(act_low, down_full, preferred_element_type=jnp.float32)
    block_out = resid_one + branch_out + table[7]
    grad_act = contract_cols(grad_low, down_full)
    down_grad = contract_rows(act_low, grad_low)
    grad_pre = gelu_back(pre_act, grad_act)
    up_bias_grad = jnp.sum(grad_pre, axis=0)
    pre_low = grad_pre.astype(jnp.bfloat16)
    up_grad_t = contract_rows(pre_low, inner_low)
    grad_inner = jnp.dot(pre_low, up_full_t, preferred_element_type=jnp.float32)
    gain_two_grad = jnp.sum(grad_inner * normed_two, axis=0)
    shift_two_grad = jnp.sum(grad_inner, axis=0)
    grad_resid = grad_out + norm_back(grad_inner * table[5], normed_two, inverse_two)
    resid_low = grad_resid.astype(jnp.bfloat16)
    out_grad = contract_rows(attended_low, resid_low)
    grad_resid, resid_low, up_grad_t, down_grad, out_grad = lax.optimization_barrier(
        (grad_resid, resid_low, up_grad_t, down_grad, out_grad)
    )
    out_sum, up_sum_t, down_sum = reduce_rows(
        [split_rows(out_grad), split_rows(up_grad_t), split_rows(down_grad)]
    )
    out_total = out_sum.reshape(out_weight.shape)
    up_total = up_sum_t.reshape(up_weight.shape[::-1]).T
    down_total = down_sum.reshape(down_weight.shape)
    out_bias_grad = jnp.sum(grad_resid, axis=0)
    grad_mixture = contract_cols(resid_low, out_full).astype(jnp.bfloat16)
    grad_heads = split_heads(grad_mixture)

    def head_backward(head_item):
        head_query, head_keys, head_values, head_grad, head_lse, slope = head_item
        scores = head_scores(head_query, head_keys, slope, allowed, distance, score_scale)
        probs = jnp.exp(scores - head_lse[:, None])
        probs_low = probs.astype(jnp.bfloat16)
        grad_values = contract_rows(probs_low, head_grad)
        grad_probs = contract_cols(head_grad, head_values)
        row_delta = jnp.sum(probs * grad_probs, axis=-1, keepdims=True)
        grad_scores = (probs * (grad_probs - row_delta)).astype(jnp.bfloat16)
        grad_query = (
            jnp.dot(grad_scores, head_keys, preferred_element_type=jnp.float32) * score_scale
        )
        grad_keys = contract_rows(grad_scores, head_query) * score_scale
        return (grad_query, grad_keys, grad_values)

    query_parts, key_parts, value_parts = [], [], []
    for group in range(groups):
        chosen = slice(group * per_group, (group + 1) * per_group)
        group_query, group_keys, group_values = lax.map(
            head_backward,
            (
                query_groups[group],
                key_groups[group],
                value_groups[group],
                grad_heads[chosen],
                log_total[chosen],
                slopes[chosen],
            ),
        )
        returned = passed_along(
            jnp.concatenate(
                [merge_heads(group_keys[:, :tok_rows]), merge_heads(group_values[:, :tok_rows])], 1
            ).astype(jnp.bfloat16),
            "shard",
            -1,
        ).astype(jnp.float32)
        query_parts.append(merge_heads(group_query))
        key_parts.append(merge_heads(group_keys[:, tok_rows:]) + returned[:, :group_width])
        value_parts.append(merge_heads(group_values[:, tok_rows:]) + returned[:, group_width:])
    grad_query = jnp.concatenate(query_parts, 1)
    grad_key_own = jnp.concatenate(key_parts, 1)
    grad_value_own = jnp.concatenate(value_parts, 1)
    query_bias_grad = jnp.sum(grad_query, axis=0)
    value_bias_grad = jnp.sum(grad_value_own, axis=0)
    mapped_low = jnp.concatenate([grad_query, grad_key_own, grad_value_own], 1).astype(jnp.bfloat16)
    qkv_grad = contract_rows(entry_low, mapped_low)
    grad_entry = contract_cols(mapped_low, qkv_full)
    gain_one_grad = jnp.sum(grad_entry * normed_one, axis=0)
    shift_one_grad = jnp.sum(grad_entry, axis=0)
    input_grad = grad_resid + norm_back(grad_entry * table[0], normed_one, inverse_one)
    head_rows = jnp.stack(
        [
            gain_one_grad,
            shift_one_grad,
            query_bias_grad,
            value_bias_grad,
            out_bias_grad,
            gain_two_grad,
            shift_two_grad,
            down_bias_grad,
        ]
    )
    small_grad = jnp.concatenate([head_rows, up_bias_grad.reshape(4, model_width)], 0)
    small_halves = small_grad.reshape(small_grad.shape[0], shard_count, -1).transpose(1, 0, 2)
    small_packed = jnp.stack(
        [small_rows(small_halves[index], blocks) for index in range(shard_count)]
    ).reshape(shard_count, lax.axis_size("core"), lax.axis_size("outer"), 1, SMALL_WIDTH)
    qkv_sum, small_sum = reduce_rows([split_rows(qkv_grad), small_packed])
    qkv_total = qkv_sum.reshape(qkv_weight.shape)
    small_total = small_sum.reshape(-1)[: small_params.size].reshape(small_params.shape)
    rate = 2.0 / math.sqrt(model_width * tok_rows * shard_count * group_count)
    qkv_new = nesterov(qkv_total, qkv_weight, qkv_momentum, qkv_average, rate)
    out_new = nesterov(out_total, out_weight, out_momentum, out_average, rate)
    up_new = nesterov(up_total, up_weight, up_momentum, up_average, rate)
    down_new = nesterov(down_total, down_weight, down_momentum, down_average, rate)
    small_new = nesterov(small_total, small_params, small_momentum, small_average, rate)
    return (
        block_out,
        input_grad,
        qkv_new[0],
        qkv_new[1],
        qkv_new[2],
        out_new[0],
        out_new[1],
        out_new[2],
        up_new[0],
        up_new[1],
        up_new[2],
        down_new[0],
        down_new[1],
        down_new[2],
        small_new[0],
        small_new[1],
        small_new[2],
    )


def solution(mesh):
    cores = 2
    devices = mesh.devices.reshape(mesh.shape["group"] // cores, cores, mesh.shape["shard"])
    inner_mesh = jax.sharding.Mesh(devices, ("outer", "core", "shard"))
    rows = P(("outer", "core", "shard"), None)
    in_specs = (
        rows,
        rows,
        P(),
        P("shard", None),
        P("shard", None),
        P("shard", None),
        P("shard", None),
        P("shard", None),
        P("shard", None),
        P(None, "shard"),
        P(None, "shard"),
        P(None, "shard"),
        P("shard", None),
        P("shard", None),
        P("shard", None),
        P(None, "shard"),
        P(None, "shard"),
        P(None, "shard"),
    )
    out_specs = (
        rows,
        rows,
        P("shard", None),
        P("shard", None),
        P("shard", None),
        P("shard", None),
        P("shard", None),
        P("shard", None),
        P(None, "shard"),
        P(None, "shard"),
        P(None, "shard"),
        P("shard", None),
        P("shard", None),
        P("shard", None),
        P(None, "shard"),
        P(None, "shard"),
        P(None, "shard"),
    )

    return jax.shard_map(body, mesh=inner_mesh, in_specs=in_specs, out_specs=out_specs, check_vma=False)
```

```python
import math

import jax
import jax.numpy as jnp
from jax import lax
from jax.sharding import PartitionSpec as P


HEADS = 16
FF = 4096


EPS = 1e-05
MOMENTUM = 0.9
AVERAGING = 0.9
NEG_FILL = -1e30
SHARD = "shard"
OUTER = "outer"
CORE = "core"


def passed_along(value, axis, steps):
    count = lax.axis_size(axis)
    leading, last = (max(0, -steps), min(count, count - steps))
    return lax.ppermute(value, axis, [(source, source + steps) for source in range(leading, last)])


SMALL_WIDTH = 3072


def small_rows(small_half, blocks):
    flat = small_half.reshape(-1)
    padded = blocks * SMALL_WIDTH
    return jnp.pad(flat, (0, padded - flat.shape[0])).reshape(blocks, 1, SMALL_WIDTH)


def gather_rows(row_arrays):
    cores = lax.axis_size(CORE)
    outer = lax.axis_size(OUTER)
    blocks = cores * outer
    place = lax.axis_index(CORE) * outer + lax.axis_index(OUTER)
    heights = [piece.shape[1] for piece in row_arrays]
    mine = jnp.concatenate(
        [lax.dynamic_index_in_dim(piece, place, 0, keepdims=False) for piece in row_arrays], 0
    )
    other = lax.ppermute(mine, SHARD, [(0, 1), (1, 0)])
    got = lax.all_gather(other, OUTER, axis=0, tiled=False)
    got = lax.all_gather(got, CORE, axis=0, tiled=False)
    got = got.reshape(blocks, -1, got.shape[-1])
    pieces = []
    offset = 0
    for height in heights:
        pieces.append(got[:, offset : offset + height])
        offset += height
    return pieces


def join_halves(own, other, dim):
    upper = lax.axis_index(SHARD) == 1
    in_order = jnp.concatenate([own, other], axis=dim)
    swapped = jnp.concatenate([other, own], axis=dim)
    return jnp.where(upper, swapped, in_order)


def reduce_rows(row_grads):
    shard_count = lax.axis_size(SHARD)
    cores = lax.axis_size(CORE)
    outer = lax.axis_size(OUTER)
    blocks = cores * outer
    heights = [piece.shape[3] for piece in row_grads]
    width = row_grads[0].shape[-1]
    stacked = jnp.concatenate([piece.astype(jnp.bfloat16) for piece in row_grads], 3)
    stacked = stacked.reshape(cores, -1, width)
    stacked = lax.psum_scatter(stacked, CORE, scatter_dimension=0, tiled=True)
    stacked = stacked.reshape(outer, -1, width)
    stacked = lax.psum_scatter(stacked, OUTER, scatter_dimension=0, tiled=True)
    stacked = stacked.reshape(shard_count, -1, width)
    stacked = lax.psum_scatter(stacked, SHARD, scatter_dimension=0, tiled=True)
    stacked = stacked.reshape(stacked.shape[1:])
    stacked = lax.all_gather(stacked, OUTER, axis=0, tiled=True)
    stacked = lax.all_gather(stacked, CORE, axis=0, tiled=True)
    stacked = stacked.reshape(blocks, -1, width)
    pieces = []
    offset = 0
    for height in heights:
        pieces.append(stacked[:, offset : offset + height].astype(jnp.float32))
        offset += height
    return pieces


def split_rows(grad_full):
    shard_count = lax.axis_size(SHARD)
    cores = lax.axis_size(CORE)
    outer = lax.axis_size(OUTER)
    rows, cols = grad_full.shape
    split = grad_full.reshape(shard_count, cores, outer, rows // (shard_count * cores * outer), cols)
    return split.transpose(1, 2, 0, 3, 4)


def block_major(grad_perm):
    shard_count = lax.axis_size(SHARD)
    cores = lax.axis_size(CORE)
    outer = lax.axis_size(OUTER)
    rows, cols = grad_perm.shape
    return grad_perm.reshape(cores, outer, shard_count, rows // (shard_count * cores * outer), cols)


def ff_order(values, blocks):
    shard_count = lax.axis_size(SHARD)
    rest = values.shape[1:]
    split = values.reshape((shard_count, blocks, values.shape[0] // (shard_count * blocks)) + rest)
    return jnp.swapaxes(split, 0, 1).reshape(values.shape)


def ff_natural(values, blocks):
    shard_count = lax.axis_size(SHARD)
    rest = values.shape[1:]
    split = values.reshape((blocks, shard_count, values.shape[0] // (shard_count * blocks)) + rest)
    return jnp.swapaxes(split, 0, 1).reshape(values.shape)


def join_blocks(own, other, blocks):
    upper = lax.axis_index(SHARD) == 1
    own_b = own.reshape((blocks, -1) + own.shape[1:])
    other_b = other.reshape((blocks, -1) + other.shape[1:])
    in_order = jnp.stack([own_b, other_b], 1)
    swapped = jnp.stack([other_b, own_b], 1)
    joined = jnp.where(upper, swapped, in_order)
    return joined.reshape((2 * own.shape[0],) + own.shape[1:])


def norm_stats(field_in):
    centred = field_in - jnp.mean(field_in, axis=-1, keepdims=True)
    inverse = lax.rsqrt(jnp.mean(centred * centred, axis=-1, keepdims=True) + EPS)
    return (centred * inverse, inverse)


def norm_back(grad_hat, normed, inverse):
    first_mean = jnp.mean(grad_hat, axis=-1, keepdims=True)
    second_mean = jnp.mean(grad_hat * normed, axis=-1, keepdims=True)
    return inverse * (grad_hat - first_mean - normed * second_mean)


def contract_rows(left_side, right_side):
    return lax.dot_general(
        left_side, right_side, (((0,), (0,)), ((), ())), preferred_element_type=jnp.float32
    )


def contract_cols(left_side, right_side):
    return lax.dot_general(
        left_side, right_side, (((1,), (1,)), ((), ())), preferred_element_type=jnp.float32
    )


def split_heads(field_in):
    return field_in.reshape(field_in.shape[0], HEADS, -1).transpose(1, 0, 2)


def split_heads_n(field_in, heads):
    return field_in.reshape(field_in.shape[0], heads, -1).transpose(1, 0, 2)


def merge_heads(field_in):
    return field_in.transpose(1, 0, 2).reshape(field_in.shape[1], -1)


def gelu_tanh(field_in):
    return jax.nn.gelu(field_in, approximate=True)


def gelu_back(pre_act, grad_act):
    _, pull_back = jax.vjp(gelu_tanh, pre_act)
    return pull_back(grad_act)[0]


def head_scores(queries, key_block, slope, allowed, distance, score_scale):
    raw = contract_cols(queries, key_block) * score_scale - slope * distance
    return jnp.where(allowed, raw, NEG_FILL)


def nesterov(grad_total, weight_old, moment_old, average_old, rate):
    moment_new = MOMENTUM * moment_old + grad_total
    weight_new = weight_old - rate * (grad_total + MOMENTUM * moment_new)
    average_new = AVERAGING * average_old + (1.0 - AVERAGING) * weight_new
    return (weight_new, moment_new, average_new)


def body(
    tokens,
    cotangent,
    lengths,
    qkv_weight,
    qkv_momentum,
    qkv_average,
    out_weight,
    out_momentum,
    out_average,
    up_weight,
    up_momentum,
    up_average,
    down_weight,
    down_momentum,
    down_average,
    small_params,
    small_momentum,
    small_average,
):
    tok_rows = tokens.shape[0]
    model_width = tokens.shape[1]
    shard_count = lax.axis_size(SHARD)
    group_count = lax.axis_size(OUTER) * lax.axis_size(CORE)
    shard_place = lax.axis_index(SHARD)
    group_place = lax.axis_index(OUTER) * lax.axis_size(CORE) + lax.axis_index(CORE)
    upper_half = shard_place % 2
    seq_place = group_place * (shard_count // 2) + shard_place // 2
    seq_length = lax.dynamic_index_in_dim(lengths, seq_place, 0, keepdims=False)
    local_pos = jnp.arange(tok_rows, dtype=jnp.int32)
    query_pos = upper_half * tok_rows + local_pos
    key_pos = jnp.concatenate([local_pos, query_pos])
    prev_live = jnp.full((tok_rows,), upper_half == 1)
    key_live = jnp.concatenate([prev_live, jnp.ones((tok_rows,), bool)]) & (key_pos < seq_length)
    allowed = key_live[None, :] & (key_pos[None, :] <= query_pos[:, None])
    distance = (query_pos[:, None] - key_pos[None, :]).astype(jnp.float32)
    row_live = (query_pos < seq_length).astype(jnp.float32)[:, None]
    head_size = model_width // HEADS
    score_scale = head_size ** (-0.5)
    slopes = 2.0 ** (-8.0 * (jnp.arange(HEADS, dtype=jnp.float32) + 1.0) / HEADS)
    blocks = lax.axis_size(CORE) * lax.axis_size(OUTER)
    qkv_own = qkv_weight.astype(jnp.bfloat16)
    small_own = small_params.astype(jnp.bfloat16)
    qkv_other, small_other = gather_rows(
        [qkv_own.reshape(blocks, -1, qkv_own.shape[1]), small_rows(small_own, blocks)]
    )
    qkv_full = join_halves(qkv_own, qkv_other.reshape(qkv_own.shape), 0)
    small_full = join_halves(
        small_own, small_other.reshape(-1)[: small_own.size].reshape(small_own.shape), 1
    )
    out_own = out_weight.astype(jnp.bfloat16)
    up_own_t = up_weight.astype(jnp.bfloat16).T
    down_own = down_weight.astype(jnp.bfloat16)
    out_other, up_other_t, down_other = gather_rows(
        [piece.reshape(blocks, -1, piece.shape[1]) for piece in (out_own, up_own_t, down_own)],
    )
    out_full = join_halves(out_own, out_other.reshape(out_own.shape), 0)
    up_full_t = join_blocks(up_own_t, up_other_t.reshape(up_own_t.shape), blocks)
    down_full = join_blocks(down_own, down_other.reshape(down_own.shape), blocks)
    table = small_full.astype(jnp.float32)
    up_bias = ff_order(table[8:12].reshape(FF), blocks)
    normed_one, inverse_one = norm_stats(tokens)
    entry_low = (normed_one * table[0] + table[1]).astype(jnp.bfloat16)
    mapped = jnp.dot(entry_low, qkv_full, preferred_element_type=jnp.float32)
    queries = (mapped[:, :model_width] + table[2]).astype(jnp.bfloat16)
    key_own = mapped[:, model_width : 2 * model_width].astype(jnp.bfloat16)
    value_own = (mapped[:, 2 * model_width :] + table[3]).astype(jnp.bfloat16)
    groups = 4
    per_group = HEADS // groups
    group_width = per_group * (model_width // HEADS)
    query_groups, key_groups, value_groups = [], [], []
    for group in range(groups):
        cols = slice(group * group_width, (group + 1) * group_width)
        received = passed_along(
            jnp.concatenate([key_own[:, cols], value_own[:, cols]], 1), SHARD, 1
        )
        query_groups.append(split_heads_n(queries[:, cols], per_group))
        key_groups.append(
            split_heads_n(jnp.concatenate([received[:, :group_width], key_own[:, cols]], 0), per_group)
        )
        value_groups.append(
            split_heads_n(jnp.concatenate([received[:, group_width:], value_own[:, cols]], 0), per_group)
        )

    def head_forward(head_item):
        head_query, head_keys, head_values, slope = head_item
        scores = head_scores(head_query, head_keys, slope, allowed, distance, score_scale)
        row_top = jnp.max(scores, axis=-1, keepdims=True)
        weights = jnp.exp(scores - row_top)
        row_total = jnp.sum(weights, axis=-1, keepdims=True)
        probs_low = (weights / row_total).astype(jnp.bfloat16)
        mixture = jnp.dot(probs_low, head_values, preferred_element_type=jnp.float32)
        return (mixture, (row_top + jnp.log(row_total))[:, 0])

    fwd_parts = []
    for group in range(groups):
        chosen = slice(group * per_group, (group + 1) * per_group)
        fwd_parts.append(
            lax.map(
                head_forward,
                (query_groups[group], key_groups[group], value_groups[group], slopes[chosen]),
            )
        )
    mixture_heads = jnp.concatenate([part[0] for part in fwd_parts], 0)
    log_total = jnp.concatenate([part[1] for part in fwd_parts], 0)
    attended_low = merge_heads(mixture_heads).astype(jnp.bfloat16)
    resid_one = (
        tokens + jnp.dot(attended_low, out_full, preferred_element_type=jnp.float32) + table[4]
    )
    normed_two, inverse_two = norm_stats(resid_one)
    inner_low = (normed_two * table[5] + table[6]).astype(jnp.bfloat16)
    grad_out = cotangent * row_live
    down_bias_grad = jnp.sum(grad_out, axis=0)
    grad_low = grad_out.astype(jnp.bfloat16)
    pre_act = contract_cols(inner_low, up_full_t) + up_bias
    act_low = gelu_tanh(pre_act).astype(jnp.bfloat16)
    branch_out = jnp.dot(act_low, down_full, preferred_element_type=jnp.float32)
    block_out = resid_one + branch_out + table[7]
    grad_act = contract_cols(grad_low, down_full)
    down_grad = contract_rows(act_low, grad_low)
    grad_pre = gelu_back(pre_act, grad_act)
    up_bias_grad = ff_natural(jnp.sum(grad_pre, axis=0), blocks)
    pre_low = grad_pre.astype(jnp.bfloat16)
    up_grad_t = contract_rows(pre_low, inner_low)
    grad_inner = jnp.dot(pre_low, up_full_t, preferred_element_type=jnp.float32)
    gain_two_grad = jnp.sum(grad_inner * normed_two, axis=0)
    shift_two_grad = jnp.sum(grad_inner, axis=0)
    grad_resid = grad_out + norm_back(grad_inner * table[5], normed_two, inverse_two)
    resid_low = grad_resid.astype(jnp.bfloat16)
    out_grad = contract_rows(attended_low, resid_low)
    grad_resid, resid_low, up_grad_t, down_grad, out_grad = lax.optimization_barrier(
        (grad_resid, resid_low, up_grad_t, down_grad, out_grad)
    )
    out_sum, up_sum_t, down_sum = reduce_rows(
        [split_rows(out_grad), block_major(up_grad_t), block_major(down_grad)]
    )
    out_total = out_sum.reshape(out_weight.shape)
    up_total = up_sum_t.reshape(up_weight.shape[::-1]).T
    down_total = down_sum.reshape(down_weight.shape)
    out_bias_grad = jnp.sum(grad_resid, axis=0)
    grad_mixture = contract_cols(resid_low, out_full).astype(jnp.bfloat16)
    grad_heads = split_heads(grad_mixture)

    def head_backward(head_item):
        head_query, head_keys, head_values, head_grad, head_lse, slope = head_item
        scores = head_scores(head_query, head_keys, slope, allowed, distance, score_scale)
        probs = jnp.exp(scores - head_lse[:, None])
        probs_low = probs.astype(jnp.bfloat16)
        grad_values = contract_rows(probs_low, head_grad)
        grad_probs = contract_cols(head_grad, head_values)
        row_delta = jnp.sum(probs * grad_probs, axis=-1, keepdims=True)
        grad_scores = (probs * (grad_probs - row_delta)).astype(jnp.bfloat16)
        grad_query = (
            jnp.dot(grad_scores, head_keys, preferred_element_type=jnp.float32) * score_scale
        )
        grad_keys = contract_rows(grad_scores, head_query) * score_scale
        return (grad_query, grad_keys, grad_values)

    query_parts, key_parts, value_parts = [], [], []
    for group in range(groups):
        chosen = slice(group * per_group, (group + 1) * per_group)
        group_query, group_keys, group_values = lax.map(
            head_backward,
            (
                query_groups[group],
                key_groups[group],
                value_groups[group],
                grad_heads[chosen],
                log_total[chosen],
                slopes[chosen],
            ),
        )
        returned = passed_along(
            jnp.concatenate(
                [merge_heads(group_keys[:, :tok_rows]), merge_heads(group_values[:, :tok_rows])], 1
            ).astype(jnp.bfloat16),
            SHARD,
            -1,
        ).astype(jnp.float32)
        query_parts.append(merge_heads(group_query))
        key_parts.append(merge_heads(group_keys[:, tok_rows:]) + returned[:, :group_width])
        value_parts.append(merge_heads(group_values[:, tok_rows:]) + returned[:, group_width:])
    grad_query = jnp.concatenate(query_parts, 1)
    grad_key_own = jnp.concatenate(key_parts, 1)
    grad_value_own = jnp.concatenate(value_parts, 1)
    query_bias_grad = jnp.sum(grad_query, axis=0)
    value_bias_grad = jnp.sum(grad_value_own, axis=0)
    mapped_low = jnp.concatenate([grad_query, grad_key_own, grad_value_own], 1).astype(jnp.bfloat16)
    qkv_grad = contract_rows(entry_low, mapped_low)
    grad_entry = contract_cols(mapped_low, qkv_full)
    gain_one_grad = jnp.sum(grad_entry * normed_one, axis=0)
    shift_one_grad = jnp.sum(grad_entry, axis=0)
    input_grad = grad_resid + norm_back(grad_entry * table[0], normed_one, inverse_one)
    head_rows = jnp.stack(
        [
            gain_one_grad,
            shift_one_grad,
            query_bias_grad,
            value_bias_grad,
            out_bias_grad,
            gain_two_grad,
            shift_two_grad,
            down_bias_grad,
        ]
    )
    small_grad = jnp.concatenate([head_rows, up_bias_grad.reshape(4, model_width)], 0)
    small_halves = small_grad.reshape(small_grad.shape[0], shard_count, -1).transpose(1, 0, 2)
    small_packed = jnp.stack(
        [small_rows(small_halves[index], blocks) for index in range(shard_count)]
    ).reshape(shard_count, lax.axis_size(CORE), lax.axis_size(OUTER), 1, SMALL_WIDTH)
    small_packed = small_packed.transpose(1, 2, 0, 3, 4)
    qkv_sum, small_sum = reduce_rows([split_rows(qkv_grad), small_packed])
    qkv_total = qkv_sum.reshape(qkv_weight.shape)
    small_total = small_sum.reshape(-1)[: small_params.size].reshape(small_params.shape)
    rate = 2.0 / math.sqrt(model_width * tok_rows * shard_count * group_count)
    qkv_new = nesterov(qkv_total, qkv_weight, qkv_momentum, qkv_average, rate)
    out_new = nesterov(out_total, out_weight, out_momentum, out_average, rate)
    up_new = nesterov(up_total, up_weight, up_momentum, up_average, rate)
    down_new = nesterov(down_total, down_weight, down_momentum, down_average, rate)
    small_new = nesterov(small_total, small_params, small_momentum, small_average, rate)
    return (
        block_out,
        input_grad,
        qkv_new[0],
        qkv_new[1],
        qkv_new[2],
        out_new[0],
        out_new[1],
        out_new[2],
        up_new[0],
        up_new[1],
        up_new[2],
        down_new[0],
        down_new[1],
        down_new[2],
        small_new[0],
        small_new[1],
        small_new[2],
    )


def solution(mesh):
    cores = 2
    devices = mesh.devices.reshape(mesh.shape["group"] // cores, cores, mesh.shape[SHARD])
    inner_mesh = jax.sharding.Mesh(devices, (OUTER, CORE, SHARD))
    rows = P((OUTER, CORE, SHARD), None)
    in_specs = (
        rows,
        rows,
        P(),
        P(SHARD, None),
        P(SHARD, None),
        P(SHARD, None),
        P(SHARD, None),
        P(SHARD, None),
        P(SHARD, None),
        P(None, SHARD),
        P(None, SHARD),
        P(None, SHARD),
        P(SHARD, None),
        P(SHARD, None),
        P(SHARD, None),
        P(None, SHARD),
        P(None, SHARD),
        P(None, SHARD),
    )
    out_specs = (
        rows,
        rows,
        P(SHARD, None),
        P(SHARD, None),
        P(SHARD, None),
        P(SHARD, None),
        P(SHARD, None),
        P(SHARD, None),
        P(None, SHARD),
        P(None, SHARD),
        P(None, SHARD),
        P(SHARD, None),
        P(SHARD, None),
        P(SHARD, None),
        P(None, SHARD),
        P(None, SHARD),
        P(None, SHARD),
    )

    return jax.shard_map(body, mesh=inner_mesh, in_specs=in_specs, out_specs=out_specs, check_vma=False)
```

```python
import functools
import math

import jax
import jax.numpy as jnp
from jax import lax
from jax.experimental import pallas as pl
from jax.experimental.pallas import tpu as pltpu
from jax.sharding import PartitionSpec as P


HEADS = 16
FF = 4096


EPS = 1e-05
MOMENTUM = 0.9
AVERAGING = 0.9
NEG_FILL = -1e30
SHARD = "shard"
OUTER = "outer"
CORE = "core"


def _scores(info_ref, slope_ref, q, k, score_scale):
    upper = info_ref[0]
    seq_length = info_ref[1]
    rows, cols = q.shape[0], k.shape[0]
    own = cols - rows
    raw = lax.dot_general(q, k, (((1,), (1,)), ((), ())), preferred_element_type=jnp.float32)
    query_pos = upper * rows + lax.broadcasted_iota(jnp.int32, (rows, cols), 0)
    key_index = lax.broadcasted_iota(jnp.int32, (rows, cols), 1)
    key_pos = jnp.where(key_index < own, key_index, upper * rows + key_index - own)
    allowed = ((key_index >= own) | (upper == 1)) & (key_pos < seq_length) & (key_pos <= query_pos)
    distance = (query_pos - key_pos).astype(jnp.float32)
    slope = slope_ref[0][:, 0:1]
    raw = raw * score_scale - slope * distance
    return jnp.where(allowed, raw, NEG_FILL)


def _fwd_kernel(score_scale, info_ref, slope_ref, q_ref, k_ref, v_ref, mix_ref, lse_ref):
    scores = _scores(info_ref, slope_ref, q_ref[0], k_ref[0], score_scale)
    row_top = jnp.max(scores, axis=-1, keepdims=True)
    weights = jnp.exp(scores - row_top)
    row_total = jnp.sum(weights, axis=-1, keepdims=True)
    probs_low = (weights / row_total).astype(jnp.bfloat16)
    mix = jnp.dot(probs_low, v_ref[0], preferred_element_type=jnp.float32)
    mix_ref[0] = mix.astype(mix_ref.dtype)
    lse_ref[0] = row_top + jnp.log(row_total)


def _bwd_kernel(score_scale, info_ref, slope_ref, q_ref, k_ref, v_ref, g_ref, lse_ref, dq_ref, dk_ref, dv_ref):
    q = q_ref[0]
    k = k_ref[0]
    grad = g_ref[0]
    scores = _scores(info_ref, slope_ref, q, k, score_scale)
    probs = jnp.exp(scores - lse_ref[0])
    probs_low = probs.astype(jnp.bfloat16)
    dv_ref[0] = lax.dot_general(probs_low, grad, (((0,), (0,)), ((), ())), preferred_element_type=jnp.float32)
    grad_probs = lax.dot_general(grad, v_ref[0], (((1,), (1,)), ((), ())), preferred_element_type=jnp.float32)
    row_delta = jnp.sum(probs * grad_probs, axis=-1, keepdims=True)
    grad_scores = (probs * (grad_probs - row_delta)).astype(jnp.bfloat16)
    dq_ref[0] = jnp.dot(grad_scores, k, preferred_element_type=jnp.float32) * score_scale
    dk_ref[0] = lax.dot_general(grad_scores, q, (((0,), (0,)), ((), ())), preferred_element_type=jnp.float32) * score_scale


def _slope_rows(slopes):
    return jnp.broadcast_to(slopes[:, None, None], (slopes.shape[0], 1, 128)).astype(jnp.float32)


def attention_fwd(info, slopes, queries, keys, values, score_scale):
    heads, rows, width = queries.shape
    cols = keys.shape[1]
    head_map = lambda h, info_ref: (h, 0, 0)
    flops = 4 * heads * rows * cols * width
    return pl.pallas_call(
        functools.partial(_fwd_kernel, score_scale),
        grid_spec=pltpu.PrefetchScalarGridSpec(
            num_scalar_prefetch=1,
            grid=(heads,),
            in_specs=[
                pl.BlockSpec((1, 1, 128), head_map),
                pl.BlockSpec((1, rows, width), head_map),
                pl.BlockSpec((1, cols, width), head_map),
                pl.BlockSpec((1, cols, width), head_map),
            ],
            out_specs=[
                pl.BlockSpec((1, rows, width), head_map),
                pl.BlockSpec((1, rows, 1), head_map),
            ],
        ),
        out_shape=[
            jax.ShapeDtypeStruct((heads, rows, width), jnp.bfloat16),
            jax.ShapeDtypeStruct((heads, rows, 1), jnp.float32),
        ],
        compiler_params=pltpu.CompilerParams(vmem_limit_bytes=48 * 1024 * 1024),
        cost_estimate=pl.CostEstimate(
            flops=flops, transcendentals=heads * rows * cols, bytes_accessed=2 * heads * (rows + 2 * cols) * width * 2
        ),
    )(info, _slope_rows(slopes), queries, keys, values)


def attention_bwd(info, slopes, queries, keys, values, grads, lse, score_scale):
    heads, rows, width = queries.shape
    cols = keys.shape[1]
    head_map = lambda h, info_ref: (h, 0, 0)
    flops = 8 * heads * rows * cols * width
    return pl.pallas_call(
        functools.partial(_bwd_kernel, score_scale),
        grid_spec=pltpu.PrefetchScalarGridSpec(
            num_scalar_prefetch=1,
            grid=(heads,),
            in_specs=[
                pl.BlockSpec((1, 1, 128), head_map),
                pl.BlockSpec((1, rows, width), head_map),
                pl.BlockSpec((1, cols, width), head_map),
                pl.BlockSpec((1, cols, width), head_map),
                pl.BlockSpec((1, rows, width), head_map),
                pl.BlockSpec((1, rows, 1), head_map),
            ],
            out_specs=[
                pl.BlockSpec((1, rows, width), head_map),
                pl.BlockSpec((1, cols, width), head_map),
                pl.BlockSpec((1, cols, width), head_map),
            ],
        ),
        out_shape=[
            jax.ShapeDtypeStruct((heads, rows, width), jnp.float32),
            jax.ShapeDtypeStruct((heads, cols, width), jnp.float32),
            jax.ShapeDtypeStruct((heads, cols, width), jnp.float32),
        ],
        compiler_params=pltpu.CompilerParams(vmem_limit_bytes=48 * 1024 * 1024),
        cost_estimate=pl.CostEstimate(
            flops=flops, transcendentals=heads * rows * cols, bytes_accessed=heads * (rows + 2 * cols) * width * 6
        ),
    )(info, _slope_rows(slopes), queries, keys, values, grads, lse)


def passed_along(value, axis, steps):
    count = lax.axis_size(axis)
    leading, last = (max(0, -steps), min(count, count - steps))
    return lax.ppermute(value, axis, [(source, source + steps) for source in range(leading, last)])


SMALL_WIDTH = 3072


def small_rows(small_half, blocks):
    flat = small_half.reshape(-1)
    padded = blocks * SMALL_WIDTH
    return jnp.pad(flat, (0, padded - flat.shape[0])).reshape(blocks, 1, SMALL_WIDTH)


def gather_rows(row_arrays):
    cores = lax.axis_size(CORE)
    outer = lax.axis_size(OUTER)
    blocks = cores * outer
    place = lax.axis_index(CORE) * outer + lax.axis_index(OUTER)
    heights = [piece.shape[1] for piece in row_arrays]
    mine = jnp.concatenate(
        [lax.dynamic_index_in_dim(piece, place, 0, keepdims=False) for piece in row_arrays], 0
    )
    other = lax.ppermute(mine, SHARD, [(0, 1), (1, 0)])
    got = lax.all_gather(other, OUTER, axis=0, tiled=False)
    got = lax.all_gather(got, CORE, axis=0, tiled=False)
    got = got.reshape(blocks, -1, got.shape[-1])
    pieces = []
    offset = 0
    for height in heights:
        pieces.append(got[:, offset : offset + height])
        offset += height
    return pieces


def join_halves(own, other, dim):
    upper = lax.axis_index(SHARD) == 1
    in_order = jnp.concatenate([own, other], axis=dim)
    swapped = jnp.concatenate([other, own], axis=dim)
    return jnp.where(upper, swapped, in_order)


def reduce_rows(row_grads):
    shard_count = lax.axis_size(SHARD)
    cores = lax.axis_size(CORE)
    outer = lax.axis_size(OUTER)
    blocks = cores * outer
    heights = [piece.shape[3] for piece in row_grads]
    width = row_grads[0].shape[-1]
    stacked = jnp.concatenate([piece.astype(jnp.bfloat16) for piece in row_grads], 3)
    stacked = stacked.reshape(cores, -1, width)
    stacked = lax.psum_scatter(stacked, CORE, scatter_dimension=0, tiled=True)
    stacked = stacked.reshape(outer, -1, width)
    stacked = lax.psum_scatter(stacked, OUTER, scatter_dimension=0, tiled=True)
    stacked = stacked.reshape(shard_count, -1, width)
    stacked = lax.psum_scatter(stacked, SHARD, scatter_dimension=0, tiled=True)
    stacked = stacked.reshape(stacked.shape[1:])
    stacked = lax.all_gather(stacked, OUTER, axis=0, tiled=True)
    stacked = lax.all_gather(stacked, CORE, axis=0, tiled=True)
    stacked = stacked.reshape(blocks, -1, width)
    pieces = []
    offset = 0
    for height in heights:
        pieces.append(stacked[:, offset : offset + height].astype(jnp.float32))
        offset += height
    return pieces


def split_rows(grad_full):
    shard_count = lax.axis_size(SHARD)
    cores = lax.axis_size(CORE)
    outer = lax.axis_size(OUTER)
    rows, cols = grad_full.shape
    split = grad_full.reshape(shard_count, cores, outer, rows // (shard_count * cores * outer), cols)
    return split.transpose(1, 2, 0, 3, 4)


def block_major(grad_perm):
    shard_count = lax.axis_size(SHARD)
    cores = lax.axis_size(CORE)
    outer = lax.axis_size(OUTER)
    rows, cols = grad_perm.shape
    return grad_perm.reshape(cores, outer, shard_count, rows // (shard_count * cores * outer), cols)


def ff_order(values, blocks):
    shard_count = lax.axis_size(SHARD)
    rest = values.shape[1:]
    split = values.reshape((shard_count, blocks, values.shape[0] // (shard_count * blocks)) + rest)
    return jnp.swapaxes(split, 0, 1).reshape(values.shape)


def ff_natural(values, blocks):
    shard_count = lax.axis_size(SHARD)
    rest = values.shape[1:]
    split = values.reshape((blocks, shard_count, values.shape[0] // (shard_count * blocks)) + rest)
    return jnp.swapaxes(split, 0, 1).reshape(values.shape)


def join_blocks(own, other, blocks):
    upper = lax.axis_index(SHARD) == 1
    own_b = own.reshape((blocks, -1) + own.shape[1:])
    other_b = other.reshape((blocks, -1) + other.shape[1:])
    in_order = jnp.stack([own_b, other_b], 1)
    swapped = jnp.stack([other_b, own_b], 1)
    joined = jnp.where(upper, swapped, in_order)
    return joined.reshape((2 * own.shape[0],) + own.shape[1:])


def norm_stats(field_in):
    centred = field_in - jnp.mean(field_in, axis=-1, keepdims=True)
    inverse = lax.rsqrt(jnp.mean(centred * centred, axis=-1, keepdims=True) + EPS)
    return (centred * inverse, inverse)


def norm_back(grad_hat, normed, inverse):
    first_mean = jnp.mean(grad_hat, axis=-1, keepdims=True)
    second_mean = jnp.mean(grad_hat * normed, axis=-1, keepdims=True)
    return inverse * (grad_hat - first_mean - normed * second_mean)


def contract_rows(left_side, right_side):
    return lax.dot_general(
        left_side, right_side, (((0,), (0,)), ((), ())), preferred_element_type=jnp.float32
    )


def contract_cols(left_side, right_side):
    return lax.dot_general(
        left_side, right_side, (((1,), (1,)), ((), ())), preferred_element_type=jnp.float32
    )


def split_heads(field_in):
    return field_in.reshape(field_in.shape[0], HEADS, -1).transpose(1, 0, 2)


def split_heads_n(field_in, heads):
    return field_in.reshape(field_in.shape[0], heads, -1).transpose(1, 0, 2)


def merge_heads(field_in):
    return field_in.transpose(1, 0, 2).reshape(field_in.shape[1], -1)


def gelu_tanh(field_in):
    return jax.nn.gelu(field_in, approximate=True)


def gelu_back(pre_act, grad_act):
    _, pull_back = jax.vjp(gelu_tanh, pre_act)
    return pull_back(grad_act)[0]


def nesterov(grad_total, weight_old, moment_old, average_old, rate):
    moment_new = MOMENTUM * moment_old + grad_total
    weight_new = weight_old - rate * (grad_total + MOMENTUM * moment_new)
    average_new = AVERAGING * average_old + (1.0 - AVERAGING) * weight_new
    return (weight_new, moment_new, average_new)


def body(
    tokens,
    cotangent,
    lengths,
    qkv_weight,
    qkv_momentum,
    qkv_average,
    out_weight,
    out_momentum,
    out_average,
    up_weight,
    up_momentum,
    up_average,
    down_weight,
    down_momentum,
    down_average,
    small_params,
    small_momentum,
    small_average,
):
    tok_rows = tokens.shape[0]
    model_width = tokens.shape[1]
    shard_count = lax.axis_size(SHARD)
    group_count = lax.axis_size(OUTER) * lax.axis_size(CORE)
    shard_place = lax.axis_index(SHARD)
    group_place = lax.axis_index(OUTER) * lax.axis_size(CORE) + lax.axis_index(CORE)
    upper_half = shard_place % 2
    seq_place = group_place * (shard_count // 2) + shard_place // 2
    seq_length = lax.dynamic_index_in_dim(lengths, seq_place, 0, keepdims=False)
    local_pos = jnp.arange(tok_rows, dtype=jnp.int32)
    query_pos = upper_half * tok_rows + local_pos
    key_pos = jnp.concatenate([local_pos, query_pos])
    prev_live = jnp.full((tok_rows,), upper_half == 1)
    key_live = jnp.concatenate([prev_live, jnp.ones((tok_rows,), bool)]) & (key_pos < seq_length)
    distance = (query_pos[:, None] - key_pos[None, :]).astype(jnp.float32)
    row_live = (query_pos < seq_length).astype(jnp.float32)[:, None]
    head_size = model_width // HEADS
    score_scale = head_size ** (-0.5)
    slopes = 2.0 ** (-8.0 * (jnp.arange(HEADS, dtype=jnp.float32) + 1.0) / HEADS)
    blocks = lax.axis_size(CORE) * lax.axis_size(OUTER)
    qkv_own = qkv_weight.astype(jnp.bfloat16)
    small_own = small_params.astype(jnp.bfloat16)
    qkv_other, small_other = gather_rows(
        [qkv_own.reshape(blocks, -1, qkv_own.shape[1]), small_rows(small_own, blocks)]
    )
    qkv_full = join_halves(qkv_own, qkv_other.reshape(qkv_own.shape), 0)
    small_full = join_halves(
        small_own, small_other.reshape(-1)[: small_own.size].reshape(small_own.shape), 1
    )
    out_own = out_weight.astype(jnp.bfloat16)
    up_own_t = up_weight.astype(jnp.bfloat16).T
    down_own = down_weight.astype(jnp.bfloat16)
    out_other, up_other_t, down_other = gather_rows(
        [piece.reshape(blocks, -1, piece.shape[1]) for piece in (out_own, up_own_t, down_own)],
    )
    out_full = join_halves(out_own, out_other.reshape(out_own.shape), 0)
    up_full_t = join_blocks(up_own_t, up_other_t.reshape(up_own_t.shape), blocks)
    down_full = join_blocks(down_own, down_other.reshape(down_own.shape), blocks)
    table = small_full.astype(jnp.float32)
    up_bias = ff_order(table[8:12].reshape(FF), blocks)
    normed_one, inverse_one = norm_stats(tokens)
    entry_low = (normed_one * table[0] + table[1]).astype(jnp.bfloat16)
    mapped = jnp.dot(entry_low, qkv_full, preferred_element_type=jnp.float32)
    queries = (mapped[:, :model_width] + table[2]).astype(jnp.bfloat16)
    key_own = mapped[:, model_width : 2 * model_width].astype(jnp.bfloat16)
    value_own = (mapped[:, 2 * model_width :] + table[3]).astype(jnp.bfloat16)
    groups = 4
    per_group = HEADS // groups
    group_width = per_group * (model_width // HEADS)
    query_groups, key_groups, value_groups = [], [], []
    for group in range(groups):
        cols = slice(group * group_width, (group + 1) * group_width)
        received = passed_along(
            jnp.concatenate([key_own[:, cols], value_own[:, cols]], 1), SHARD, 1
        )
        query_groups.append(split_heads_n(queries[:, cols], per_group))
        key_groups.append(
            split_heads_n(jnp.concatenate([received[:, :group_width], key_own[:, cols]], 0), per_group)
        )
        value_groups.append(
            split_heads_n(jnp.concatenate([received[:, group_width:], value_own[:, cols]], 0), per_group)
        )

    info = jnp.stack([upper_half, seq_length]).astype(jnp.int32)
    fwd_parts = []
    for group in range(groups):
        chosen = slice(group * per_group, (group + 1) * per_group)
        fwd_parts.append(
            attention_fwd(
                info,
                slopes[chosen],
                query_groups[group],
                key_groups[group],
                value_groups[group],
                score_scale,
            )
        )
    mixture_heads = jnp.concatenate([part[0] for part in fwd_parts], 0)
    log_total = jnp.concatenate([part[1] for part in fwd_parts], 0)
    attended_low = merge_heads(mixture_heads).astype(jnp.bfloat16)
    resid_one = (
        tokens + jnp.dot(attended_low, out_full, preferred_element_type=jnp.float32) + table[4]
    )
    normed_two, inverse_two = norm_stats(resid_one)
    inner_low = (normed_two * table[5] + table[6]).astype(jnp.bfloat16)
    grad_out = cotangent * row_live
    down_bias_grad = jnp.sum(grad_out, axis=0)
    grad_low = grad_out.astype(jnp.bfloat16)
    pre_act = contract_cols(inner_low, up_full_t) + up_bias
    act_low = gelu_tanh(pre_act).astype(jnp.bfloat16)
    branch_out = jnp.dot(act_low, down_full, preferred_element_type=jnp.float32)
    block_out = resid_one + branch_out + table[7]
    grad_act = contract_cols(grad_low, down_full)
    down_grad = contract_rows(act_low, grad_low)
    grad_pre = gelu_back(pre_act, grad_act)
    up_bias_grad = ff_natural(jnp.sum(grad_pre, axis=0), blocks)
    pre_low = grad_pre.astype(jnp.bfloat16)
    up_grad_t = contract_rows(pre_low, inner_low)
    grad_inner = jnp.dot(pre_low, up_full_t, preferred_element_type=jnp.float32)
    gain_two_grad = jnp.sum(grad_inner * normed_two, axis=0)
    shift_two_grad = jnp.sum(grad_inner, axis=0)
    grad_resid = grad_out + norm_back(grad_inner * table[5], normed_two, inverse_two)
    resid_low = grad_resid.astype(jnp.bfloat16)
    out_grad = contract_rows(attended_low, resid_low)
    grad_resid, resid_low, up_grad_t, down_grad, out_grad = lax.optimization_barrier(
        (grad_resid, resid_low, up_grad_t, down_grad, out_grad)
    )
    out_sum, up_sum_t, down_sum = reduce_rows(
        [split_rows(out_grad), block_major(up_grad_t), block_major(down_grad)]
    )
    out_total = out_sum.reshape(out_weight.shape)
    up_total = up_sum_t.reshape(up_weight.shape[::-1]).T
    down_total = down_sum.reshape(down_weight.shape)
    out_bias_grad = jnp.sum(grad_resid, axis=0)
    grad_mixture = contract_cols(resid_low, out_full).astype(jnp.bfloat16)
    grad_heads = split_heads(grad_mixture)

    query_parts, key_parts, value_parts = [], [], []
    for group in range(groups):
        chosen = slice(group * per_group, (group + 1) * per_group)
        group_query, group_keys, group_values = attention_bwd(
            info,
            slopes[chosen],
            query_groups[group],
            key_groups[group],
            value_groups[group],
            grad_heads[chosen],
            log_total[chosen],
            score_scale,
        )
        returned = passed_along(
            jnp.concatenate(
                [merge_heads(group_keys[:, :tok_rows]), merge_heads(group_values[:, :tok_rows])], 1
            ).astype(jnp.bfloat16),
            SHARD,
            -1,
        ).astype(jnp.float32)
        query_parts.append(merge_heads(group_query))
        key_parts.append(merge_heads(group_keys[:, tok_rows:]) + returned[:, :group_width])
        value_parts.append(merge_heads(group_values[:, tok_rows:]) + returned[:, group_width:])
    grad_query = jnp.concatenate(query_parts, 1)
    grad_key_own = jnp.concatenate(key_parts, 1)
    grad_value_own = jnp.concatenate(value_parts, 1)
    query_bias_grad = jnp.sum(grad_query, axis=0)
    value_bias_grad = jnp.sum(grad_value_own, axis=0)
    mapped_low = jnp.concatenate([grad_query, grad_key_own, grad_value_own], 1).astype(jnp.bfloat16)
    qkv_grad = contract_rows(entry_low, mapped_low)
    grad_entry = contract_cols(mapped_low, qkv_full)
    gain_one_grad = jnp.sum(grad_entry * normed_one, axis=0)
    shift_one_grad = jnp.sum(grad_entry, axis=0)
    input_grad = grad_resid + norm_back(grad_entry * table[0], normed_one, inverse_one)
    head_rows = jnp.stack(
        [
            gain_one_grad,
            shift_one_grad,
            query_bias_grad,
            value_bias_grad,
            out_bias_grad,
            gain_two_grad,
            shift_two_grad,
            down_bias_grad,
        ]
    )
    small_grad = jnp.concatenate([head_rows, up_bias_grad.reshape(4, model_width)], 0)
    small_halves = small_grad.reshape(small_grad.shape[0], shard_count, -1).transpose(1, 0, 2)
    small_packed = jnp.stack(
        [small_rows(small_halves[index], blocks) for index in range(shard_count)]
    ).reshape(shard_count, lax.axis_size(CORE), lax.axis_size(OUTER), 1, SMALL_WIDTH)
    small_packed = small_packed.transpose(1, 2, 0, 3, 4)
    qkv_sum, small_sum = reduce_rows([split_rows(qkv_grad), small_packed])
    qkv_total = qkv_sum.reshape(qkv_weight.shape)
    small_total = small_sum.reshape(-1)[: small_params.size].reshape(small_params.shape)
    rate = 2.0 / math.sqrt(model_width * tok_rows * shard_count * group_count)
    qkv_new = nesterov(qkv_total, qkv_weight, qkv_momentum, qkv_average, rate)
    out_new = nesterov(out_total, out_weight, out_momentum, out_average, rate)
    up_new = nesterov(up_total, up_weight, up_momentum, up_average, rate)
    down_new = nesterov(down_total, down_weight, down_momentum, down_average, rate)
    small_new = nesterov(small_total, small_params, small_momentum, small_average, rate)
    return (
        block_out,
        input_grad,
        qkv_new[0],
        qkv_new[1],
        qkv_new[2],
        out_new[0],
        out_new[1],
        out_new[2],
        up_new[0],
        up_new[1],
        up_new[2],
        down_new[0],
        down_new[1],
        down_new[2],
        small_new[0],
        small_new[1],
        small_new[2],
    )


def solution(mesh):
    cores = 2
    devices = mesh.devices.reshape(mesh.shape["group"] // cores, cores, mesh.shape[SHARD])
    inner_mesh = jax.sharding.Mesh(devices, (OUTER, CORE, SHARD))
    rows = P((OUTER, CORE, SHARD), None)
    in_specs = (
        rows,
        rows,
        P(),
        P(SHARD, None),
        P(SHARD, None),
        P(SHARD, None),
        P(SHARD, None),
        P(SHARD, None),
        P(SHARD, None),
        P(None, SHARD),
        P(None, SHARD),
        P(None, SHARD),
        P(SHARD, None),
        P(SHARD, None),
        P(SHARD, None),
        P(None, SHARD),
        P(None, SHARD),
        P(None, SHARD),
    )
    out_specs = (
        rows,
        rows,
        P(SHARD, None),
        P(SHARD, None),
        P(SHARD, None),
        P(SHARD, None),
        P(SHARD, None),
        P(SHARD, None),
        P(None, SHARD),
        P(None, SHARD),
        P(None, SHARD),
        P(SHARD, None),
        P(SHARD, None),
        P(SHARD, None),
        P(None, SHARD),
        P(None, SHARD),
        P(None, SHARD),
    )

    return jax.shard_map(body, mesh=inner_mesh, in_specs=in_specs, out_specs=out_specs, check_vma=False)
```

```python
import functools
import math

import jax
import jax.numpy as jnp
from jax import lax
from jax.experimental import pallas as pl
from jax.experimental.pallas import tpu as pltpu
from jax.sharding import PartitionSpec as P


HEADS = 16
FF = 4096


EPS = 1e-05
MOMENTUM = 0.9
AVERAGING = 0.9
NEG_FILL = -1e30
SHARD = "shard"
OUTER = "outer"
CORE = "core"


def _scores(info_ref, slope_ref, q, k, score_scale):
    upper = info_ref[0]
    seq_length = info_ref[1]
    rows, cols = q.shape[0], k.shape[0]
    own = cols - rows
    raw = lax.dot_general(q, k, (((1,), (1,)), ((), ())), preferred_element_type=jnp.float32)
    query_pos = upper * rows + lax.broadcasted_iota(jnp.int32, (rows, cols), 0)
    key_index = lax.broadcasted_iota(jnp.int32, (rows, cols), 1)
    key_pos = jnp.where(key_index < own, key_index, upper * rows + key_index - own)
    allowed = ((key_index >= own) | (upper == 1)) & (key_pos < seq_length) & (key_pos <= query_pos)
    distance = (query_pos - key_pos).astype(jnp.float32)
    slope = slope_ref[0][:, 0:1]
    raw = raw * score_scale - slope * distance
    return jnp.where(allowed, raw, NEG_FILL)


def _fwd_kernel(score_scale, info_ref, slope_ref, q_ref, k_ref, v_ref, mix_ref, lse_ref):
    scores = _scores(info_ref, slope_ref, q_ref[0], k_ref[0], score_scale)
    row_top = jnp.max(scores, axis=-1, keepdims=True)
    weights = jnp.exp(scores - row_top)
    row_total = jnp.sum(weights, axis=-1, keepdims=True)
    probs_low = (weights / row_total).astype(jnp.bfloat16)
    mix = jnp.dot(probs_low, v_ref[0], preferred_element_type=jnp.float32)
    mix_ref[0] = mix.astype(mix_ref.dtype)
    lse_ref[0] = row_top + jnp.log(row_total)


def _bwd_kernel(score_scale, info_ref, slope_ref, q_ref, k_ref, v_ref, g_ref, lse_ref, dq_ref, dk_ref, dv_ref):
    q = q_ref[0]
    k = k_ref[0]
    grad = g_ref[0]
    scores = _scores(info_ref, slope_ref, q, k, score_scale)
    probs = jnp.exp(scores - lse_ref[0])
    probs_low = probs.astype(jnp.bfloat16)
    dv_ref[0] = lax.dot_general(probs_low, grad, (((0,), (0,)), ((), ())), preferred_element_type=jnp.float32)
    grad_probs = lax.dot_general(grad, v_ref[0], (((1,), (1,)), ((), ())), preferred_element_type=jnp.float32)
    row_delta = jnp.sum(probs * grad_probs, axis=-1, keepdims=True)
    grad_scores = (probs * (grad_probs - row_delta)).astype(jnp.bfloat16)
    dq_ref[0] = jnp.dot(grad_scores, k, preferred_element_type=jnp.float32) * score_scale
    dk_ref[0] = lax.dot_general(grad_scores, q, (((0,), (0,)), ((), ())), preferred_element_type=jnp.float32) * score_scale


def _slope_rows(slopes):
    return jnp.broadcast_to(slopes[:, None, None], (slopes.shape[0], 1, 128)).astype(jnp.float32)


def attention_fwd(info, slopes, queries, keys, values, score_scale):
    heads, rows, width = queries.shape
    cols = keys.shape[1]
    head_map = lambda h, info_ref: (h, 0, 0)
    flops = 4 * heads * rows * cols * width
    return pl.pallas_call(
        functools.partial(_fwd_kernel, score_scale),
        grid_spec=pltpu.PrefetchScalarGridSpec(
            num_scalar_prefetch=1,
            grid=(heads,),
            in_specs=[
                pl.BlockSpec((1, 1, 128), head_map),
                pl.BlockSpec((1, rows, width), head_map),
                pl.BlockSpec((1, cols, width), head_map),
                pl.BlockSpec((1, cols, width), head_map),
            ],
            out_specs=[
                pl.BlockSpec((1, rows, width), head_map),
                pl.BlockSpec((1, rows, 1), head_map),
            ],
        ),
        out_shape=[
            jax.ShapeDtypeStruct((heads, rows, width), jnp.bfloat16),
            jax.ShapeDtypeStruct((heads, rows, 1), jnp.float32),
        ],
        compiler_params=pltpu.CompilerParams(vmem_limit_bytes=48 * 1024 * 1024),
        cost_estimate=pl.CostEstimate(
            flops=flops, transcendentals=heads * rows * cols, bytes_accessed=2 * heads * (rows + 2 * cols) * width * 2
        ),
    )(info, _slope_rows(slopes), queries, keys, values)


def attention_bwd(info, slopes, queries, keys, values, grads, lse, score_scale):
    heads, rows, width = queries.shape
    cols = keys.shape[1]
    head_map = lambda h, info_ref: (h, 0, 0)
    flops = 8 * heads * rows * cols * width
    return pl.pallas_call(
        functools.partial(_bwd_kernel, score_scale),
        grid_spec=pltpu.PrefetchScalarGridSpec(
            num_scalar_prefetch=1,
            grid=(heads,),
            in_specs=[
                pl.BlockSpec((1, 1, 128), head_map),
                pl.BlockSpec((1, rows, width), head_map),
                pl.BlockSpec((1, cols, width), head_map),
                pl.BlockSpec((1, cols, width), head_map),
                pl.BlockSpec((1, rows, width), head_map),
                pl.BlockSpec((1, rows, 1), head_map),
            ],
            out_specs=[
                pl.BlockSpec((1, rows, width), head_map),
                pl.BlockSpec((1, cols, width), head_map),
                pl.BlockSpec((1, cols, width), head_map),
            ],
        ),
        out_shape=[
            jax.ShapeDtypeStruct((heads, rows, width), jnp.float32),
            jax.ShapeDtypeStruct((heads, cols, width), jnp.float32),
            jax.ShapeDtypeStruct((heads, cols, width), jnp.float32),
        ],
        compiler_params=pltpu.CompilerParams(vmem_limit_bytes=48 * 1024 * 1024),
        cost_estimate=pl.CostEstimate(
            flops=flops, transcendentals=heads * rows * cols, bytes_accessed=heads * (rows + 2 * cols) * width * 6
        ),
    )(info, _slope_rows(slopes), queries, keys, values, grads, lse)


def passed_along(value, axis, steps):
    count = lax.axis_size(axis)
    leading, last = (max(0, -steps), min(count, count - steps))
    return lax.ppermute(value, axis, [(source, source + steps) for source in range(leading, last)])


SMALL_WIDTH = 3072


def small_rows(small_half, blocks):
    flat = small_half.reshape(-1)
    padded = blocks * SMALL_WIDTH
    return jnp.pad(flat, (0, padded - flat.shape[0])).reshape(blocks, 1, SMALL_WIDTH)


def gather_rows(row_arrays):
    cores = lax.axis_size(CORE)
    outer = lax.axis_size(OUTER)
    blocks = cores * outer
    place = lax.axis_index(CORE) * outer + lax.axis_index(OUTER)
    heights = [piece.shape[1] for piece in row_arrays]
    mine = jnp.concatenate(
        [lax.dynamic_index_in_dim(piece, place, 0, keepdims=False) for piece in row_arrays], 0
    )
    other = lax.ppermute(mine, SHARD, [(0, 1), (1, 0)])
    got = lax.all_gather(other, OUTER, axis=0, tiled=False)
    got = lax.all_gather(got, CORE, axis=0, tiled=False)
    got = got.reshape(blocks, -1, got.shape[-1])
    pieces = []
    offset = 0
    for height in heights:
        pieces.append(got[:, offset : offset + height])
        offset += height
    return pieces


def join_halves(own, other, dim):
    upper = lax.axis_index(SHARD) == 1
    in_order = jnp.concatenate([own, other], axis=dim)
    swapped = jnp.concatenate([other, own], axis=dim)
    return jnp.where(upper, swapped, in_order)


def reduce_rows(row_grads):
    shard_count = lax.axis_size(SHARD)
    cores = lax.axis_size(CORE)
    outer = lax.axis_size(OUTER)
    blocks = cores * outer
    heights = [piece.shape[3] for piece in row_grads]
    width = row_grads[0].shape[-1]
    stacked = jnp.concatenate([piece.astype(jnp.bfloat16) for piece in row_grads], 3)
    stacked = stacked.reshape(cores, -1, width)
    stacked = lax.psum_scatter(stacked, CORE, scatter_dimension=0, tiled=True)
    stacked = stacked.reshape(outer, -1, width)
    stacked = lax.psum_scatter(stacked, OUTER, scatter_dimension=0, tiled=True)
    stacked = stacked.reshape(shard_count, -1, width)
    stacked = lax.psum_scatter(stacked, SHARD, scatter_dimension=0, tiled=True)
    stacked = stacked.reshape(stacked.shape[1:])
    stacked = lax.all_gather(stacked, OUTER, axis=0, tiled=True)
    stacked = lax.all_gather(stacked, CORE, axis=0, tiled=True)
    stacked = stacked.reshape(blocks, -1, width)
    pieces = []
    offset = 0
    for height in heights:
        pieces.append(stacked[:, offset : offset + height].astype(jnp.float32))
        offset += height
    return pieces


def split_rows(grad_full):
    shard_count = lax.axis_size(SHARD)
    cores = lax.axis_size(CORE)
    outer = lax.axis_size(OUTER)
    rows, cols = grad_full.shape
    split = grad_full.reshape(shard_count, cores, outer, rows // (shard_count * cores * outer), cols)
    return split.transpose(1, 2, 0, 3, 4)


def block_major(grad_perm):
    shard_count = lax.axis_size(SHARD)
    cores = lax.axis_size(CORE)
    outer = lax.axis_size(OUTER)
    rows, cols = grad_perm.shape
    return grad_perm.reshape(cores, outer, shard_count, rows // (shard_count * cores * outer), cols)


def ff_order(values, blocks):
    shard_count = lax.axis_size(SHARD)
    rest = values.shape[1:]
    split = values.reshape((shard_count, blocks, values.shape[0] // (shard_count * blocks)) + rest)
    return jnp.swapaxes(split, 0, 1).reshape(values.shape)


def ff_natural(values, blocks):
    shard_count = lax.axis_size(SHARD)
    rest = values.shape[1:]
    split = values.reshape((blocks, shard_count, values.shape[0] // (shard_count * blocks)) + rest)
    return jnp.swapaxes(split, 0, 1).reshape(values.shape)


def col_order(values, blocks):
    shard_count = lax.axis_size(SHARD)
    rows, cols = values.shape
    split = values.reshape(rows, shard_count, blocks, cols // (shard_count * blocks))
    return jnp.swapaxes(split, 1, 2).reshape(rows, cols)


def join_blocks(own, other, blocks):
    upper = lax.axis_index(SHARD) == 1
    own_b = own.reshape((blocks, -1) + own.shape[1:])
    other_b = other.reshape((blocks, -1) + other.shape[1:])
    in_order = jnp.stack([own_b, other_b], 1)
    swapped = jnp.stack([other_b, own_b], 1)
    joined = jnp.where(upper, swapped, in_order)
    return joined.reshape((2 * own.shape[0],) + own.shape[1:])


def norm_stats(field_in):
    centred = field_in - jnp.mean(field_in, axis=-1, keepdims=True)
    inverse = lax.rsqrt(jnp.mean(centred * centred, axis=-1, keepdims=True) + EPS)
    return (centred * inverse, inverse)


def norm_back(grad_hat, normed, inverse):
    first_mean = jnp.mean(grad_hat, axis=-1, keepdims=True)
    second_mean = jnp.mean(grad_hat * normed, axis=-1, keepdims=True)
    return inverse * (grad_hat - first_mean - normed * second_mean)


def contract_rows(left_side, right_side):
    return lax.dot_general(
        left_side, right_side, (((0,), (0,)), ((), ())), preferred_element_type=jnp.float32
    )


def contract_cols(left_side, right_side):
    return lax.dot_general(
        left_side, right_side, (((1,), (1,)), ((), ())), preferred_element_type=jnp.float32
    )


def split_heads(field_in):
    return field_in.reshape(field_in.shape[0], HEADS, -1).transpose(1, 0, 2)


def split_heads_n(field_in, heads):
    return field_in.reshape(field_in.shape[0], heads, -1).transpose(1, 0, 2)


def merge_heads(field_in):
    return field_in.transpose(1, 0, 2).reshape(field_in.shape[1], -1)


def gelu_tanh(field_in):
    return jax.nn.gelu(field_in, approximate=True)


def gelu_back(pre_act, grad_act):
    _, pull_back = jax.vjp(gelu_tanh, pre_act)
    return pull_back(grad_act)[0]


def nesterov(grad_total, weight_old, moment_old, average_old, rate):
    moment_new = MOMENTUM * moment_old + grad_total
    weight_new = weight_old - rate * (grad_total + MOMENTUM * moment_new)
    average_new = AVERAGING * average_old + (1.0 - AVERAGING) * weight_new
    return (weight_new, moment_new, average_new)


def body(
    tokens,
    cotangent,
    lengths,
    qkv_weight,
    qkv_momentum,
    qkv_average,
    out_weight,
    out_momentum,
    out_average,
    up_weight,
    up_momentum,
    up_average,
    down_weight,
    down_momentum,
    down_average,
    small_params,
    small_momentum,
    small_average,
):
    tok_rows = tokens.shape[0]
    model_width = tokens.shape[1]
    shard_count = lax.axis_size(SHARD)
    group_count = lax.axis_size(OUTER) * lax.axis_size(CORE)
    shard_place = lax.axis_index(SHARD)
    group_place = lax.axis_index(OUTER) * lax.axis_size(CORE) + lax.axis_index(CORE)
    upper_half = shard_place % 2
    seq_place = group_place * (shard_count // 2) + shard_place // 2
    seq_length = lax.dynamic_index_in_dim(lengths, seq_place, 0, keepdims=False)
    local_pos = jnp.arange(tok_rows, dtype=jnp.int32)
    query_pos = upper_half * tok_rows + local_pos
    key_pos = jnp.concatenate([local_pos, query_pos])
    prev_live = jnp.full((tok_rows,), upper_half == 1)
    key_live = jnp.concatenate([prev_live, jnp.ones((tok_rows,), bool)]) & (key_pos < seq_length)
    distance = (query_pos[:, None] - key_pos[None, :]).astype(jnp.float32)
    row_live = (query_pos < seq_length).astype(jnp.float32)[:, None]
    head_size = model_width // HEADS
    score_scale = head_size ** (-0.5)
    slopes = 2.0 ** (-8.0 * (jnp.arange(HEADS, dtype=jnp.float32) + 1.0) / HEADS)
    blocks = lax.axis_size(CORE) * lax.axis_size(OUTER)
    qkv_own = qkv_weight.astype(jnp.bfloat16)
    small_own = small_params.astype(jnp.bfloat16)
    qkv_other, small_other = gather_rows(
        [qkv_own.reshape(blocks, -1, qkv_own.shape[1]), small_rows(small_own, blocks)]
    )
    qkv_full = join_halves(qkv_own, qkv_other.reshape(qkv_own.shape), 0)
    small_full = join_halves(
        small_own, small_other.reshape(-1)[: small_own.size].reshape(small_own.shape), 1
    )
    out_own = out_weight.astype(jnp.bfloat16)
    up_own_t = up_weight.astype(jnp.bfloat16).T
    down_own = down_weight.astype(jnp.bfloat16)
    out_other, up_other_t, down_other = gather_rows(
        [piece.reshape(blocks, -1, piece.shape[1]) for piece in (out_own, up_own_t, down_own)],
    )
    out_full = join_halves(out_own, out_other.reshape(out_own.shape), 0)
    up_full_t = join_blocks(up_own_t, up_other_t.reshape(up_own_t.shape), blocks)
    down_full = join_blocks(down_own, down_other.reshape(down_own.shape), blocks)
    table = small_full.astype(jnp.float32)
    up_bias = ff_order(table[8:12].reshape(FF), blocks)
    normed_one, inverse_one = norm_stats(tokens)
    entry_low = (normed_one * table[0] + table[1]).astype(jnp.bfloat16)
    mapped = jnp.dot(entry_low, qkv_full, preferred_element_type=jnp.float32)
    queries = (mapped[:, :model_width] + table[2]).astype(jnp.bfloat16)
    key_own = mapped[:, model_width : 2 * model_width].astype(jnp.bfloat16)
    value_own = (mapped[:, 2 * model_width :] + table[3]).astype(jnp.bfloat16)
    groups = 4
    per_group = HEADS // groups
    group_width = per_group * (model_width // HEADS)
    query_groups, key_groups, value_groups = [], [], []
    for group in range(groups):
        cols = slice(group * group_width, (group + 1) * group_width)
        received = passed_along(
            jnp.concatenate([key_own[:, cols], value_own[:, cols]], 1), SHARD, 1
        )
        query_groups.append(split_heads_n(queries[:, cols], per_group))
        key_groups.append(
            split_heads_n(jnp.concatenate([received[:, :group_width], key_own[:, cols]], 0), per_group)
        )
        value_groups.append(
            split_heads_n(jnp.concatenate([received[:, group_width:], value_own[:, cols]], 0), per_group)
        )

    info = jnp.stack([upper_half, seq_length]).astype(jnp.int32)
    fwd_parts = []
    for group in range(groups):
        chosen = slice(group * per_group, (group + 1) * per_group)
        fwd_parts.append(
            attention_fwd(
                info,
                slopes[chosen],
                query_groups[group],
                key_groups[group],
                value_groups[group],
                score_scale,
            )
        )
    mixture_heads = jnp.concatenate([part[0] for part in fwd_parts], 0)
    log_total = jnp.concatenate([part[1] for part in fwd_parts], 0)
    attended_low = merge_heads(mixture_heads).astype(jnp.bfloat16)
    resid_one = (
        tokens + jnp.dot(attended_low, out_full, preferred_element_type=jnp.float32) + table[4]
    )
    normed_two, inverse_two = norm_stats(resid_one)
    inner_low = (normed_two * table[5] + table[6]).astype(jnp.bfloat16)
    grad_out = cotangent * row_live
    down_bias_grad = jnp.sum(grad_out, axis=0)
    grad_low = grad_out.astype(jnp.bfloat16)
    pre_act = contract_cols(inner_low, up_full_t) + up_bias
    act_low = gelu_tanh(pre_act).astype(jnp.bfloat16)
    branch_out = jnp.dot(act_low, down_full, preferred_element_type=jnp.float32)
    block_out = resid_one + branch_out + table[7]
    grad_act = contract_cols(grad_low, down_full)
    down_grad = contract_rows(act_low, grad_low)
    grad_pre = gelu_back(pre_act, grad_act)
    up_bias_grad = ff_natural(jnp.sum(grad_pre, axis=0), blocks)
    pre_low = grad_pre.astype(jnp.bfloat16)
    up_grad_t = contract_rows(pre_low, inner_low)
    grad_inner = jnp.dot(pre_low, up_full_t, preferred_element_type=jnp.float32)
    gain_two_grad = jnp.sum(grad_inner * normed_two, axis=0)
    shift_two_grad = jnp.sum(grad_inner, axis=0)
    grad_resid = grad_out + norm_back(grad_inner * table[5], normed_two, inverse_two)
    resid_low = grad_resid.astype(jnp.bfloat16)
    out_grad = contract_rows(attended_low, resid_low)
    grad_resid, resid_low, up_grad_t, down_grad, out_grad = lax.optimization_barrier(
        (grad_resid, resid_low, up_grad_t, down_grad, out_grad)
    )
    out_sum, up_sum_t, down_sum = reduce_rows(
        [split_rows(out_grad), block_major(up_grad_t), block_major(down_grad)]
    )
    out_total = out_sum.reshape(out_weight.shape)
    up_total = up_sum_t.reshape(up_weight.shape[::-1]).T
    down_total = down_sum.reshape(down_weight.shape)
    out_bias_grad = jnp.sum(grad_resid, axis=0)
    grad_mixture = contract_cols(resid_low, out_full).astype(jnp.bfloat16)
    grad_heads = split_heads(grad_mixture)

    query_parts, key_parts, value_parts = [], [], []
    for group in range(groups):
        chosen = slice(group * per_group, (group + 1) * per_group)
        group_query, group_keys, group_values = attention_bwd(
            info,
            slopes[chosen],
            query_groups[group],
            key_groups[group],
            value_groups[group],
            grad_heads[chosen],
            log_total[chosen],
            score_scale,
        )
        returned = passed_along(
            jnp.concatenate(
                [merge_heads(group_keys[:, :tok_rows]), merge_heads(group_values[:, :tok_rows])], 1
            ).astype(jnp.bfloat16),
            SHARD,
            -1,
        ).astype(jnp.float32)
        query_parts.append(merge_heads(group_query))
        key_parts.append(merge_heads(group_keys[:, tok_rows:]) + returned[:, :group_width])
        value_parts.append(merge_heads(group_values[:, tok_rows:]) + returned[:, group_width:])
    grad_query = jnp.concatenate(query_parts, 1)
    grad_key_own = jnp.concatenate(key_parts, 1)
    grad_value_own = jnp.concatenate(value_parts, 1)
    query_bias_grad = jnp.sum(grad_query, axis=0)
    value_bias_grad = jnp.sum(grad_value_own, axis=0)
    mapped_low = jnp.concatenate([grad_query, grad_key_own, grad_value_own], 1).astype(jnp.bfloat16)
    qkv_grad = contract_rows(col_order(entry_low, blocks), mapped_low)
    grad_entry = contract_cols(mapped_low, qkv_full)
    gain_one_grad = jnp.sum(grad_entry * normed_one, axis=0)
    shift_one_grad = jnp.sum(grad_entry, axis=0)
    input_grad = grad_resid + norm_back(grad_entry * table[0], normed_one, inverse_one)
    head_rows = jnp.stack(
        [
            gain_one_grad,
            shift_one_grad,
            query_bias_grad,
            value_bias_grad,
            out_bias_grad,
            gain_two_grad,
            shift_two_grad,
            down_bias_grad,
        ]
    )
    small_grad = jnp.concatenate([head_rows, up_bias_grad.reshape(4, model_width)], 0)
    small_halves = small_grad.reshape(small_grad.shape[0], shard_count, -1).transpose(1, 0, 2)
    small_packed = jnp.stack(
        [small_rows(small_halves[index], blocks) for index in range(shard_count)]
    ).reshape(shard_count, lax.axis_size(CORE), lax.axis_size(OUTER), 1, SMALL_WIDTH)
    small_packed = small_packed.transpose(1, 2, 0, 3, 4)
    qkv_sum, small_sum = reduce_rows([block_major(qkv_grad), small_packed])
    qkv_total = qkv_sum.reshape(qkv_weight.shape)
    small_total = small_sum.reshape(-1)[: small_params.size].reshape(small_params.shape)
    rate = 2.0 / math.sqrt(model_width * tok_rows * shard_count * group_count)
    qkv_new = nesterov(qkv_total, qkv_weight, qkv_momentum, qkv_average, rate)
    out_new = nesterov(out_total, out_weight, out_momentum, out_average, rate)
    up_new = nesterov(up_total, up_weight, up_momentum, up_average, rate)
    down_new = nesterov(down_total, down_weight, down_momentum, down_average, rate)
    small_new = nesterov(small_total, small_params, small_momentum, small_average, rate)
    return (
        block_out,
        input_grad,
        qkv_new[0],
        qkv_new[1],
        qkv_new[2],
        out_new[0],
        out_new[1],
        out_new[2],
        up_new[0],
        up_new[1],
        up_new[2],
        down_new[0],
        down_new[1],
        down_new[2],
        small_new[0],
        small_new[1],
        small_new[2],
    )


def solution(mesh):
    cores = 2
    devices = mesh.devices.reshape(mesh.shape["group"] // cores, cores, mesh.shape[SHARD])
    inner_mesh = jax.sharding.Mesh(devices, (OUTER, CORE, SHARD))
    rows = P((OUTER, CORE, SHARD), None)
    in_specs = (
        rows,
        rows,
        P(),
        P(SHARD, None),
        P(SHARD, None),
        P(SHARD, None),
        P(SHARD, None),
        P(SHARD, None),
        P(SHARD, None),
        P(None, SHARD),
        P(None, SHARD),
        P(None, SHARD),
        P(SHARD, None),
        P(SHARD, None),
        P(SHARD, None),
        P(None, SHARD),
        P(None, SHARD),
        P(None, SHARD),
    )
    out_specs = (
        rows,
        rows,
        P(SHARD, None),
        P(SHARD, None),
        P(SHARD, None),
        P(SHARD, None),
        P(SHARD, None),
        P(SHARD, None),
        P(None, SHARD),
        P(None, SHARD),
        P(None, SHARD),
        P(SHARD, None),
        P(SHARD, None),
        P(SHARD, None),
        P(None, SHARD),
        P(None, SHARD),
        P(None, SHARD),
    )

    return jax.shard_map(body, mesh=inner_mesh, in_specs=in_specs, out_specs=out_specs, check_vma=False)
```

```python
import functools
import math

import jax
import jax.numpy as jnp
from jax import lax
from jax.experimental import pallas as pl
from jax.experimental.pallas import tpu as pltpu
from jax.sharding import PartitionSpec as P


HEADS = 16
FF = 4096


EPS = 1e-05
MOMENTUM = 0.9
AVERAGING = 0.9
NEG_FILL = -1e30
SHARD = "shard"
OUTER = "outer"
CORE = "core"


def _scores(info_ref, slope_ref, q, k, score_scale):
    upper = info_ref[0]
    seq_length = info_ref[1]
    rows, cols = q.shape[0], k.shape[0]
    own = cols - rows
    raw = lax.dot_general(q, k, (((1,), (1,)), ((), ())), preferred_element_type=jnp.float32)
    query_pos = upper * rows + lax.broadcasted_iota(jnp.int32, (rows, cols), 0)
    key_index = lax.broadcasted_iota(jnp.int32, (rows, cols), 1)
    key_pos = jnp.where(key_index < own, key_index, upper * rows + key_index - own)
    allowed = ((key_index >= own) | (upper == 1)) & (key_pos < seq_length) & (key_pos <= query_pos)
    distance = (query_pos - key_pos).astype(jnp.float32)
    slope = slope_ref[0][:, 0:1]
    raw = raw * score_scale - slope * distance
    return jnp.where(allowed, raw, NEG_FILL)


def _fwd_kernel(score_scale, info_ref, slope_ref, q_ref, k_ref, v_ref, mix_ref, lse_ref):
    scores = _scores(info_ref, slope_ref, q_ref[0], k_ref[0], score_scale)
    row_top = jnp.max(scores, axis=-1, keepdims=True)
    weights = jnp.exp(scores - row_top)
    row_total = jnp.sum(weights, axis=-1, keepdims=True)
    probs_low = (weights / row_total).astype(jnp.bfloat16)
    mix = jnp.dot(probs_low, v_ref[0], preferred_element_type=jnp.float32)
    mix_ref[0] = mix.astype(mix_ref.dtype)
    lse_ref[0] = row_top + jnp.log(row_total)


def _bwd_kernel(score_scale, info_ref, slope_ref, q_ref, k_ref, v_ref, g_ref, lse_ref, dq_ref, dk_ref, dv_ref):
    q = q_ref[0]
    k = k_ref[0]
    grad = g_ref[0]
    scores = _scores(info_ref, slope_ref, q, k, score_scale)
    probs = jnp.exp(scores - lse_ref[0])
    probs_low = probs.astype(jnp.bfloat16)
    dv_ref[0] = lax.dot_general(probs_low, grad, (((0,), (0,)), ((), ())), preferred_element_type=jnp.float32)
    grad_probs = lax.dot_general(grad, v_ref[0], (((1,), (1,)), ((), ())), preferred_element_type=jnp.float32)
    row_delta = jnp.sum(probs * grad_probs, axis=-1, keepdims=True)
    grad_scores = (probs * (grad_probs - row_delta)).astype(jnp.bfloat16)
    dq_ref[0] = jnp.dot(grad_scores, k, preferred_element_type=jnp.float32) * score_scale
    dk_ref[0] = lax.dot_general(grad_scores, q, (((0,), (0,)), ((), ())), preferred_element_type=jnp.float32) * score_scale


def _slope_rows(slopes):
    return jnp.broadcast_to(slopes[:, None, None], (slopes.shape[0], 1, 128)).astype(jnp.float32)


def attention_fwd(info, slopes, queries, keys, values, score_scale):
    heads, rows, width = queries.shape
    cols = keys.shape[1]
    head_map = lambda h, info_ref: (h, 0, 0)
    flops = 4 * heads * rows * cols * width
    return pl.pallas_call(
        functools.partial(_fwd_kernel, score_scale),
        grid_spec=pltpu.PrefetchScalarGridSpec(
            num_scalar_prefetch=1,
            grid=(heads,),
            in_specs=[
                pl.BlockSpec((1, 1, 128), head_map),
                pl.BlockSpec((1, rows, width), head_map),
                pl.BlockSpec((1, cols, width), head_map),
                pl.BlockSpec((1, cols, width), head_map),
            ],
            out_specs=[
                pl.BlockSpec((1, rows, width), head_map),
                pl.BlockSpec((1, rows, 1), head_map),
            ],
        ),
        out_shape=[
            jax.ShapeDtypeStruct((heads, rows, width), jnp.bfloat16),
            jax.ShapeDtypeStruct((heads, rows, 1), jnp.float32),
        ],
        compiler_params=pltpu.CompilerParams(vmem_limit_bytes=48 * 1024 * 1024),
        cost_estimate=pl.CostEstimate(
            flops=flops, transcendentals=heads * rows * cols, bytes_accessed=2 * heads * (rows + 2 * cols) * width * 2
        ),
    )(info, _slope_rows(slopes), queries, keys, values)


def attention_bwd(info, slopes, queries, keys, values, grads, lse, score_scale):
    heads, rows, width = queries.shape
    cols = keys.shape[1]
    head_map = lambda h, info_ref: (h, 0, 0)
    flops = 8 * heads * rows * cols * width
    return pl.pallas_call(
        functools.partial(_bwd_kernel, score_scale),
        grid_spec=pltpu.PrefetchScalarGridSpec(
            num_scalar_prefetch=1,
            grid=(heads,),
            in_specs=[
                pl.BlockSpec((1, 1, 128), head_map),
                pl.BlockSpec((1, rows, width), head_map),
                pl.BlockSpec((1, cols, width), head_map),
                pl.BlockSpec((1, cols, width), head_map),
                pl.BlockSpec((1, rows, width), head_map),
                pl.BlockSpec((1, rows, 1), head_map),
            ],
            out_specs=[
                pl.BlockSpec((1, rows, width), head_map),
                pl.BlockSpec((1, cols, width), head_map),
                pl.BlockSpec((1, cols, width), head_map),
            ],
        ),
        out_shape=[
            jax.ShapeDtypeStruct((heads, rows, width), jnp.float32),
            jax.ShapeDtypeStruct((heads, cols, width), jnp.float32),
            jax.ShapeDtypeStruct((heads, cols, width), jnp.float32),
        ],
        compiler_params=pltpu.CompilerParams(vmem_limit_bytes=48 * 1024 * 1024),
        cost_estimate=pl.CostEstimate(
            flops=flops, transcendentals=heads * rows * cols, bytes_accessed=heads * (rows + 2 * cols) * width * 6
        ),
    )(info, _slope_rows(slopes), queries, keys, values, grads, lse)


def passed_along(value, axis, steps):
    count = lax.axis_size(axis)
    leading, last = (max(0, -steps), min(count, count - steps))
    return lax.ppermute(value, axis, [(source, source + steps) for source in range(leading, last)])


SMALL_WIDTH = 3072


def small_rows(small_half, blocks):
    flat = small_half.reshape(-1)
    padded = blocks * SMALL_WIDTH
    return jnp.pad(flat, (0, padded - flat.shape[0])).reshape(blocks, 1, SMALL_WIDTH)


def gather_ring(piece, axis):
    count = lax.axis_size(axis)
    place = lax.axis_index(axis)
    held = piece[None]
    step = 1
    while step < count:
        received = lax.ppermute(held, axis, [(index, index ^ step) for index in range(count)])
        first = (place & step) == 0
        held = jnp.where(
            first, jnp.concatenate([held, received], 0), jnp.concatenate([received, held], 0)
        )
        step *= 2
    return held


def gather_rows(row_arrays, on_dma=False):
    cores = lax.axis_size(CORE)
    outer = lax.axis_size(OUTER)
    blocks = cores * outer
    place = lax.axis_index(CORE) * outer + lax.axis_index(OUTER)
    heights = [piece.shape[1] for piece in row_arrays]
    mine = jnp.concatenate(
        [lax.dynamic_index_in_dim(piece, place, 0, keepdims=False) for piece in row_arrays], 0
    )
    other = lax.ppermute(mine, SHARD, [(0, 1), (1, 0)])
    if on_dma:
        got = gather_ring(gather_ring(other, OUTER), CORE)
    else:
        got = lax.all_gather(other, OUTER, axis=0, tiled=False)
        got = lax.all_gather(got, CORE, axis=0, tiled=False)
    got = got.reshape(blocks, -1, got.shape[-1])
    pieces = []
    offset = 0
    for height in heights:
        pieces.append(got[:, offset : offset + height])
        offset += height
    return pieces


def join_halves(own, other, dim):
    upper = lax.axis_index(SHARD) == 1
    in_order = jnp.concatenate([own, other], axis=dim)
    swapped = jnp.concatenate([other, own], axis=dim)
    return jnp.where(upper, swapped, in_order)


def reduce_rows(row_grads):
    shard_count = lax.axis_size(SHARD)
    cores = lax.axis_size(CORE)
    outer = lax.axis_size(OUTER)
    blocks = cores * outer
    heights = [piece.shape[3] for piece in row_grads]
    width = row_grads[0].shape[-1]
    stacked = jnp.concatenate([piece.astype(jnp.bfloat16) for piece in row_grads], 3)
    stacked = stacked.reshape(cores, -1, width)
    stacked = lax.psum_scatter(stacked, CORE, scatter_dimension=0, tiled=True)
    stacked = stacked.reshape(outer, -1, width)
    stacked = lax.psum_scatter(stacked, OUTER, scatter_dimension=0, tiled=True)
    stacked = stacked.reshape(shard_count, -1, width)
    stacked = lax.psum_scatter(stacked, SHARD, scatter_dimension=0, tiled=True)
    stacked = stacked.reshape(stacked.shape[1:])
    stacked = lax.all_gather(stacked, OUTER, axis=0, tiled=True)
    stacked = lax.all_gather(stacked, CORE, axis=0, tiled=True)
    stacked = stacked.reshape(blocks, -1, width)
    pieces = []
    offset = 0
    for height in heights:
        pieces.append(stacked[:, offset : offset + height].astype(jnp.float32))
        offset += height
    return pieces


def split_rows(grad_full):
    shard_count = lax.axis_size(SHARD)
    cores = lax.axis_size(CORE)
    outer = lax.axis_size(OUTER)
    rows, cols = grad_full.shape
    split = grad_full.reshape(shard_count, cores, outer, rows // (shard_count * cores * outer), cols)
    return split.transpose(1, 2, 0, 3, 4)


def block_major(grad_perm):
    shard_count = lax.axis_size(SHARD)
    cores = lax.axis_size(CORE)
    outer = lax.axis_size(OUTER)
    rows, cols = grad_perm.shape
    return grad_perm.reshape(cores, outer, shard_count, rows // (shard_count * cores * outer), cols)


def ff_order(values, blocks):
    shard_count = lax.axis_size(SHARD)
    rest = values.shape[1:]
    split = values.reshape((shard_count, blocks, values.shape[0] // (shard_count * blocks)) + rest)
    return jnp.swapaxes(split, 0, 1).reshape(values.shape)


def ff_natural(values, blocks):
    shard_count = lax.axis_size(SHARD)
    rest = values.shape[1:]
    split = values.reshape((blocks, shard_count, values.shape[0] // (shard_count * blocks)) + rest)
    return jnp.swapaxes(split, 0, 1).reshape(values.shape)


def join_blocks(own, other, blocks):
    upper = lax.axis_index(SHARD) == 1
    own_b = own.reshape((blocks, -1) + own.shape[1:])
    other_b = other.reshape((blocks, -1) + other.shape[1:])
    in_order = jnp.stack([own_b, other_b], 1)
    swapped = jnp.stack([other_b, own_b], 1)
    joined = jnp.where(upper, swapped, in_order)
    return joined.reshape((2 * own.shape[0],) + own.shape[1:])


def norm_stats(field_in):
    centred = field_in - jnp.mean(field_in, axis=-1, keepdims=True)
    inverse = lax.rsqrt(jnp.mean(centred * centred, axis=-1, keepdims=True) + EPS)
    return (centred * inverse, inverse)


def norm_back(grad_hat, normed, inverse):
    first_mean = jnp.mean(grad_hat, axis=-1, keepdims=True)
    second_mean = jnp.mean(grad_hat * normed, axis=-1, keepdims=True)
    return inverse * (grad_hat - first_mean - normed * second_mean)


def contract_rows(left_side, right_side):
    return lax.dot_general(
        left_side, right_side, (((0,), (0,)), ((), ())), preferred_element_type=jnp.float32
    )


def contract_cols(left_side, right_side):
    return lax.dot_general(
        left_side, right_side, (((1,), (1,)), ((), ())), preferred_element_type=jnp.float32
    )


def split_heads(field_in):
    return field_in.reshape(field_in.shape[0], HEADS, -1).transpose(1, 0, 2)


def split_heads_n(field_in, heads):
    return field_in.reshape(field_in.shape[0], heads, -1).transpose(1, 0, 2)


def merge_heads(field_in):
    return field_in.transpose(1, 0, 2).reshape(field_in.shape[1], -1)


def gelu_tanh(field_in):
    return jax.nn.gelu(field_in, approximate=True)


def gelu_back(pre_act, grad_act):
    _, pull_back = jax.vjp(gelu_tanh, pre_act)
    return pull_back(grad_act)[0]


def nesterov(grad_total, weight_old, moment_old, average_old, rate):
    moment_new = MOMENTUM * moment_old + grad_total
    weight_new = weight_old - rate * (grad_total + MOMENTUM * moment_new)
    average_new = AVERAGING * average_old + (1.0 - AVERAGING) * weight_new
    return (weight_new, moment_new, average_new)


def body(
    tokens,
    cotangent,
    lengths,
    qkv_weight,
    qkv_momentum,
    qkv_average,
    out_weight,
    out_momentum,
    out_average,
    up_weight,
    up_momentum,
    up_average,
    down_weight,
    down_momentum,
    down_average,
    small_params,
    small_momentum,
    small_average,
):
    tok_rows = tokens.shape[0]
    model_width = tokens.shape[1]
    shard_count = lax.axis_size(SHARD)
    group_count = lax.axis_size(OUTER) * lax.axis_size(CORE)
    shard_place = lax.axis_index(SHARD)
    group_place = lax.axis_index(OUTER) * lax.axis_size(CORE) + lax.axis_index(CORE)
    upper_half = shard_place % 2
    seq_place = group_place * (shard_count // 2) + shard_place // 2
    seq_length = lax.dynamic_index_in_dim(lengths, seq_place, 0, keepdims=False)
    local_pos = jnp.arange(tok_rows, dtype=jnp.int32)
    query_pos = upper_half * tok_rows + local_pos
    key_pos = jnp.concatenate([local_pos, query_pos])
    prev_live = jnp.full((tok_rows,), upper_half == 1)
    key_live = jnp.concatenate([prev_live, jnp.ones((tok_rows,), bool)]) & (key_pos < seq_length)
    distance = (query_pos[:, None] - key_pos[None, :]).astype(jnp.float32)
    row_live = (query_pos < seq_length).astype(jnp.float32)[:, None]
    head_size = model_width // HEADS
    score_scale = head_size ** (-0.5)
    slopes = 2.0 ** (-8.0 * (jnp.arange(HEADS, dtype=jnp.float32) + 1.0) / HEADS)
    blocks = lax.axis_size(CORE) * lax.axis_size(OUTER)
    qkv_own = qkv_weight.astype(jnp.bfloat16)
    small_own = small_params.astype(jnp.bfloat16)
    qkv_other, small_other = gather_rows(
        [qkv_own.reshape(blocks, -1, qkv_own.shape[1]), small_rows(small_own, blocks)], on_dma=True
    )
    qkv_full = join_halves(qkv_own, qkv_other.reshape(qkv_own.shape), 0)
    small_full = join_halves(
        small_own, small_other.reshape(-1)[: small_own.size].reshape(small_own.shape), 1
    )
    out_own = out_weight.astype(jnp.bfloat16)
    up_own_t = up_weight.astype(jnp.bfloat16).T
    down_own = down_weight.astype(jnp.bfloat16)
    out_other, up_other_t, down_other = gather_rows(
        [piece.reshape(blocks, -1, piece.shape[1]) for piece in (out_own, up_own_t, down_own)],
    )
    out_full = join_halves(out_own, out_other.reshape(out_own.shape), 0)
    up_full_t = join_blocks(up_own_t, up_other_t.reshape(up_own_t.shape), blocks)
    down_full = join_blocks(down_own, down_other.reshape(down_own.shape), blocks)
    table = small_full.astype(jnp.float32)
    up_bias = ff_order(table[8:12].reshape(FF), blocks)
    normed_one, inverse_one = norm_stats(tokens)
    entry_low = (normed_one * table[0] + table[1]).astype(jnp.bfloat16)
    mapped = jnp.dot(entry_low, qkv_full, preferred_element_type=jnp.float32)
    queries = (mapped[:, :model_width] + table[2]).astype(jnp.bfloat16)
    key_own = mapped[:, model_width : 2 * model_width].astype(jnp.bfloat16)
    value_own = (mapped[:, 2 * model_width :] + table[3]).astype(jnp.bfloat16)
    groups = 4
    per_group = HEADS // groups
    group_width = per_group * (model_width // HEADS)
    query_groups, key_groups, value_groups = [], [], []
    for group in range(groups):
        cols = slice(group * group_width, (group + 1) * group_width)
        received = passed_along(
            jnp.concatenate([key_own[:, cols], value_own[:, cols]], 1), SHARD, 1
        )
        query_groups.append(split_heads_n(queries[:, cols], per_group))
        key_groups.append(
            split_heads_n(jnp.concatenate([received[:, :group_width], key_own[:, cols]], 0), per_group)
        )
        value_groups.append(
            split_heads_n(jnp.concatenate([received[:, group_width:], value_own[:, cols]], 0), per_group)
        )

    info = jnp.stack([upper_half, seq_length]).astype(jnp.int32)
    fwd_parts = []
    for group in range(groups):
        chosen = slice(group * per_group, (group + 1) * per_group)
        fwd_parts.append(
            attention_fwd(
                info,
                slopes[chosen],
                query_groups[group],
                key_groups[group],
                value_groups[group],
                score_scale,
            )
        )
    mixture_heads = jnp.concatenate([part[0] for part in fwd_parts], 0)
    log_total = jnp.concatenate([part[1] for part in fwd_parts], 0)
    attended_low = merge_heads(mixture_heads).astype(jnp.bfloat16)
    resid_one = (
        tokens + jnp.dot(attended_low, out_full, preferred_element_type=jnp.float32) + table[4]
    )
    normed_two, inverse_two = norm_stats(resid_one)
    inner_low = (normed_two * table[5] + table[6]).astype(jnp.bfloat16)
    grad_out = cotangent * row_live
    down_bias_grad = jnp.sum(grad_out, axis=0)
    grad_low = grad_out.astype(jnp.bfloat16)
    pre_act = contract_cols(inner_low, up_full_t) + up_bias
    act_low = gelu_tanh(pre_act).astype(jnp.bfloat16)
    branch_out = jnp.dot(act_low, down_full, preferred_element_type=jnp.float32)
    block_out = resid_one + branch_out + table[7]
    grad_act = contract_cols(grad_low, down_full)
    down_grad = contract_rows(act_low, grad_low)
    grad_pre = gelu_back(pre_act, grad_act)
    up_bias_grad = ff_natural(jnp.sum(grad_pre, axis=0), blocks)
    pre_low = grad_pre.astype(jnp.bfloat16)
    up_grad_t = contract_rows(pre_low, inner_low)
    grad_inner = jnp.dot(pre_low, up_full_t, preferred_element_type=jnp.float32)
    gain_two_grad = jnp.sum(grad_inner * normed_two, axis=0)
    shift_two_grad = jnp.sum(grad_inner, axis=0)
    grad_resid = grad_out + norm_back(grad_inner * table[5], normed_two, inverse_two)
    resid_low = grad_resid.astype(jnp.bfloat16)
    out_grad = contract_rows(attended_low, resid_low)
    grad_resid, resid_low, up_grad_t, down_grad, out_grad = lax.optimization_barrier(
        (grad_resid, resid_low, up_grad_t, down_grad, out_grad)
    )
    out_sum, up_sum_t, down_sum = reduce_rows(
        [split_rows(out_grad), block_major(up_grad_t), block_major(down_grad)]
    )
    out_total = out_sum.reshape(out_weight.shape)
    up_total = up_sum_t.reshape(up_weight.shape[::-1]).T
    down_total = down_sum.reshape(down_weight.shape)
    out_bias_grad = jnp.sum(grad_resid, axis=0)
    grad_mixture = contract_cols(resid_low, out_full).astype(jnp.bfloat16)
    grad_heads = split_heads(grad_mixture)

    query_parts, key_parts, value_parts = [], [], []
    for group in range(groups):
        chosen = slice(group * per_group, (group + 1) * per_group)
        group_query, group_keys, group_values = attention_bwd(
            info,
            slopes[chosen],
            query_groups[group],
            key_groups[group],
            value_groups[group],
            grad_heads[chosen],
            log_total[chosen],
            score_scale,
        )
        returned = passed_along(
            jnp.concatenate(
                [merge_heads(group_keys[:, :tok_rows]), merge_heads(group_values[:, :tok_rows])], 1
            ).astype(jnp.bfloat16),
            SHARD,
            -1,
        ).astype(jnp.float32)
        query_parts.append(merge_heads(group_query))
        key_parts.append(merge_heads(group_keys[:, tok_rows:]) + returned[:, :group_width])
        value_parts.append(merge_heads(group_values[:, tok_rows:]) + returned[:, group_width:])
    grad_query = jnp.concatenate(query_parts, 1)
    grad_key_own = jnp.concatenate(key_parts, 1)
    grad_value_own = jnp.concatenate(value_parts, 1)
    query_bias_grad = jnp.sum(grad_query, axis=0)
    value_bias_grad = jnp.sum(grad_value_own, axis=0)
    mapped_low = jnp.concatenate([grad_query, grad_key_own, grad_value_own], 1).astype(jnp.bfloat16)
    qkv_grad = contract_rows(entry_low, mapped_low)
    grad_entry = contract_cols(mapped_low, qkv_full)
    gain_one_grad = jnp.sum(grad_entry * normed_one, axis=0)
    shift_one_grad = jnp.sum(grad_entry, axis=0)
    input_grad = grad_resid + norm_back(grad_entry * table[0], normed_one, inverse_one)
    head_rows = jnp.stack(
        [
            gain_one_grad,
            shift_one_grad,
            query_bias_grad,
            value_bias_grad,
            out_bias_grad,
            gain_two_grad,
            shift_two_grad,
            down_bias_grad,
        ]
    )
    small_grad = jnp.concatenate([head_rows, up_bias_grad.reshape(4, model_width)], 0)
    small_halves = small_grad.reshape(small_grad.shape[0], shard_count, -1).transpose(1, 0, 2)
    small_packed = jnp.stack(
        [small_rows(small_halves[index], blocks) for index in range(shard_count)]
    ).reshape(shard_count, lax.axis_size(CORE), lax.axis_size(OUTER), 1, SMALL_WIDTH)
    small_packed = small_packed.transpose(1, 2, 0, 3, 4)
    qkv_sum, small_sum = reduce_rows([split_rows(qkv_grad), small_packed])
    qkv_total = qkv_sum.reshape(qkv_weight.shape)
    small_total = small_sum.reshape(-1)[: small_params.size].reshape(small_params.shape)
    rate = 2.0 / math.sqrt(model_width * tok_rows * shard_count * group_count)
    qkv_new = nesterov(qkv_total, qkv_weight, qkv_momentum, qkv_average, rate)
    out_new = nesterov(out_total, out_weight, out_momentum, out_average, rate)
    up_new = nesterov(up_total, up_weight, up_momentum, up_average, rate)
    down_new = nesterov(down_total, down_weight, down_momentum, down_average, rate)
    small_new = nesterov(small_total, small_params, small_momentum, small_average, rate)
    return (
        block_out,
        input_grad,
        qkv_new[0],
        qkv_new[1],
        qkv_new[2],
        out_new[0],
        out_new[1],
        out_new[2],
        up_new[0],
        up_new[1],
        up_new[2],
        down_new[0],
        down_new[1],
        down_new[2],
        small_new[0],
        small_new[1],
        small_new[2],
    )


def solution(mesh):
    cores = 2
    devices = mesh.devices.reshape(mesh.shape["group"] // cores, cores, mesh.shape[SHARD])
    inner_mesh = jax.sharding.Mesh(devices, (OUTER, CORE, SHARD))
    rows = P((OUTER, CORE, SHARD), None)
    in_specs = (
        rows,
        rows,
        P(),
        P(SHARD, None),
        P(SHARD, None),
        P(SHARD, None),
        P(SHARD, None),
        P(SHARD, None),
        P(SHARD, None),
        P(None, SHARD),
        P(None, SHARD),
        P(None, SHARD),
        P(SHARD, None),
        P(SHARD, None),
        P(SHARD, None),
        P(None, SHARD),
        P(None, SHARD),
        P(None, SHARD),
    )
    out_specs = (
        rows,
        rows,
        P(SHARD, None),
        P(SHARD, None),
        P(SHARD, None),
        P(SHARD, None),
        P(SHARD, None),
        P(SHARD, None),
        P(None, SHARD),
        P(None, SHARD),
        P(None, SHARD),
        P(SHARD, None),
        P(SHARD, None),
        P(SHARD, None),
        P(None, SHARD),
        P(None, SHARD),
        P(None, SHARD),
    )

    return jax.shard_map(body, mesh=inner_mesh, in_specs=in_specs, out_specs=out_specs, check_vma=False)
```

```python
import functools
import math

import jax
import jax.numpy as jnp
from jax import lax
from jax.experimental import pallas as pl
from jax.experimental.pallas import tpu as pltpu
from jax.sharding import PartitionSpec as P


HEADS = 16
FF = 4096


EPS = 1e-05
MOMENTUM = 0.9
AVERAGING = 0.9
NEG_FILL = -1e30
SHARD = "shard"
OUTER = "outer"
CORE = "core"


HEAD = 64
PAIR = 128


def pair_scores(info_ref, slope, q, k, score_scale):
    upper = info_ref[0]
    seq_length = info_ref[1]
    rows, cols = q.shape[0], k.shape[0]
    own = cols - rows
    raw = lax.dot_general(q, k, (((1,), (1,)), ((), ())), preferred_element_type=jnp.float32)
    query_pos = upper * rows + lax.broadcasted_iota(jnp.int32, (rows, cols), 0)
    key_index = lax.broadcasted_iota(jnp.int32, (rows, cols), 1)
    key_pos = jnp.where(key_index < own, key_index, upper * rows + key_index - own)
    allowed = ((key_index >= own) | (upper == 1)) & (key_pos < seq_length) & (key_pos <= query_pos)
    distance = (query_pos - key_pos).astype(jnp.float32)
    raw = raw * score_scale - slope * distance
    return jnp.where(allowed, raw, NEG_FILL)


def pair_fwd_kernel(score_scale, info_ref, slope_ref, q_ref, kr_ref, ko_ref, vr_ref, vo_ref, mix_ref, lse_ref):
    for head in range(PAIR // HEAD):
        cols = slice(head * HEAD, (head + 1) * HEAD)
        keys = jnp.concatenate([kr_ref[:, cols], ko_ref[:, cols]], 0)
        values = jnp.concatenate([vr_ref[:, cols], vo_ref[:, cols]], 0)
        slope = slope_ref[head][:, 0:1]
        scores = pair_scores(info_ref, slope, q_ref[:, cols], keys, score_scale)
        row_top = jnp.max(scores, axis=-1, keepdims=True)
        weights = jnp.exp(scores - row_top)
        row_total = jnp.sum(weights, axis=-1, keepdims=True)
        probs_low = (weights / row_total).astype(jnp.bfloat16)
        mix = jnp.dot(probs_low, values, preferred_element_type=jnp.float32)
        mix_ref[:, cols] = mix.astype(mix_ref.dtype)
        lse_ref[head] = row_top + jnp.log(row_total)


def pair_bwd_kernel(
    score_scale, info_ref, slope_ref, q_ref, kr_ref, ko_ref, vr_ref, vo_ref, g_ref, lse_ref,
    dq_ref, dkr_ref, dko_ref, dvr_ref, dvo_ref,
):
    rows = q_ref.shape[0]
    for head in range(PAIR // HEAD):
        cols = slice(head * HEAD, (head + 1) * HEAD)
        q = q_ref[:, cols]
        keys = jnp.concatenate([kr_ref[:, cols], ko_ref[:, cols]], 0)
        values = jnp.concatenate([vr_ref[:, cols], vo_ref[:, cols]], 0)
        grad = g_ref[:, cols]
        slope = slope_ref[head][:, 0:1]
        scores = pair_scores(info_ref, slope, q, keys, score_scale)
        probs = jnp.exp(scores - lse_ref[head])
        probs_low = probs.astype(jnp.bfloat16)
        dv = lax.dot_general(probs_low, grad, (((0,), (0,)), ((), ())), preferred_element_type=jnp.float32)
        grad_probs = lax.dot_general(grad, values, (((1,), (1,)), ((), ())), preferred_element_type=jnp.float32)
        row_delta = jnp.sum(probs * grad_probs, axis=-1, keepdims=True)
        grad_scores = (probs * (grad_probs - row_delta)).astype(jnp.bfloat16)
        dq_ref[:, cols] = jnp.dot(grad_scores, keys, preferred_element_type=jnp.float32) * score_scale
        dk = lax.dot_general(grad_scores, q, (((0,), (0,)), ((), ())), preferred_element_type=jnp.float32) * score_scale
        dkr_ref[:, cols] = dk[:rows]
        dko_ref[:, cols] = dk[rows:]
        dvr_ref[:, cols] = dv[:rows]
        dvo_ref[:, cols] = dv[rows:]


def slope_rows(slopes):
    return jnp.broadcast_to(slopes[:, None, None], (slopes.shape[0], 1, 128)).astype(jnp.float32)


def group_attention_fwd(info, slopes, queries, key_own, value_own, received, group, score_scale):
    rows = queries.shape[0]
    width = received.shape[1] // 2
    pairs = width // PAIR
    base = group * pairs
    full = lambda j, info_ref: (0, base + j)
    recv_k = lambda j, info_ref: (0, j)
    recv_v = lambda j, info_ref: (0, pairs + j)
    local = lambda j, info_ref: (0, j)
    per_pair = lambda j, info_ref: (j, 0, 0)
    heads = pairs * (PAIR // HEAD)
    return pl.pallas_call(
        functools.partial(pair_fwd_kernel, score_scale),
        grid_spec=pltpu.PrefetchScalarGridSpec(
            num_scalar_prefetch=1,
            grid=(pairs,),
            in_specs=[
                pl.BlockSpec((PAIR // HEAD, 1, 128), per_pair),
                pl.BlockSpec((rows, PAIR), full),
                pl.BlockSpec((rows, PAIR), recv_k),
                pl.BlockSpec((rows, PAIR), full),
                pl.BlockSpec((rows, PAIR), recv_v),
                pl.BlockSpec((rows, PAIR), full),
            ],
            out_specs=[
                pl.BlockSpec((rows, PAIR), local),
                pl.BlockSpec((PAIR // HEAD, rows, 1), per_pair),
            ],
        ),
        out_shape=[
            jax.ShapeDtypeStruct((rows, width), jnp.bfloat16),
            jax.ShapeDtypeStruct((heads, rows, 1), jnp.float32),
        ],
        compiler_params=pltpu.CompilerParams(vmem_limit_bytes=48 * 1024 * 1024),
        cost_estimate=pl.CostEstimate(
            flops=4 * heads * rows * 2 * rows * HEAD,
            transcendentals=heads * rows * 2 * rows,
            bytes_accessed=12 * rows * width,
        ),
    )(info, slope_rows(slopes), queries, received, key_own, received, value_own)


def group_attention_bwd(info, slopes, queries, key_own, value_own, received, grads, lse, group, score_scale):
    rows = queries.shape[0]
    width = received.shape[1] // 2
    pairs = width // PAIR
    base = group * pairs
    full = lambda j, info_ref: (0, base + j)
    recv_k = lambda j, info_ref: (0, j)
    recv_v = lambda j, info_ref: (0, pairs + j)
    local = lambda j, info_ref: (0, j)
    per_pair = lambda j, info_ref: (j, 0, 0)
    heads = pairs * (PAIR // HEAD)
    part = jax.ShapeDtypeStruct((rows, width), jnp.float32)
    return pl.pallas_call(
        functools.partial(pair_bwd_kernel, score_scale),
        grid_spec=pltpu.PrefetchScalarGridSpec(
            num_scalar_prefetch=1,
            grid=(pairs,),
            in_specs=[
                pl.BlockSpec((PAIR // HEAD, 1, 128), per_pair),
                pl.BlockSpec((rows, PAIR), full),
                pl.BlockSpec((rows, PAIR), recv_k),
                pl.BlockSpec((rows, PAIR), full),
                pl.BlockSpec((rows, PAIR), recv_v),
                pl.BlockSpec((rows, PAIR), full),
                pl.BlockSpec((rows, PAIR), full),
                pl.BlockSpec((PAIR // HEAD, rows, 1), per_pair),
            ],
            out_specs=[pl.BlockSpec((rows, PAIR), local)] * 5,
        ),
        out_shape=[part] * 5,
        compiler_params=pltpu.CompilerParams(vmem_limit_bytes=48 * 1024 * 1024),
        cost_estimate=pl.CostEstimate(
            flops=8 * heads * rows * 2 * rows * HEAD,
            transcendentals=heads * rows * 2 * rows,
            bytes_accessed=40 * rows * width,
        ),
    )(info, slope_rows(slopes), queries, received, key_own, received, value_own, grads, lse)


def passed_along(value, axis, steps):
    count = lax.axis_size(axis)
    leading, last = (max(0, -steps), min(count, count - steps))
    return lax.ppermute(value, axis, [(source, source + steps) for source in range(leading, last)])


SMALL_WIDTH = 3072


def small_rows(small_half, blocks):
    flat = small_half.reshape(-1)
    padded = blocks * SMALL_WIDTH
    return jnp.pad(flat, (0, padded - flat.shape[0])).reshape(blocks, 1, SMALL_WIDTH)


def gather_rows(row_arrays):
    cores = lax.axis_size(CORE)
    outer = lax.axis_size(OUTER)
    blocks = cores * outer
    place = lax.axis_index(CORE) * outer + lax.axis_index(OUTER)
    heights = [piece.shape[1] for piece in row_arrays]
    mine = jnp.concatenate(
        [lax.dynamic_index_in_dim(piece, place, 0, keepdims=False) for piece in row_arrays], 0
    )
    other = lax.ppermute(mine, SHARD, [(0, 1), (1, 0)])
    got = lax.all_gather(other, OUTER, axis=0, tiled=False)
    got = lax.all_gather(got, CORE, axis=0, tiled=False)
    got = got.reshape(blocks, -1, got.shape[-1])
    pieces = []
    offset = 0
    for height in heights:
        pieces.append(got[:, offset : offset + height])
        offset += height
    return pieces


def join_halves(own, other, dim):
    upper = lax.axis_index(SHARD) == 1
    in_order = jnp.concatenate([own, other], axis=dim)
    swapped = jnp.concatenate([other, own], axis=dim)
    return jnp.where(upper, swapped, in_order)


def reduce_rows(row_grads):
    shard_count = lax.axis_size(SHARD)
    cores = lax.axis_size(CORE)
    outer = lax.axis_size(OUTER)
    blocks = cores * outer
    heights = [piece.shape[3] for piece in row_grads]
    width = row_grads[0].shape[-1]
    stacked = jnp.concatenate([piece.astype(jnp.bfloat16) for piece in row_grads], 3)
    stacked = stacked.reshape(cores, -1, width)
    stacked = lax.psum_scatter(stacked, CORE, scatter_dimension=0, tiled=True)
    stacked = stacked.reshape(outer, -1, width)
    stacked = lax.psum_scatter(stacked, OUTER, scatter_dimension=0, tiled=True)
    stacked = stacked.reshape(shard_count, -1, width)
    stacked = lax.psum_scatter(stacked, SHARD, scatter_dimension=0, tiled=True)
    stacked = stacked.reshape(stacked.shape[1:])
    stacked = lax.all_gather(stacked, OUTER, axis=0, tiled=True)
    stacked = lax.all_gather(stacked, CORE, axis=0, tiled=True)
    stacked = stacked.reshape(blocks, -1, width)
    pieces = []
    offset = 0
    for height in heights:
        pieces.append(stacked[:, offset : offset + height].astype(jnp.float32))
        offset += height
    return pieces


def split_rows(grad_full):
    shard_count = lax.axis_size(SHARD)
    cores = lax.axis_size(CORE)
    outer = lax.axis_size(OUTER)
    rows, cols = grad_full.shape
    split = grad_full.reshape(shard_count, cores, outer, rows // (shard_count * cores * outer), cols)
    return split.transpose(1, 2, 0, 3, 4)


def block_major(grad_perm):
    shard_count = lax.axis_size(SHARD)
    cores = lax.axis_size(CORE)
    outer = lax.axis_size(OUTER)
    rows, cols = grad_perm.shape
    return grad_perm.reshape(cores, outer, shard_count, rows // (shard_count * cores * outer), cols)


def ff_order(values, blocks):
    shard_count = lax.axis_size(SHARD)
    rest = values.shape[1:]
    split = values.reshape((shard_count, blocks, values.shape[0] // (shard_count * blocks)) + rest)
    return jnp.swapaxes(split, 0, 1).reshape(values.shape)


def ff_natural(values, blocks):
    shard_count = lax.axis_size(SHARD)
    rest = values.shape[1:]
    split = values.reshape((blocks, shard_count, values.shape[0] // (shard_count * blocks)) + rest)
    return jnp.swapaxes(split, 0, 1).reshape(values.shape)


def join_blocks(own, other, blocks):
    upper = lax.axis_index(SHARD) == 1
    own_b = own.reshape((blocks, -1) + own.shape[1:])
    other_b = other.reshape((blocks, -1) + other.shape[1:])
    in_order = jnp.stack([own_b, other_b], 1)
    swapped = jnp.stack([other_b, own_b], 1)
    joined = jnp.where(upper, swapped, in_order)
    return joined.reshape((2 * own.shape[0],) + own.shape[1:])


def norm_stats(field_in):
    centred = field_in - jnp.mean(field_in, axis=-1, keepdims=True)
    inverse = lax.rsqrt(jnp.mean(centred * centred, axis=-1, keepdims=True) + EPS)
    return (centred * inverse, inverse)


def norm_back(grad_hat, normed, inverse):
    first_mean = jnp.mean(grad_hat, axis=-1, keepdims=True)
    second_mean = jnp.mean(grad_hat * normed, axis=-1, keepdims=True)
    return inverse * (grad_hat - first_mean - normed * second_mean)


def contract_rows(left_side, right_side):
    return lax.dot_general(
        left_side, right_side, (((0,), (0,)), ((), ())), preferred_element_type=jnp.float32
    )


def contract_cols(left_side, right_side):
    return lax.dot_general(
        left_side, right_side, (((1,), (1,)), ((), ())), preferred_element_type=jnp.float32
    )


def gelu_tanh(field_in):
    return jax.nn.gelu(field_in, approximate=True)


def gelu_back(pre_act, grad_act):
    _, pull_back = jax.vjp(gelu_tanh, pre_act)
    return pull_back(grad_act)[0]


def nesterov(grad_total, weight_old, moment_old, average_old, rate):
    moment_new = MOMENTUM * moment_old + grad_total
    weight_new = weight_old - rate * (grad_total + MOMENTUM * moment_new)
    average_new = AVERAGING * average_old + (1.0 - AVERAGING) * weight_new
    return (weight_new, moment_new, average_new)


def body(
    tokens,
    cotangent,
    lengths,
    qkv_weight,
    qkv_momentum,
    qkv_average,
    out_weight,
    out_momentum,
    out_average,
    up_weight,
    up_momentum,
    up_average,
    down_weight,
    down_momentum,
    down_average,
    small_params,
    small_momentum,
    small_average,
):
    tok_rows = tokens.shape[0]
    model_width = tokens.shape[1]
    shard_count = lax.axis_size(SHARD)
    group_count = lax.axis_size(OUTER) * lax.axis_size(CORE)
    shard_place = lax.axis_index(SHARD)
    group_place = lax.axis_index(OUTER) * lax.axis_size(CORE) + lax.axis_index(CORE)
    upper_half = shard_place % 2
    seq_place = group_place * (shard_count // 2) + shard_place // 2
    seq_length = lax.dynamic_index_in_dim(lengths, seq_place, 0, keepdims=False)
    local_pos = jnp.arange(tok_rows, dtype=jnp.int32)
    query_pos = upper_half * tok_rows + local_pos
    key_pos = jnp.concatenate([local_pos, query_pos])
    prev_live = jnp.full((tok_rows,), upper_half == 1)
    key_live = jnp.concatenate([prev_live, jnp.ones((tok_rows,), bool)]) & (key_pos < seq_length)
    distance = (query_pos[:, None] - key_pos[None, :]).astype(jnp.float32)
    row_live = (query_pos < seq_length).astype(jnp.float32)[:, None]
    head_size = model_width // HEADS
    score_scale = head_size ** (-0.5)
    slopes = 2.0 ** (-8.0 * (jnp.arange(HEADS, dtype=jnp.float32) + 1.0) / HEADS)
    blocks = lax.axis_size(CORE) * lax.axis_size(OUTER)
    qkv_own = qkv_weight.astype(jnp.bfloat16)
    small_own = small_params.astype(jnp.bfloat16)
    qkv_other, small_other = gather_rows(
        [qkv_own.reshape(blocks, -1, qkv_own.shape[1]), small_rows(small_own, blocks)]
    )
    qkv_full = join_halves(qkv_own, qkv_other.reshape(qkv_own.shape), 0)
    small_full = join_halves(
        small_own, small_other.reshape(-1)[: small_own.size].reshape(small_own.shape), 1
    )
    out_own = out_weight.astype(jnp.bfloat16)
    up_own_t = up_weight.astype(jnp.bfloat16).T
    down_own = down_weight.astype(jnp.bfloat16)
    out_other, up_other_t, down_other = gather_rows(
        [piece.reshape(blocks, -1, piece.shape[1]) for piece in (out_own, up_own_t, down_own)],
    )
    out_full = join_halves(out_own, out_other.reshape(out_own.shape), 0)
    up_full_t = join_blocks(up_own_t, up_other_t.reshape(up_own_t.shape), blocks)
    down_full = join_blocks(down_own, down_other.reshape(down_own.shape), blocks)
    table = small_full.astype(jnp.float32)
    up_bias = ff_order(table[8:12].reshape(FF), blocks)
    normed_one, inverse_one = norm_stats(tokens)
    entry_low = (normed_one * table[0] + table[1]).astype(jnp.bfloat16)
    mapped = jnp.dot(entry_low, qkv_full, preferred_element_type=jnp.float32)
    queries = (mapped[:, :model_width] + table[2]).astype(jnp.bfloat16)
    key_own = mapped[:, model_width : 2 * model_width].astype(jnp.bfloat16)
    value_own = (mapped[:, 2 * model_width :] + table[3]).astype(jnp.bfloat16)
    groups = 4
    per_group = HEADS // groups
    group_width = per_group * (model_width // HEADS)
    received_groups = []
    for group in range(groups):
        cols = slice(group * group_width, (group + 1) * group_width)
        received_groups.append(
            passed_along(jnp.concatenate([key_own[:, cols], value_own[:, cols]], 1), SHARD, 1)
        )

    info = jnp.stack([upper_half, seq_length]).astype(jnp.int32)
    fwd_parts = []
    for group in range(groups):
        chosen = slice(group * per_group, (group + 1) * per_group)
        fwd_parts.append(
            group_attention_fwd(
                info,
                slopes[chosen],
                queries,
                key_own,
                value_own,
                received_groups[group],
                group,
                score_scale,
            )
        )
    attended_low = jnp.concatenate([part[0] for part in fwd_parts], 1)
    resid_one = (
        tokens + jnp.dot(attended_low, out_full, preferred_element_type=jnp.float32) + table[4]
    )
    normed_two, inverse_two = norm_stats(resid_one)
    inner_low = (normed_two * table[5] + table[6]).astype(jnp.bfloat16)
    grad_out = cotangent * row_live
    down_bias_grad = jnp.sum(grad_out, axis=0)
    grad_low = grad_out.astype(jnp.bfloat16)
    pre_act = contract_cols(inner_low, up_full_t) + up_bias
    act_low = gelu_tanh(pre_act).astype(jnp.bfloat16)
    branch_out = jnp.dot(act_low, down_full, preferred_element_type=jnp.float32)
    block_out = resid_one + branch_out + table[7]
    grad_act = contract_cols(grad_low, down_full)
    down_grad = contract_rows(act_low, grad_low)
    grad_pre = gelu_back(pre_act, grad_act)
    up_bias_grad = ff_natural(jnp.sum(grad_pre, axis=0), blocks)
    pre_low = grad_pre.astype(jnp.bfloat16)
    up_grad_t = contract_rows(pre_low, inner_low)
    grad_inner = jnp.dot(pre_low, up_full_t, preferred_element_type=jnp.float32)
    gain_two_grad = jnp.sum(grad_inner * normed_two, axis=0)
    shift_two_grad = jnp.sum(grad_inner, axis=0)
    grad_resid = grad_out + norm_back(grad_inner * table[5], normed_two, inverse_two)
    resid_low = grad_resid.astype(jnp.bfloat16)
    out_grad = contract_rows(attended_low, resid_low)
    grad_resid, resid_low, up_grad_t, down_grad, out_grad = lax.optimization_barrier(
        (grad_resid, resid_low, up_grad_t, down_grad, out_grad)
    )
    out_sum, up_sum_t, down_sum = reduce_rows(
        [split_rows(out_grad), block_major(up_grad_t), block_major(down_grad)]
    )
    out_total = out_sum.reshape(out_weight.shape)
    up_total = up_sum_t.reshape(up_weight.shape[::-1]).T
    down_total = down_sum.reshape(down_weight.shape)
    out_bias_grad = jnp.sum(grad_resid, axis=0)
    grad_mixture = contract_cols(resid_low, out_full).astype(jnp.bfloat16)

    query_parts, key_parts, value_parts = [], [], []
    for group in range(groups):
        chosen = slice(group * per_group, (group + 1) * per_group)
        group_query, keys_back, keys_kept, values_back, values_kept = group_attention_bwd(
            info,
            slopes[chosen],
            queries,
            key_own,
            value_own,
            received_groups[group],
            grad_mixture,
            fwd_parts[group][1],
            group,
            score_scale,
        )
        returned = passed_along(
            jnp.concatenate([keys_back, values_back], 1).astype(jnp.bfloat16), SHARD, -1
        ).astype(jnp.float32)
        query_parts.append(group_query)
        key_parts.append(keys_kept + returned[:, :group_width])
        value_parts.append(values_kept + returned[:, group_width:])
    grad_query = jnp.concatenate(query_parts, 1)
    grad_key_own = jnp.concatenate(key_parts, 1)
    grad_value_own = jnp.concatenate(value_parts, 1)
    query_bias_grad = jnp.sum(grad_query, axis=0)
    value_bias_grad = jnp.sum(grad_value_own, axis=0)
    mapped_low = jnp.concatenate([grad_query, grad_key_own, grad_value_own], 1).astype(jnp.bfloat16)
    qkv_grad = contract_rows(entry_low, mapped_low)
    grad_entry = contract_cols(mapped_low, qkv_full)
    gain_one_grad = jnp.sum(grad_entry * normed_one, axis=0)
    shift_one_grad = jnp.sum(grad_entry, axis=0)
    input_grad = grad_resid + norm_back(grad_entry * table[0], normed_one, inverse_one)
    head_rows = jnp.stack(
        [
            gain_one_grad,
            shift_one_grad,
            query_bias_grad,
            value_bias_grad,
            out_bias_grad,
            gain_two_grad,
            shift_two_grad,
            down_bias_grad,
        ]
    )
    small_grad = jnp.concatenate([head_rows, up_bias_grad.reshape(4, model_width)], 0)
    small_halves = small_grad.reshape(small_grad.shape[0], shard_count, -1).transpose(1, 0, 2)
    small_packed = jnp.stack(
        [small_rows(small_halves[index], blocks) for index in range(shard_count)]
    ).reshape(shard_count, lax.axis_size(CORE), lax.axis_size(OUTER), 1, SMALL_WIDTH)
    small_packed = small_packed.transpose(1, 2, 0, 3, 4)
    qkv_sum, small_sum = reduce_rows([split_rows(qkv_grad), small_packed])
    qkv_total = qkv_sum.reshape(qkv_weight.shape)
    small_total = small_sum.reshape(-1)[: small_params.size].reshape(small_params.shape)
    rate = 2.0 / math.sqrt(model_width * tok_rows * shard_count * group_count)
    qkv_new = nesterov(qkv_total, qkv_weight, qkv_momentum, qkv_average, rate)
    out_new = nesterov(out_total, out_weight, out_momentum, out_average, rate)
    up_new = nesterov(up_total, up_weight, up_momentum, up_average, rate)
    down_new = nesterov(down_total, down_weight, down_momentum, down_average, rate)
    small_new = nesterov(small_total, small_params, small_momentum, small_average, rate)
    return (
        block_out,
        input_grad,
        qkv_new[0],
        qkv_new[1],
        qkv_new[2],
        out_new[0],
        out_new[1],
        out_new[2],
        up_new[0],
        up_new[1],
        up_new[2],
        down_new[0],
        down_new[1],
        down_new[2],
        small_new[0],
        small_new[1],
        small_new[2],
    )


def solution(mesh):
    cores = 2
    devices = mesh.devices.reshape(mesh.shape["group"] // cores, cores, mesh.shape[SHARD])
    inner_mesh = jax.sharding.Mesh(devices, (OUTER, CORE, SHARD))
    rows = P((OUTER, CORE, SHARD), None)
    in_specs = (
        rows,
        rows,
        P(),
        P(SHARD, None),
        P(SHARD, None),
        P(SHARD, None),
        P(SHARD, None),
        P(SHARD, None),
        P(SHARD, None),
        P(None, SHARD),
        P(None, SHARD),
        P(None, SHARD),
        P(SHARD, None),
        P(SHARD, None),
        P(SHARD, None),
        P(None, SHARD),
        P(None, SHARD),
        P(None, SHARD),
    )
    out_specs = (
        rows,
        rows,
        P(SHARD, None),
        P(SHARD, None),
        P(SHARD, None),
        P(SHARD, None),
        P(SHARD, None),
        P(SHARD, None),
        P(None, SHARD),
        P(None, SHARD),
        P(None, SHARD),
        P(SHARD, None),
        P(SHARD, None),
        P(SHARD, None),
        P(None, SHARD),
        P(None, SHARD),
        P(None, SHARD),
    )

    return jax.shard_map(body, mesh=inner_mesh, in_specs=in_specs, out_specs=out_specs, check_vma=False)
```

```python
import functools
import math

import jax
import jax.numpy as jnp
from jax import lax
from jax.experimental import pallas as pl
from jax.experimental.pallas import tpu as pltpu
from jax.sharding import PartitionSpec as P


HEADS = 16
FF = 4096


EPS = 1e-05
MOMENTUM = 0.9
AVERAGING = 0.9
NEG_FILL = -1e30
SHARD = "shard"
OUTER = "outer"
CORE = "core"


HEAD = 64
PAIR = 128


def pair_scores(info_ref, slope, q, k, score_scale):
    upper = info_ref[0]
    seq_length = info_ref[1]
    rows, cols = q.shape[0], k.shape[0]
    own = cols - rows
    raw = lax.dot_general(q, k, (((1,), (1,)), ((), ())), preferred_element_type=jnp.float32)
    query_pos = upper * rows + lax.broadcasted_iota(jnp.int32, (rows, cols), 0)
    key_index = lax.broadcasted_iota(jnp.int32, (rows, cols), 1)
    key_pos = jnp.where(key_index < own, key_index, upper * rows + key_index - own)
    allowed = ((key_index >= own) | (upper == 1)) & (key_pos < seq_length) & (key_pos <= query_pos)
    distance = (query_pos - key_pos).astype(jnp.float32)
    raw = raw * score_scale - slope * distance
    return jnp.where(allowed, raw, NEG_FILL)


def pair_fwd_kernel(score_scale, info_ref, slope_ref, q_ref, kr_ref, ko_ref, vr_ref, vo_ref, mix_ref, lse_ref):
    for head in range(PAIR // HEAD):
        cols = slice(head * HEAD, (head + 1) * HEAD)
        keys = jnp.concatenate([kr_ref[:, cols], ko_ref[:, cols]], 0)
        values = jnp.concatenate([vr_ref[:, cols], vo_ref[:, cols]], 0)
        slope = slope_ref[head][:, 0:1]
        scores = pair_scores(info_ref, slope, q_ref[:, cols], keys, score_scale)
        row_top = jnp.max(scores, axis=-1, keepdims=True)
        weights = jnp.exp(scores - row_top)
        row_total = jnp.sum(weights, axis=-1, keepdims=True)
        probs_low = (weights / row_total).astype(jnp.bfloat16)
        mix = jnp.dot(probs_low, values, preferred_element_type=jnp.float32)
        mix_ref[:, cols] = mix.astype(mix_ref.dtype)
        lse_ref[head] = row_top + jnp.log(row_total)


def pair_bwd_kernel(
    score_scale, info_ref, slope_ref, q_ref, kr_ref, ko_ref, vr_ref, vo_ref, g_ref, lse_ref,
    dq_ref, dkr_ref, dko_ref, dvr_ref, dvo_ref,
):
    rows = q_ref.shape[0]
    for head in range(PAIR // HEAD):
        cols = slice(head * HEAD, (head + 1) * HEAD)
        q = q_ref[:, cols]
        keys = jnp.concatenate([kr_ref[:, cols], ko_ref[:, cols]], 0)
        values = jnp.concatenate([vr_ref[:, cols], vo_ref[:, cols]], 0)
        grad = g_ref[:, cols]
        slope = slope_ref[head][:, 0:1]
        scores = pair_scores(info_ref, slope, q, keys, score_scale)
        probs = jnp.exp(scores - lse_ref[head])
        probs_low = probs.astype(jnp.bfloat16)
        dv = lax.dot_general(probs_low, grad, (((0,), (0,)), ((), ())), preferred_element_type=jnp.float32)
        grad_probs = lax.dot_general(grad, values, (((1,), (1,)), ((), ())), preferred_element_type=jnp.float32)
        row_delta = jnp.sum(probs * grad_probs, axis=-1, keepdims=True)
        grad_scores = (probs * (grad_probs - row_delta)).astype(jnp.bfloat16)
        dq_ref[:, cols] = jnp.dot(grad_scores, keys, preferred_element_type=jnp.float32) * score_scale
        dk = lax.dot_general(grad_scores, q, (((0,), (0,)), ((), ())), preferred_element_type=jnp.float32) * score_scale
        dkr_ref[:, cols] = dk[:rows]
        dko_ref[:, cols] = dk[rows:]
        dvr_ref[:, cols] = dv[:rows]
        dvo_ref[:, cols] = dv[rows:]


def slope_rows(slopes):
    return jnp.broadcast_to(slopes[:, None, None], (slopes.shape[0], 1, 128)).astype(jnp.float32)


def group_attention_fwd(info, slopes, queries, key_own, value_own, received, group, score_scale):
    rows = queries.shape[0]
    width = received.shape[1] // 2
    pairs = width // PAIR
    base = group * pairs
    full = lambda j, info_ref: (0, base + j)
    recv_k = lambda j, info_ref: (0, j)
    recv_v = lambda j, info_ref: (0, pairs + j)
    local = lambda j, info_ref: (0, j)
    per_pair = lambda j, info_ref: (j, 0, 0)
    heads = pairs * (PAIR // HEAD)
    return pl.pallas_call(
        functools.partial(pair_fwd_kernel, score_scale),
        grid_spec=pltpu.PrefetchScalarGridSpec(
            num_scalar_prefetch=1,
            grid=(pairs,),
            in_specs=[
                pl.BlockSpec((PAIR // HEAD, 1, 128), per_pair),
                pl.BlockSpec((rows, PAIR), full),
                pl.BlockSpec((rows, PAIR), recv_k),
                pl.BlockSpec((rows, PAIR), full),
                pl.BlockSpec((rows, PAIR), recv_v),
                pl.BlockSpec((rows, PAIR), full),
            ],
            out_specs=[
                pl.BlockSpec((rows, PAIR), local),
                pl.BlockSpec((PAIR // HEAD, rows, 1), per_pair),
            ],
        ),
        out_shape=[
            jax.ShapeDtypeStruct((rows, width), jnp.bfloat16),
            jax.ShapeDtypeStruct((heads, rows, 1), jnp.float32),
        ],
        compiler_params=pltpu.CompilerParams(vmem_limit_bytes=48 * 1024 * 1024),
        cost_estimate=pl.CostEstimate(
            flops=4 * heads * rows * 2 * rows * HEAD,
            transcendentals=heads * rows * 2 * rows,
            bytes_accessed=12 * rows * width,
        ),
    )(info, slope_rows(slopes), queries, received, key_own, received, value_own)


def group_attention_bwd(info, slopes, queries, key_own, value_own, received, grads, lse, group, score_scale):
    rows = queries.shape[0]
    width = received.shape[1] // 2
    pairs = width // PAIR
    base = group * pairs
    full = lambda j, info_ref: (0, base + j)
    recv_k = lambda j, info_ref: (0, j)
    recv_v = lambda j, info_ref: (0, pairs + j)
    local = lambda j, info_ref: (0, j)
    per_pair = lambda j, info_ref: (j, 0, 0)
    heads = pairs * (PAIR // HEAD)
    part = jax.ShapeDtypeStruct((rows, width), jnp.float32)
    return pl.pallas_call(
        functools.partial(pair_bwd_kernel, score_scale),
        grid_spec=pltpu.PrefetchScalarGridSpec(
            num_scalar_prefetch=1,
            grid=(pairs,),
            in_specs=[
                pl.BlockSpec((PAIR // HEAD, 1, 128), per_pair),
                pl.BlockSpec((rows, PAIR), full),
                pl.BlockSpec((rows, PAIR), recv_k),
                pl.BlockSpec((rows, PAIR), full),
                pl.BlockSpec((rows, PAIR), recv_v),
                pl.BlockSpec((rows, PAIR), full),
                pl.BlockSpec((rows, PAIR), full),
                pl.BlockSpec((PAIR // HEAD, rows, 1), per_pair),
            ],
            out_specs=[pl.BlockSpec((rows, PAIR), local)] * 5,
        ),
        out_shape=[part] * 5,
        compiler_params=pltpu.CompilerParams(vmem_limit_bytes=48 * 1024 * 1024),
        cost_estimate=pl.CostEstimate(
            flops=8 * heads * rows * 2 * rows * HEAD,
            transcendentals=heads * rows * 2 * rows,
            bytes_accessed=40 * rows * width,
        ),
    )(info, slope_rows(slopes), queries, received, key_own, received, value_own, grads, lse)


def passed_along(value, axis, steps):
    count = lax.axis_size(axis)
    leading, last = (max(0, -steps), min(count, count - steps))
    return lax.ppermute(value, axis, [(source, source + steps) for source in range(leading, last)])


SMALL_WIDTH = 3072


def small_rows(small_half, blocks):
    flat = small_half.reshape(-1)
    padded = blocks * SMALL_WIDTH
    return jnp.pad(flat, (0, padded - flat.shape[0])).reshape(blocks, 1, SMALL_WIDTH)


def gather_ring(piece, axis):
    count = lax.axis_size(axis)
    place = lax.axis_index(axis)
    held = piece[None]
    step = 1
    while step < count:
        received = lax.ppermute(held, axis, [(index, index ^ step) for index in range(count)])
        first = (place & step) == 0
        held = jnp.where(
            first, jnp.concatenate([held, received], 0), jnp.concatenate([received, held], 0)
        )
        step *= 2
    return held


def gather_rows(row_arrays):
    cores = lax.axis_size(CORE)
    outer = lax.axis_size(OUTER)
    blocks = cores * outer
    place = lax.axis_index(CORE) * outer + lax.axis_index(OUTER)
    heights = [piece.shape[1] for piece in row_arrays]
    mine = jnp.concatenate(
        [lax.dynamic_index_in_dim(piece, place, 0, keepdims=False) for piece in row_arrays], 0
    )
    other = lax.ppermute(mine, SHARD, [(0, 1), (1, 0)])
    got = lax.all_gather(other, OUTER, axis=0, tiled=False)
    got = gather_ring(got, CORE)
    got = got.reshape(blocks, -1, got.shape[-1])
    pieces = []
    offset = 0
    for height in heights:
        pieces.append(got[:, offset : offset + height])
        offset += height
    return pieces


def join_halves(own, other, dim):
    upper = lax.axis_index(SHARD) == 1
    in_order = jnp.concatenate([own, other], axis=dim)
    swapped = jnp.concatenate([other, own], axis=dim)
    return jnp.where(upper, swapped, in_order)


def reduce_rows(row_grads, core_on_dma=False):
    shard_count = lax.axis_size(SHARD)
    cores = lax.axis_size(CORE)
    outer = lax.axis_size(OUTER)
    blocks = cores * outer
    heights = [piece.shape[3] for piece in row_grads]
    width = row_grads[0].shape[-1]
    stacked = jnp.concatenate([piece.astype(jnp.bfloat16) for piece in row_grads], 3)
    stacked = stacked.reshape(cores, -1, width)
    stacked = lax.psum_scatter(stacked, CORE, scatter_dimension=0, tiled=True)
    stacked = stacked.reshape(outer, -1, width)
    stacked = lax.psum_scatter(stacked, OUTER, scatter_dimension=0, tiled=True)
    stacked = stacked.reshape(shard_count, -1, width)
    stacked = lax.psum_scatter(stacked, SHARD, scatter_dimension=0, tiled=True)
    stacked = stacked.reshape(stacked.shape[1:])
    stacked = lax.all_gather(stacked, OUTER, axis=0, tiled=True)
    if core_on_dma:
        stacked = gather_ring(stacked, CORE)
    else:
        stacked = lax.all_gather(stacked, CORE, axis=0, tiled=True)
    stacked = stacked.reshape(blocks, -1, width)
    pieces = []
    offset = 0
    for height in heights:
        pieces.append(stacked[:, offset : offset + height].astype(jnp.float32))
        offset += height
    return pieces


def split_rows(grad_full):
    shard_count = lax.axis_size(SHARD)
    cores = lax.axis_size(CORE)
    outer = lax.axis_size(OUTER)
    rows, cols = grad_full.shape
    split = grad_full.reshape(shard_count, cores, outer, rows // (shard_count * cores * outer), cols)
    return split.transpose(1, 2, 0, 3, 4)


def block_major(grad_perm):
    shard_count = lax.axis_size(SHARD)
    cores = lax.axis_size(CORE)
    outer = lax.axis_size(OUTER)
    rows, cols = grad_perm.shape
    return grad_perm.reshape(cores, outer, shard_count, rows // (shard_count * cores * outer), cols)


def ff_order(values, blocks):
    shard_count = lax.axis_size(SHARD)
    rest = values.shape[1:]
    split = values.reshape((shard_count, blocks, values.shape[0] // (shard_count * blocks)) + rest)
    return jnp.swapaxes(split, 0, 1).reshape(values.shape)


def ff_natural(values, blocks):
    shard_count = lax.axis_size(SHARD)
    rest = values.shape[1:]
    split = values.reshape((blocks, shard_count, values.shape[0] // (shard_count * blocks)) + rest)
    return jnp.swapaxes(split, 0, 1).reshape(values.shape)


def join_blocks(own, other, blocks):
    upper = lax.axis_index(SHARD) == 1
    own_b = own.reshape((blocks, -1) + own.shape[1:])
    other_b = other.reshape((blocks, -1) + other.shape[1:])
    in_order = jnp.stack([own_b, other_b], 1)
    swapped = jnp.stack([other_b, own_b], 1)
    joined = jnp.where(upper, swapped, in_order)
    return joined.reshape((2 * own.shape[0],) + own.shape[1:])


def norm_stats(field_in):
    centred = field_in - jnp.mean(field_in, axis=-1, keepdims=True)
    inverse = lax.rsqrt(jnp.mean(centred * centred, axis=-1, keepdims=True) + EPS)
    return (centred * inverse, inverse)


def norm_back(grad_hat, normed, inverse):
    first_mean = jnp.mean(grad_hat, axis=-1, keepdims=True)
    second_mean = jnp.mean(grad_hat * normed, axis=-1, keepdims=True)
    return inverse * (grad_hat - first_mean - normed * second_mean)


def contract_rows(left_side, right_side):
    return lax.dot_general(
        left_side, right_side, (((0,), (0,)), ((), ())), preferred_element_type=jnp.float32
    )


def contract_cols(left_side, right_side):
    return lax.dot_general(
        left_side, right_side, (((1,), (1,)), ((), ())), preferred_element_type=jnp.float32
    )


def gelu_tanh(field_in):
    return jax.nn.gelu(field_in, approximate=True)


def gelu_back(pre_act, grad_act):
    _, pull_back = jax.vjp(gelu_tanh, pre_act)
    return pull_back(grad_act)[0]


def nesterov(grad_total, weight_old, moment_old, average_old, rate):
    moment_new = MOMENTUM * moment_old + grad_total
    weight_new = weight_old - rate * (grad_total + MOMENTUM * moment_new)
    average_new = AVERAGING * average_old + (1.0 - AVERAGING) * weight_new
    return (weight_new, moment_new, average_new)


def body(
    tokens,
    cotangent,
    lengths,
    qkv_weight,
    qkv_momentum,
    qkv_average,
    out_weight,
    out_momentum,
    out_average,
    up_weight,
    up_momentum,
    up_average,
    down_weight,
    down_momentum,
    down_average,
    small_params,
    small_momentum,
    small_average,
):
    tok_rows = tokens.shape[0]
    model_width = tokens.shape[1]
    shard_count = lax.axis_size(SHARD)
    group_count = lax.axis_size(OUTER) * lax.axis_size(CORE)
    shard_place = lax.axis_index(SHARD)
    group_place = lax.axis_index(OUTER) * lax.axis_size(CORE) + lax.axis_index(CORE)
    upper_half = shard_place % 2
    seq_place = group_place * (shard_count // 2) + shard_place // 2
    seq_length = lax.dynamic_index_in_dim(lengths, seq_place, 0, keepdims=False)
    local_pos = jnp.arange(tok_rows, dtype=jnp.int32)
    query_pos = upper_half * tok_rows + local_pos
    key_pos = jnp.concatenate([local_pos, query_pos])
    prev_live = jnp.full((tok_rows,), upper_half == 1)
    key_live = jnp.concatenate([prev_live, jnp.ones((tok_rows,), bool)]) & (key_pos < seq_length)
    distance = (query_pos[:, None] - key_pos[None, :]).astype(jnp.float32)
    row_live = (query_pos < seq_length).astype(jnp.float32)[:, None]
    head_size = model_width // HEADS
    score_scale = head_size ** (-0.5)
    slopes = 2.0 ** (-8.0 * (jnp.arange(HEADS, dtype=jnp.float32) + 1.0) / HEADS)
    blocks = lax.axis_size(CORE) * lax.axis_size(OUTER)
    qkv_own = qkv_weight.astype(jnp.bfloat16)
    small_own = small_params.astype(jnp.bfloat16)
    qkv_other, small_other = gather_rows(
        [qkv_own.reshape(blocks, -1, qkv_own.shape[1]), small_rows(small_own, blocks)]
    )
    qkv_full = join_halves(qkv_own, qkv_other.reshape(qkv_own.shape), 0)
    small_full = join_halves(
        small_own, small_other.reshape(-1)[: small_own.size].reshape(small_own.shape), 1
    )
    out_own = out_weight.astype(jnp.bfloat16)
    up_own_t = up_weight.astype(jnp.bfloat16).T
    down_own = down_weight.astype(jnp.bfloat16)
    out_other, up_other_t, down_other = gather_rows(
        [piece.reshape(blocks, -1, piece.shape[1]) for piece in (out_own, up_own_t, down_own)],
    )
    out_full = join_halves(out_own, out_other.reshape(out_own.shape), 0)
    up_full_t = join_blocks(up_own_t, up_other_t.reshape(up_own_t.shape), blocks)
    down_full = join_blocks(down_own, down_other.reshape(down_own.shape), blocks)
    table = small_full.astype(jnp.float32)
    up_bias = ff_order(table[8:12].reshape(FF), blocks)
    normed_one, inverse_one = norm_stats(tokens)
    entry_low = (normed_one * table[0] + table[1]).astype(jnp.bfloat16)
    mapped = jnp.dot(entry_low, qkv_full, preferred_element_type=jnp.float32)
    queries = (mapped[:, :model_width] + table[2]).astype(jnp.bfloat16)
    key_own = mapped[:, model_width : 2 * model_width].astype(jnp.bfloat16)
    value_own = (mapped[:, 2 * model_width :] + table[3]).astype(jnp.bfloat16)
    groups = 4
    per_group = HEADS // groups
    group_width = per_group * (model_width // HEADS)
    received_groups = []
    for group in range(groups):
        cols = slice(group * group_width, (group + 1) * group_width)
        received_groups.append(
            passed_along(jnp.concatenate([key_own[:, cols], value_own[:, cols]], 1), SHARD, 1)
        )

    info = jnp.stack([upper_half, seq_length]).astype(jnp.int32)
    fwd_parts = []
    for group in range(groups):
        chosen = slice(group * per_group, (group + 1) * per_group)
        fwd_parts.append(
            group_attention_fwd(
                info,
                slopes[chosen],
                queries,
                key_own,
                value_own,
                received_groups[group],
                group,
                score_scale,
            )
        )
    attended_low = jnp.concatenate([part[0] for part in fwd_parts], 1)
    resid_one = (
        tokens + jnp.dot(attended_low, out_full, preferred_element_type=jnp.float32) + table[4]
    )
    normed_two, inverse_two = norm_stats(resid_one)
    inner_low = (normed_two * table[5] + table[6]).astype(jnp.bfloat16)
    grad_out = cotangent * row_live
    down_bias_grad = jnp.sum(grad_out, axis=0)
    grad_low = grad_out.astype(jnp.bfloat16)
    pre_act = contract_cols(inner_low, up_full_t) + up_bias
    act_low = gelu_tanh(pre_act).astype(jnp.bfloat16)
    branch_out = jnp.dot(act_low, down_full, preferred_element_type=jnp.float32)
    block_out = resid_one + branch_out + table[7]
    grad_act = contract_cols(grad_low, down_full)
    down_grad = contract_rows(act_low, grad_low)
    grad_pre = gelu_back(pre_act, grad_act)
    up_bias_grad = ff_natural(jnp.sum(grad_pre, axis=0), blocks)
    pre_low = grad_pre.astype(jnp.bfloat16)
    up_grad_t = contract_rows(pre_low, inner_low)
    grad_inner = jnp.dot(pre_low, up_full_t, preferred_element_type=jnp.float32)
    gain_two_grad = jnp.sum(grad_inner * normed_two, axis=0)
    shift_two_grad = jnp.sum(grad_inner, axis=0)
    grad_resid = grad_out + norm_back(grad_inner * table[5], normed_two, inverse_two)
    resid_low = grad_resid.astype(jnp.bfloat16)
    out_grad = contract_rows(attended_low, resid_low)
    grad_resid, resid_low, up_grad_t, down_grad, out_grad = lax.optimization_barrier(
        (grad_resid, resid_low, up_grad_t, down_grad, out_grad)
    )
    out_sum, up_sum_t, down_sum = reduce_rows(
        [split_rows(out_grad), block_major(up_grad_t), block_major(down_grad)], core_on_dma=True
    )
    out_total = out_sum.reshape(out_weight.shape)
    up_total = up_sum_t.reshape(up_weight.shape[::-1]).T
    down_total = down_sum.reshape(down_weight.shape)
    out_bias_grad = jnp.sum(grad_resid, axis=0)
    grad_mixture = contract_cols(resid_low, out_full).astype(jnp.bfloat16)

    query_parts, key_parts, value_parts = [], [], []
    for group in range(groups):
        chosen = slice(group * per_group, (group + 1) * per_group)
        group_query, keys_back, keys_kept, values_back, values_kept = group_attention_bwd(
            info,
            slopes[chosen],
            queries,
            key_own,
            value_own,
            received_groups[group],
            grad_mixture,
            fwd_parts[group][1],
            group,
            score_scale,
        )
        returned = passed_along(
            jnp.concatenate([keys_back, values_back], 1).astype(jnp.bfloat16), SHARD, -1
        ).astype(jnp.float32)
        query_parts.append(group_query)
        key_parts.append(keys_kept + returned[:, :group_width])
        value_parts.append(values_kept + returned[:, group_width:])
    grad_query = jnp.concatenate(query_parts, 1)
    grad_key_own = jnp.concatenate(key_parts, 1)
    grad_value_own = jnp.concatenate(value_parts, 1)
    query_bias_grad = jnp.sum(grad_query, axis=0)
    value_bias_grad = jnp.sum(grad_value_own, axis=0)
    mapped_low = jnp.concatenate([grad_query, grad_key_own, grad_value_own], 1).astype(jnp.bfloat16)
    qkv_grad = contract_rows(entry_low, mapped_low)
    grad_entry = contract_cols(mapped_low, qkv_full)
    gain_one_grad = jnp.sum(grad_entry * normed_one, axis=0)
    shift_one_grad = jnp.sum(grad_entry, axis=0)
    input_grad = grad_resid + norm_back(grad_entry * table[0], normed_one, inverse_one)
    head_rows = jnp.stack(
        [
            gain_one_grad,
            shift_one_grad,
            query_bias_grad,
            value_bias_grad,
            out_bias_grad,
            gain_two_grad,
            shift_two_grad,
            down_bias_grad,
        ]
    )
    small_grad = jnp.concatenate([head_rows, up_bias_grad.reshape(4, model_width)], 0)
    small_halves = small_grad.reshape(small_grad.shape[0], shard_count, -1).transpose(1, 0, 2)
    small_packed = jnp.stack(
        [small_rows(small_halves[index], blocks) for index in range(shard_count)]
    ).reshape(shard_count, lax.axis_size(CORE), lax.axis_size(OUTER), 1, SMALL_WIDTH)
    small_packed = small_packed.transpose(1, 2, 0, 3, 4)
    qkv_sum, small_sum = reduce_rows([split_rows(qkv_grad), small_packed], core_on_dma=True)
    qkv_total = qkv_sum.reshape(qkv_weight.shape)
    small_total = small_sum.reshape(-1)[: small_params.size].reshape(small_params.shape)
    rate = 2.0 / math.sqrt(model_width * tok_rows * shard_count * group_count)
    qkv_new = nesterov(qkv_total, qkv_weight, qkv_momentum, qkv_average, rate)
    out_new = nesterov(out_total, out_weight, out_momentum, out_average, rate)
    up_new = nesterov(up_total, up_weight, up_momentum, up_average, rate)
    down_new = nesterov(down_total, down_weight, down_momentum, down_average, rate)
    small_new = nesterov(small_total, small_params, small_momentum, small_average, rate)
    return (
        block_out,
        input_grad,
        qkv_new[0],
        qkv_new[1],
        qkv_new[2],
        out_new[0],
        out_new[1],
        out_new[2],
        up_new[0],
        up_new[1],
        up_new[2],
        down_new[0],
        down_new[1],
        down_new[2],
        small_new[0],
        small_new[1],
        small_new[2],
    )


def solution(mesh):
    cores = 2
    devices = mesh.devices.reshape(mesh.shape["group"] // cores, cores, mesh.shape[SHARD])
    inner_mesh = jax.sharding.Mesh(devices, (OUTER, CORE, SHARD))
    rows = P((OUTER, CORE, SHARD), None)
    in_specs = (
        rows,
        rows,
        P(),
        P(SHARD, None),
        P(SHARD, None),
        P(SHARD, None),
        P(SHARD, None),
        P(SHARD, None),
        P(SHARD, None),
        P(None, SHARD),
        P(None, SHARD),
        P(None, SHARD),
        P(SHARD, None),
        P(SHARD, None),
        P(SHARD, None),
        P(None, SHARD),
        P(None, SHARD),
        P(None, SHARD),
    )
    out_specs = (
        rows,
        rows,
        P(SHARD, None),
        P(SHARD, None),
        P(SHARD, None),
        P(SHARD, None),
        P(SHARD, None),
        P(SHARD, None),
        P(None, SHARD),
        P(None, SHARD),
        P(None, SHARD),
        P(SHARD, None),
        P(SHARD, None),
        P(SHARD, None),
        P(None, SHARD),
        P(None, SHARD),
        P(None, SHARD),
    )

    return jax.shard_map(body, mesh=inner_mesh, in_specs=in_specs, out_specs=out_specs, check_vma=False)
```
